32 devices in a mesh: data: 2 (over x), outer: 4 (over z), expert: 4 (over y, core).
Axes of the slice: x: 2, y: 2, z: 4, core: 2. Of those that a mesh axis runs over, the one named last changes fastest.
Arguments:
- tokens: bfloat16 [2048, 2048], P(('data', 'outer', 'expert')), parts along dimension 0
- w_router: bfloat16 [2048, 64], replicated
- routes: int32 [2048, 8], P(('data', 'outer', 'expert')), parts along dimension 0
- w_gate: bfloat16 [64, 2048, 1024], P(('outer', 'expert'))
- w_up: bfloat16 [64, 2048, 1024], P(('outer', 'expert'))
- w_down: bfloat16 [64, 1024, 2048], P(('outer', 'expert'))
Outputs:
- output: bfloat16 [2048, 2048], P(('data', 'outer', 'expert')), parts along dimension 0
There are 2 independent parts. The reference program is written for one: setup_inputs(seed, part) draws one part's arguments, and reference() takes and returns one part's arrays. A program takes and returns all parts, laid end to end along the dimension named above; an argument that names none is the same for every part.
All inputs are finite; a program needn't handle non-finite values.
Results may differ from the reference program's by a relative error of at most 0.00127.
Values are sent between devices in bfloat16 or wider.
A program may use at most 1 GiB of HBM per device.

```python
import jax
import jax.numpy as jnp
from jax import lax

D = 2048
FF = 1024
EXPERTS = 64
TOPK = 8
TOKENS = 64
OUTER = 4
GROUP = 4
LIMIT = 2

DEVICES = OUTER * GROUP
ROWS = DEVICES * TOKENS
PER_OUTER = EXPERTS // OUTER
CAPACITY = (5 * TOKENS * TOPK + 4 * EXPERTS - 1) // (4 * EXPERTS)


def draw_routes(route_key):
    key_hot, key_grp, key_exp = jax.random.split(route_key, 3)
    score_span = 2 ** 20
    hot_dev = jax.random.randint(key_hot, (DEVICES,), 0, EXPERTS)
    hot_tok = jnp.repeat(hot_dev, TOKENS)
    forced = (jnp.arange(ROWS) % TOKENS) < CAPACITY
    outer_ids = jnp.arange(OUTER)
    grp_score = jax.random.randint(key_grp, (ROWS, OUTER), 0, score_span) * OUTER + outer_ids[None, :]
    grp_boost = forced[:, None] & (outer_ids[None, :] == (hot_tok // PER_OUTER)[:, None])
    grp_score = jnp.where(grp_boost, score_span * OUTER, grp_score)
    groups = jnp.argsort(-grp_score, axis=1)[:, :LIMIT]
    cand_count = LIMIT * PER_OUTER
    cand_ids = (groups[:, :, None] * PER_OUTER + jnp.arange(PER_OUTER)[None, None, :]).reshape(ROWS, cand_count)
    cand_score = jax.random.randint(key_exp, (ROWS, cand_count), 0, score_span) * cand_count + jnp.arange(cand_count)[None, :]
    cand_boost = forced[:, None] & (cand_ids == hot_tok[:, None])
    cand_score = jnp.where(cand_boost, score_span * cand_count, cand_score)
    pick_order = jnp.argsort(-cand_score, axis=1)[:, :TOPK]
    return jnp.take_along_axis(cand_ids, pick_order, axis=1).astype(jnp.int32)


def setup_inputs(seed: int = 0, part: int = 0) -> dict:
    base_key = jax.random.key(seed)
    part_key = jax.random.fold_in(base_key, part)
    key_tok, key_route = jax.random.split(part_key)
    key_router, key_gate, key_up, key_down = jax.random.split(base_key, 4)
    tokens = jax.random.normal(key_tok, (ROWS, D), jnp.float32).astype(jnp.bfloat16)
    w_router = (jax.random.normal(key_router, (D, EXPERTS), jnp.float32) * (2.0 / D ** 0.5)).astype(jnp.bfloat16)
    routes = draw_routes(key_route)
    w_gate = (jax.random.normal(key_gate, (EXPERTS, D, FF), jnp.float32) * D ** -0.5).astype(jnp.bfloat16)
    w_up = (jax.random.normal(key_up, (EXPERTS, D, FF), jnp.float32) * D ** -0.5).astype(jnp.bfloat16)
    w_down = (jax.random.normal(key_down, (EXPERTS, FF, D), jnp.float32) * FF ** -0.5).astype(jnp.bfloat16)
    return {'tokens': tokens, 'w_router': w_router, 'routes': routes, 'w_gate': w_gate, 'w_up': w_up, 'w_down': w_down}


def reference(tokens, w_router, routes, w_gate, w_up, w_down):
    logits = jnp.dot(tokens, w_router, preferred_element_type=jnp.float32)
    gate_vals = jax.nn.softmax(jnp.take_along_axis(logits, routes, axis=1), axis=-1)
    flat_ids = routes.reshape(DEVICES, TOKENS * TOPK)
    onehot = (flat_ids[:, :, None] == jnp.arange(EXPERTS)[None, None, :]).astype(jnp.int32)
    slot_pos = jnp.sum((jnp.cumsum(onehot, axis=1) - onehot) * onehot, axis=2)
    src_ids = jnp.arange(DEVICES)[:, None]
    total_slots = EXPERTS * DEVICES * CAPACITY
    dest_slot = jnp.where(slot_pos < CAPACITY, flat_ids * (DEVICES * CAPACITY) + src_ids * CAPACITY + slot_pos, total_slots).reshape(-1)
    pair_tok = jnp.arange(ROWS * TOPK, dtype=jnp.int32) // TOPK
    slot_tok = jnp.full((total_slots,), ROWS, jnp.int32).at[dest_slot].set(pair_tok, mode='drop')
    slot_gate = jnp.zeros((total_slots,), jnp.float32).at[dest_slot].set(gate_vals.reshape(-1), mode='drop')

    def expert_step(accum, operands):
        rows_tok, rows_gate, gate_mat, up_mat, down_mat = operands
        picked = jnp.take(tokens, rows_tok, axis=0, mode='fill', fill_value=0)
        gate_act = jnp.dot(picked, gate_mat, preferred_element_type=jnp.float32)
        up_lin = jnp.dot(picked, up_mat, preferred_element_type=jnp.float32)
        hidden = (jax.nn.silu(gate_act) * up_lin).astype(jnp.bfloat16)
        expert_out = jnp.dot(hidden, down_mat, preferred_element_type=jnp.float32).astype(jnp.bfloat16)
        accum = accum.at[rows_tok].add(rows_gate[:, None] * expert_out.astype(jnp.float32), mode='drop')
        return accum, None

    accum_init = jnp.zeros((ROWS, D), jnp.float32)
    operands = (slot_tok.reshape(EXPERTS, DEVICES * CAPACITY), slot_gate.reshape(EXPERTS, DEVICES * CAPACITY), w_gate, w_up, w_down)
    combined, _ = lax.scan(expert_step, accum_init, operands)
    return combined.astype(jnp.bfloat16)
```

```python
import functools

import jax
import jax.numpy as jnp
from jax import lax
from jax.experimental import pallas as pl
from jax.experimental.pallas import tpu as pltpu
from jax.sharding import PartitionSpec as P

MESH = pl.DeviceIdType.MESH
F32, BF16 = jnp.float32, jnp.bfloat16
PLANES = 4
COLS = 4
JLOC = 4
TOK = 64
TOPK = 8
CAP = 10
DIM = 2048
FF = 1024
NEXP = 64
CW = 512
NC = DIM // CW
SL = PLANES * CAP
ROWS = COLS * SL
CT = PLANES * TOK


def iota(shape, dim):
    return lax.broadcasted_iota(jnp.int32, shape, dim)


def dot(a, b):
    return jnp.dot(a, b, preferred_element_type=F32)


def dot_nt(a, b):
    return lax.dot_general(a, b, (((1,), (1,)), ((), ())), preferred_element_type=F32)


def dot_tn(a, b):
    return lax.dot_general(a, b, (((0,), (0,)), ((), ())), preferred_element_type=F32)


def kernel(x_hbm, wr_ref, rt_ref, wg_hbm, wu_hbm, wd_hbm, out_ref,
           x_all, r_all, xs, wgb, wub, wdb, hid, ysend, yrecv, wst, part, zr,
           lsem, wsem, dsem, bx_s, br_s, bx_r, br_r, ys_s, ys_r, zs_s, zs_r):
    d = lax.axis_index('data')
    o = lax.axis_index('outer')
    e = lax.axis_index('expert')
    c = e % 2
    y = e // 2
    mate = e + 1 - 2 * c
    yp = e + 2 - 4 * y
    diag = mate + yp - e
    rel = (e, mate, yp, diag)

    own = pl.ds(pl.multiple_of(o * TOK, TOK), TOK)
    xcp = pltpu.make_async_copy(x_hbm, x_all.at[e, own], lsem)
    xcp.start()
    wcp = []
    for j in range(JLOC):
        a = pltpu.make_async_copy(wg_hbm.at[j], wgb.at[j], wsem.at[0, j])
        b = pltpu.make_async_copy(wu_hbm.at[j], wub.at[j], wsem.at[1, j])
        a.start()
        b.start()
        wcp.append((a, b))

    def wd_copy(k):
        return pltpu.make_async_copy(
            wd_hbm.at[:, :, pl.ds(k * CW, CW)], wdb.at[k % 2], dsem.at[k % 2])

    wd_copy(0).start()
    wd_copy(1).start()

    dup = (iota((TOK, 128), 1) % TOK == iota((TOK, 128), 0)).astype(BF16)
    r_all[e, o] = dot_tn((rt_ref[...] + 1).astype(F32).astype(BF16), dup) - 1.0

    barrier = pltpu.get_barrier_semaphore()

    def greet(oo, ee):
        pl.semaphore_signal(barrier, inc=1, device_id=(d, oo, ee), device_id_type=MESH)

    for q in range(1, 4):
        greet(o, rel[q])

    @pl.when(o > 0)
    def _():
        greet(o - 1, e)

    @pl.when(o < PLANES - 1)
    def _():
        greet(o + 1, e)

    edge = (o == 0) | (o == PLANES - 1)

    @pl.when(edge)
    def _():
        pl.semaphore_wait(barrier, 4)

    @pl.when(jnp.logical_not(edge))
    def _():
        pl.semaphore_wait(barrier, 5)

    def block(col, p, direction, oo, ee):
        rows = pl.ds(pl.multiple_of(p * TOK, TOK), TOK)
        big = pltpu.make_async_remote_copy(
            src_ref=x_all.at[col, rows], dst_ref=x_all.at[col, rows],
            send_sem=bx_s.at[direction, p], recv_sem=bx_r.at[col, p],
            device_id=(d, oo, ee), device_id_type=MESH)
        small = pltpu.make_async_remote_copy(
            src_ref=r_all.at[col, p], dst_ref=r_all.at[col, p],
            send_sem=br_s.at[direction, p], recv_sem=br_r.at[col, p],
            device_id=(d, oo, ee), device_id_type=MESH)
        return small, big

    def send(col, p, direction, oo, ee):
        for cp in block(col, p, direction, oo, ee):
            cp.start()

    def arrive(col, p):
        for cp in block(col, p, 0, o, mate):
            cp.wait_recv()

    def sent(col, p, direction):
        for cp in block(col, p, direction, o, mate):
            cp.wait_send()

    xcp.wait()

    @pl.when(o < PLANES - 1)
    def _():
        send(e, o, 0, o + 1, e)

    @pl.when(o > 0)
    def _():
        send(e, o, 1, o - 1, e)

    send(e, o, 2, o, yp)
    send(e, o, 3, o, mate)

    def from_y(p):
        arrive(yp, p)
        send(yp, p, 4, o, mate)

    for dist in range(1, PLANES):
        @pl.when(o >= dist)
        def _():
            p = o - dist
            arrive(e, p)

            @pl.when(o < PLANES - 1)
            def _():
                send(e, p, 0, o + 1, e)

            send(e, p, 2, o, yp)
            send(e, p, 3, o, mate)

        @pl.when(o + dist < PLANES)
        def _():
            p = o + dist
            arrive(e, p)

            @pl.when(o > 0)
            def _():
                send(e, p, 1, o - 1, e)

            send(e, p, 2, o, yp)
            send(e, p, 3, o, mate)

        back = dist - 1

        @pl.when(o >= back)
        def _():
            from_y(o - back)

        if back:
            @pl.when(o + back < PLANES)
            def _():
                from_y(o + back)

    col_i, row_i = iota((CT, CT), 1), iota((CT, CT), 0)
    same = col_i // TOK == row_i // TOK
    before = (same & (row_i < col_i)).astype(BF16)
    after = (same & (col_i < row_i)).astype(BF16)
    eye = (col_i == row_i).astype(BF16)

    def lanes(col):
        r = r_all[col]
        low = iota((TOPK, 128), 1) < TOK
        return jnp.concatenate(
            [jnp.where(low, r[0], r[1]), jnp.where(low, r[2], r[3])], axis=1)

    r_own = lanes(e)
    exp_id = iota((NEXP, CT), 0).astype(F32)
    hot = jnp.zeros((NEXP, CT), F32)
    for k in range(TOPK):
        hot = hot + (r_own[k:k + 1, :] == exp_id).astype(F32)
    hot = hot.astype(BF16)
    chosen = dot_nt(eye, hot)
    pos = dot_nt(after, hot)
    logits = dot(x_all[e], wr_ref[...])
    top = jnp.max(jnp.where(chosen > 0.5, logits, -jnp.inf), axis=1, keepdims=True)
    ex = jnp.where(chosen > 0.5, jnp.exp(logits - top), 0.0)
    gate = ex / jnp.sum(ex, axis=1, keepdims=True)
    pos = jnp.where(chosen > 0.5, pos, -1.0)
    g1 = gate.astype(BF16)
    rest = gate - g1.astype(F32)
    g2 = rest.astype(BF16)
    g3 = (rest - g2.astype(F32)).astype(BF16)
    for q in range(COLS):
        n_i, k_i = iota((NEXP, ROWS), 1), iota((NEXP, ROWS), 0)
        first = (o * COLS + rel[q]) * JLOC
        expand = (k_i == first + n_i // SL).astype(BF16)
        slot = iota((CT, ROWS), 1) % SL
        hit = ((slot // CAP == iota((CT, ROWS), 0) // TOK)
               & (dot(pos.astype(BF16), expand) == (slot % CAP).astype(F32)))
        for k, g in enumerate((g1, g2, g3)):
            wst[q, k * CT:(k + 1) * CT, :] = jnp.where(hit, dot(g, expand), 0.0).astype(BF16)

    mine = ((o * COLS + e) * JLOC).astype(F32)

    def select(col):
        r = lanes(col)
        rows = []
        for j in range(JLOC):
            rows.append(jnp.max((r == mine + j).astype(F32), axis=0, keepdims=True))
        m = jnp.concatenate(rows + [jnp.zeros((8 - JLOC, CT), F32)], axis=0)
        pm = jnp.where(m > 0.5, dot(m.astype(BF16), before), -1.0)
        s_i = iota((SL, CT), 0)
        ok = s_i // CAP == iota((SL, CT), 1) // TOK
        want = (s_i % CAP).astype(F32)
        pieces = [(ok & (pm[j:j + 1, :] == want)).astype(F32) for j in range(JLOC)]
        return jnp.concatenate(pieces, axis=0).astype(BF16)

    def pick(ca, cb, base):
        sa, sb = select(ca), select(cb)
        for n in range(DIM // 512):
            cols = pl.ds(n * 512, 512)
            ra = dot(sa, x_all[ca, :, cols])
            rb = dot(sb, x_all[cb, :, cols])
            for j in range(JLOC):
                both = jnp.concatenate([ra[j * SL:(j + 1) * SL], rb[j * SL:(j + 1) * SL]], axis=0)
                xs[j, base:base + 2 * SL, cols] = both.astype(BF16)

    for p in range(PLANES):
        arrive(mate, p)
    pick(e, mate, 0)

    @pl.when(o == 0)
    def _():
        from_y(o + 3)

    @pl.when(o == PLANES - 1)
    def _():
        from_y(o - 3)

    for p in range(PLANES):
        arrive(diag, p)
    pick(yp, diag, 2 * SL)

    for j in range(JLOC):
        wcp[j][0].wait()
        wcp[j][1].wait()
        for n in range(FF // 512):
            cols = slice(n * 512, (n + 1) * 512)
            ga = dot(xs[j], wgb[j, :, cols])
            up = dot(xs[j], wub[j, :, cols])
            hid[j, :, cols] = (jax.nn.silu(ga) * up).astype(BF16)

    def ycopy(k, q):
        return pltpu.make_async_remote_copy(
            src_ref=ysend.at[k, q - 1], dst_ref=yrecv.at[k, q],
            send_sem=ys_s.at[k, q - 1], recv_sem=ys_r.at[k, q - 1],
            device_id=(d, o, rel[q]), device_id_type=MESH)

    for k in range(NC):
        wd_copy(k).wait()
        outs = [dot(hid[j], wdb[k % 2, j]) for j in range(JLOC)]
        for q in (2, 3, 1, 0):
            rows = jnp.concatenate([r[q * SL:(q + 1) * SL] for r in outs], axis=0).astype(BF16)
            if q:
                ysend[k, q - 1] = rows
                ycopy(k, q).start()
            else:
                yrecv[k, 0] = rows
        if k + 2 < NC:
            wd_copy(k + 2).start()

    def zcopy(k, p, slot, oo):
        return pltpu.make_async_remote_copy(
            src_ref=part.at[k, p], dst_ref=zr.at[k, slot],
            send_sem=zs_s.at[k, p], recv_sem=zs_r.at[k, slot],
            device_id=(d, oo, e), device_id_type=MESH)

    def up(k, p):
        zcopy(k, p, p, o + 1).start()

    def down(k, p):
        @pl.when(o == p + 1)
        def _():
            zcopy(k, p, PLANES, o - 1).start()

        @pl.when(o > p + 1)
        def _():
            zcopy(k, p, p, o - 1).start()

    def sums(k):
        for q in range(1, COLS):
            ycopy(k, q).wait_recv()
        acc = dot(wst[0], yrecv[k, 0])
        for q in range(1, COLS):
            acc = acc + dot(wst[q], yrecv[k, q])
        tot = acc[0:CT] + acc[CT:2 * CT] + acc[2 * CT:3 * CT]
        for p in range(PLANES):
            part[k, p] = tot[p * TOK:(p + 1) * TOK]

        @pl.when(o == 0)
        def _():
            for p in (3, 2, 1):
                up(k, p)

        @pl.when(o == PLANES - 1)
        def _():
            for p in (0, 1, 2):
                down(k, p)

    def relay(k):
        for p in (3, 2):
            @pl.when((o > 0) & (o < p))
            def _():
                zcopy(k, p, p, o).wait_recv()
                part[k, p] = part[k, p] + zr[k, p]
                up(k, p)
        for p in (0, 1):
            @pl.when((o < PLANES - 1) & (o > p))
            def _():
                zcopy(k, p, p, o).wait_recv()
                part[k, p] = part[k, p] + zr[k, p]
                down(k, p)

    def finish(k):
        cols = pl.ds(k * CW, CW)

        @pl.when(o == 0)
        def _():
            zcopy(k, 0, PLANES, o).wait_recv()
            out_ref[:, cols] = (part[k, 0] + zr[k, PLANES]).astype(BF16)

        @pl.when(o == PLANES - 1)
        def _():
            zcopy(k, 0, PLANES - 1, o).wait_recv()
            out_ref[:, cols] = (part[k, PLANES - 1] + zr[k, PLANES - 1]).astype(BF16)

        @pl.when((o > 0) & (o < PLANES - 1))
        def _():
            zcopy(k, 0, o, o).wait_recv()
            zcopy(k, 0, PLANES, o).wait_recv()
            out_ref[:, cols] = (part[k, o] + zr[k, o] + zr[k, PLANES]).astype(BF16)

    sums(0)
    for k in range(1, NC):
        sums(k)
        relay(k - 1)
    relay(NC - 1)
    for k in range(NC):
        finish(k)

    for p in range(PLANES):
        @pl.when((o < PLANES - 1) & (p <= o))
        def _():
            sent(e, p, 0)

        @pl.when((o > 0) & (p >= o))
        def _():
            sent(e, p, 1)

        sent(e, p, 2)
        sent(e, p, 3)
        sent(yp, p, 4)
    for k in range(NC):
        for q in range(1, COLS):
            ycopy(k, q).wait_send()
        for p in range(PLANES):
            @pl.when(o != p)
            def _():
                zcopy(k, p, p, o).wait_send()


def solution(mesh):
    row_spec = P(('data', 'outer', 'expert'), None)
    weight_spec = P(('outer', 'expert'), None, None)
    vmem = pl.BlockSpec(memory_space=pltpu.VMEM)
    anyspace = pl.BlockSpec(memory_space=pl.ANY)
    dma = pltpu.SemaphoreType.DMA

    def per_device(tokens, w_router, routes, w_gate, w_up, w_down):
        return pl.pallas_call(
            kernel,
            name='moe',
            out_shape=jax.ShapeDtypeStruct((TOK, DIM), BF16),
            in_specs=[anyspace, vmem, vmem, anyspace, anyspace, anyspace],
            out_specs=vmem,
            scratch_shapes=[
                pltpu.VMEM((COLS, CT, DIM), BF16),
                pltpu.VMEM((COLS, PLANES, TOPK, 128), F32),
                pltpu.VMEM((JLOC, ROWS, DIM), BF16),
                pltpu.VMEM((JLOC, DIM, FF), BF16),
                pltpu.VMEM((JLOC, DIM, FF), BF16),
                pltpu.VMEM((2, JLOC, FF, CW), BF16),
                pltpu.VMEM((JLOC, ROWS, FF), BF16),
                pltpu.VMEM((NC, COLS - 1, ROWS, CW), BF16),
                pltpu.VMEM((NC, COLS, ROWS, CW), BF16),
                pltpu.VMEM((COLS, 3 * CT, ROWS), BF16),
                pltpu.VMEM((NC, PLANES, TOK, CW), F32),
                pltpu.VMEM((NC, PLANES + 1, TOK, CW), F32),
                dma, dma((2, JLOC)), dma((2,)),
                dma((5, PLANES)), dma((5, PLANES)),
                dma((COLS, PLANES)), dma((COLS, PLANES)),
                dma((NC, COLS - 1)), dma((NC, COLS - 1)),
                dma((NC, PLANES)), dma((NC, PLANES + 1)),
            ],
            compiler_params=pltpu.CompilerParams(
                collective_id=0, has_side_effects=True, vmem_limit_bytes=67043328),
        )(tokens, w_router, routes, w_gate, w_up, w_down)

    return jax.shard_map(
        per_device, mesh=mesh,
        in_specs=(row_spec, P(), row_spec, weight_spec, weight_spec, weight_spec),
        out_specs=row_spec, check_vma=False)
```

```python
import functools

import jax
import jax.numpy as jnp
from jax import lax
from jax.experimental import pallas as pl
from jax.experimental.pallas import tpu as pltpu
from jax.sharding import PartitionSpec as P

MESH = pl.DeviceIdType.MESH
F32, BF16 = jnp.float32, jnp.bfloat16
PLANES = 4
COLS = 4
JLOC = 4
TOK = 64
TOPK = 8
CAP = 10
DIM = 2048
FF = 1024
NEXP = 64
CW = 256
NC = DIM // CW
SL = PLANES * CAP
ROWS = COLS * SL
CT = PLANES * TOK
HALF = TOK // 2
WSLOT = 4


def iota(shape, dim):
    return lax.broadcasted_iota(jnp.int32, shape, dim)


def dot(a, b):
    return jnp.dot(a, b, preferred_element_type=F32)


def dot_nt(a, b):
    return lax.dot_general(a, b, (((1,), (1,)), ((), ())), preferred_element_type=F32)


def dot_tn(a, b):
    return lax.dot_general(a, b, (((0,), (0,)), ((), ())), preferred_element_type=F32)


def kernel(x_hbm, wr_hbm, rt_ref, wg_hbm, wu_hbm, wd_hbm, out_hbm,
           x_all, r_all, wr, xs, wgb, wub, wdb, hid, ysend, yrecv, wst, part, zr, obuf,
           lsem, wsem, dsem, osem, bx_s, br_s, bx_r, br_r, ys_s, ys_r, zs_s, zs_r):
    d = lax.axis_index('data')
    o = lax.axis_index('outer')
    e = lax.axis_index('expert')
    c = e % 2
    y = e // 2
    mate = e + 1 - 2 * c
    yp = e + 2 - 4 * y
    diag = mate + yp - e
    rel = (e, mate, yp, diag)
    last = PLANES - 1

    own = pl.ds(pl.multiple_of(o * TOK, TOK), TOK)
    xcp = pltpu.make_async_copy(x_hbm, x_all.at[e, own], lsem.at[0])
    xcp.start()

    dup = (iota((TOK, 128), 1) % TOK == iota((TOK, 128), 0)).astype(BF16)
    r_all[e, o] = dot(rt_ref[...].astype(F32).astype(BF16), dup)

    barrier = pltpu.get_barrier_semaphore()

    def greet(oo, ee):
        pl.semaphore_signal(barrier, inc=1, device_id=(d, oo, ee), device_id_type=MESH)

    for q in range(1, 4):
        greet(o, rel[q])

    @pl.when(o > 0)
    def _():
        greet(o - 1, e)

    @pl.when(o < last)
    def _():
        greet(o + 1, e)

    xcp.wait()
    wrcp = pltpu.make_async_copy(wr_hbm, wr, lsem.at[1])
    wrcp.start()
    wcp = []
    for j in range(JLOC):
        a = pltpu.make_async_copy(wg_hbm.at[j], wgb.at[j], wsem.at[0, j])
        b = pltpu.make_async_copy(wu_hbm.at[j], wub.at[j], wsem.at[1, j])
        a.start()
        b.start()
        wcp.append((a, b))

    def wd_copy(k):
        return pltpu.make_async_copy(
            wd_hbm.at[:, :, pl.ds(k * CW, CW)], wdb.at[k % WSLOT], dsem.at[k % WSLOT])

    for k in range(WSLOT):
        wd_copy(k).start()

    edge = (o == 0) | (o == last)

    @pl.when(edge)
    def _():
        pl.semaphore_wait(barrier, 4)

    @pl.when(jnp.logical_not(edge))
    def _():
        pl.semaphore_wait(barrier, 5)

    UP, DOWN, SIDE, MATE, PASS, YUP, YDOWN = range(7)

    def block(col, p, h, direction, oo, ee):
        rows = pl.ds(pl.multiple_of(p * TOK + h * HALF, HALF), HALF)
        cps = [pltpu.make_async_remote_copy(
            src_ref=x_all.at[col, rows], dst_ref=x_all.at[col, rows],
            send_sem=bx_s.at[direction, p, h], recv_sem=bx_r.at[col, p, h],
            device_id=(d, oo, ee), device_id_type=MESH)]
        if h == 0:
            cps.insert(0, pltpu.make_async_remote_copy(
                src_ref=r_all.at[col, p], dst_ref=r_all.at[col, p],
                send_sem=br_s.at[direction, p], recv_sem=br_r.at[col, p],
                device_id=(d, oo, ee), device_id_type=MESH))
        return cps

    def send(col, p, h, direction, oo, ee):
        for cp in block(col, p, h, direction, oo, ee):
            cp.start()

    def arrive(col, p, h):
        for cp in block(col, p, h, 0, o, mate):
            cp.wait_recv()

    def sent(col, p, h, direction):
        for cp in block(col, p, h, direction, o, mate):
            cp.wait_send()

    def sides(dist, fn):
        @pl.when(o >= dist)
        def _():
            fn(o - dist, -1)

        @pl.when(o + dist < PLANES)
        def _():
            fn(o + dist, 1)

    def zget(dist, h):
        def one(p, side):
            arrive(e, p, h)
            if side < 0:
                @pl.when(o < last)
                def _():
                    send(e, p, h, UP, o + 1, e)
            else:
                @pl.when(o > 0)
                def _():
                    send(e, p, h, DOWN, o - 1, e)
            if (dist, h) != (1, 0):
                send(e, p, h, SIDE, o, yp)
            send(e, p, h, MATE, o, mate)

        sides(dist, one)

    def yget(dist, h):
        def one(p, side):
            arrive(yp, p, h)
            send(yp, p, h, PASS, o, mate)

        sides(dist, one)

    for h in range(2):
        @pl.when(o < last)
        def _():
            send(e, o, h, UP, o + 1, e)

        @pl.when(o > 0)
        def _():
            send(e, o, h, DOWN, o - 1, e)

        send(e, o, h, SIDE, o, yp)
        send(e, o, h, MATE, o, mate)

    zget(1, 0)
    arrive(yp, o, 0)

    @pl.when(o < last)
    def _():
        send(yp, o, 0, YUP, o + 1, e)

    @pl.when(o > 0)
    def _():
        send(yp, o, 0, YDOWN, o - 1, e)

    send(yp, o, 0, PASS, o, mate)
    zget(1, 1)
    arrive(yp, o, 1)
    send(yp, o, 1, PASS, o, mate)
    zget(2, 0)
    yget(1, 0)
    zget(2, 1)
    yget(1, 1)
    zget(3, 0)
    yget(2, 0)
    zget(3, 1)
    yget(2, 1)

    col_i, row_i = iota((CT, CT), 1), iota((CT, CT), 0)
    same = col_i // TOK == row_i // TOK
    before = (same & (row_i < col_i)).astype(BF16)
    after = (same & (col_i < row_i)).astype(BF16)
    eye = (col_i == row_i).astype(BF16)

    def lanes(col):
        r = r_all[col]
        low = iota((TOPK, 128), 1) < TOK
        return jnp.concatenate(
            [jnp.where(low, r[0], r[1]), jnp.where(low, r[2], r[3])], axis=1)

    r_own = lanes(e)
    exp_id = iota((NEXP, CT), 0).astype(F32)
    hot = jnp.zeros((NEXP, CT), F32)
    for k in range(TOPK):
        hot = hot + (r_own[k:k + 1, :] == exp_id).astype(F32)
    hot = hot.astype(BF16)
    chosen = dot_nt(eye, hot)
    pos = dot_nt(after, hot)
    wrcp.wait()
    logits = dot_nt(x_all[e], wr[...])
    top = jnp.max(jnp.where(chosen > 0.5, logits, -jnp.inf), axis=1, keepdims=True)
    ex = jnp.where(chosen > 0.5, jnp.exp(logits - top), 0.0)
    gate = ex / jnp.sum(ex, axis=1, keepdims=True)
    pos = jnp.where(chosen > 0.5, pos, -1.0)
    g1 = gate.astype(BF16)
    rest = gate - g1.astype(F32)
    g2 = rest.astype(BF16)
    g3 = (rest - g2.astype(F32)).astype(BF16)
    for q in range(COLS):
        n_i, k_i = iota((NEXP, ROWS), 1), iota((NEXP, ROWS), 0)
        first = (o * COLS + rel[q]) * JLOC
        expand = (k_i == first + n_i // SL).astype(BF16)
        slot = iota((CT, ROWS), 1) % SL
        hit = ((slot // CAP == iota((CT, ROWS), 0) // TOK)
               & (dot(pos.astype(BF16), expand) == (slot % CAP).astype(F32)))
        for k, g in enumerate((g1, g2, g3)):
            wst[q, k * CT:(k + 1) * CT, :] = jnp.where(hit, dot(g, expand), 0.0).astype(BF16)

    mine = ((o * COLS + e) * JLOC).astype(F32)

    def select(col):
        r = lanes(col)
        rows = []
        for j in range(JLOC):
            rows.append(jnp.max((r == mine + j).astype(F32), axis=0, keepdims=True))
        m = jnp.concatenate(rows + [jnp.zeros((8 - JLOC, CT), F32)], axis=0)
        pm = jnp.where(m > 0.5, dot(m.astype(BF16), before), -1.0)
        s_i = iota((SL, CT), 0)
        ok = s_i // CAP == iota((SL, CT), 1) // TOK
        want = (s_i % CAP).astype(F32)
        pieces = [(ok & (pm[j:j + 1, :] == want)).astype(F32) for j in range(JLOC)]
        return jnp.concatenate(pieces, axis=0).astype(BF16)

    def pick(ca, cb, base):
        sa, sb = select(ca), select(cb)
        for n in range(DIM // 512):
            cols = pl.ds(n * 512, 512)
            ra = dot(sa, x_all[ca, :, cols])
            rb = dot(sb, x_all[cb, :, cols])
            for j in range(JLOC):
                both = jnp.concatenate([ra[j * SL:(j + 1) * SL], rb[j * SL:(j + 1) * SL]], axis=0)
                xs[j, base:base + 2 * SL, cols] = both.astype(BF16)

    for p in range(PLANES):
        for h in range(2):
            arrive(mate, p, h)
    pick(e, mate, 0)
    yget(3, 0)
    yget(3, 1)
    for p in range(PLANES):
        for h in range(2):
            arrive(diag, p, h)
    pick(yp, diag, 2 * SL)

    for j in range(JLOC):
        wcp[j][0].wait()
        wcp[j][1].wait()
        for n in range(FF // 512):
            cols = slice(n * 512, (n + 1) * 512)
            ga = dot(xs[j], wgb[j, :, cols])
            up = dot(xs[j], wub[j, :, cols])
            hid[j, :, cols] = (jax.nn.silu(ga) * up).astype(BF16)

    def ycopy(k, q):
        return pltpu.make_async_remote_copy(
            src_ref=ysend.at[k, q - 1], dst_ref=yrecv.at[k, q],
            send_sem=ys_s.at[k, q - 1], recv_sem=ys_r.at[k, q - 1],
            device_id=(d, o, rel[q]), device_id_type=MESH)

    for k in range(NC):
        wd_copy(k).wait()
        outs = [dot(hid[j], wdb[k % WSLOT, j]) for j in range(JLOC)]
        for q in (2, 3, 1, 0):
            rows = jnp.concatenate([r[q * SL:(q + 1) * SL] for r in outs], axis=0).astype(BF16)
            if q:
                ysend[k, q - 1] = rows
                ycopy(k, q).start()
            else:
                yrecv[k, 0] = rows
        if k + WSLOT < NC:
            wd_copy(k + WSLOT).start()

    def zcopy(k, p, slot, oo):
        return pltpu.make_async_remote_copy(
            src_ref=part.at[k, p], dst_ref=zr.at[k, slot],
            send_sem=zs_s.at[k, p], recv_sem=zs_r.at[k, slot],
            device_id=(d, oo, e), device_id_type=MESH)

    def up(k, p):
        zcopy(k, p, p, o + 1).start()

    def down(k, p):
        @pl.when(o == p + 1)
        def _():
            zcopy(k, p, PLANES, o - 1).start()

        @pl.when(o > p + 1)
        def _():
            zcopy(k, p, p, o - 1).start()

    def sums(k):
        for q in range(1, COLS):
            ycopy(k, q).wait_recv()
        acc = dot(wst[0], yrecv[k, 0])
        for q in range(1, COLS):
            acc = acc + dot(wst[q], yrecv[k, q])
        tot = acc[0:CT] + acc[CT:2 * CT] + acc[2 * CT:3 * CT]
        for p in range(PLANES):
            part[k, p] = tot[p * TOK:(p + 1) * TOK]

        @pl.when(o == 0)
        def _():
            for p in (3, 2, 1):
                up(k, p)

        @pl.when(o == PLANES - 1)
        def _():
            for p in (0, 1, 2):
                down(k, p)

    def pass_up(k, p):
        zcopy(k, p, p, o + 1).wait_recv()
        part[k, p] = part[k, p] + zr[k, p]
        up(k, p)

    def pass_down(k, p):
        zcopy(k, p, p, o - 1).wait_recv()
        part[k, p] = part[k, p] + zr[k, p]
        down(k, p)

    def relay_near(k):
        @pl.when(o == 1)
        def _():
            pass_up(k, 3)
            pass_up(k, 2)

        @pl.when(o == 2)
        def _():
            pass_down(k, 0)
            pass_down(k, 1)

    def relay_far(k):
        @pl.when(o == 1)
        def _():
            pass_down(k, 0)

        @pl.when(o == 2)
        def _():
            pass_up(k, 3)

    def ocopy(k):
        cols = pl.ds(k * CW, CW)
        return pltpu.make_async_copy(obuf.at[:, cols], out_hbm.at[:, cols], osem.at[k])

    def finish(k):
        cols = pl.ds(k * CW, CW)

        @pl.when(o == 0)
        def _():
            zcopy(k, 0, PLANES, o + 1).wait_recv()
            obuf[:, cols] = (part[k, 0] + zr[k, PLANES]).astype(BF16)

        @pl.when(o == last)
        def _():
            zcopy(k, 0, last, o - 1).wait_recv()
            obuf[:, cols] = (part[k, last] + zr[k, last]).astype(BF16)

        @pl.when((o > 0) & (o < last))
        def _():
            zcopy(k, 0, o, o + 1).wait_recv()
            zcopy(k, 0, PLANES, o + 1).wait_recv()
            obuf[:, cols] = (part[k, o] + zr[k, o] + zr[k, PLANES]).astype(BF16)

        ocopy(k).start()

    for k in range(NC + 2):
        if k < NC:
            sums(k)
        if 0 <= k - 1 < NC:
            relay_near(k - 1)
        if k >= 2:
            relay_far(k - 2)
    for k in range(NC):
        finish(k)
    for k in range(NC):
        ocopy(k).wait()

    for p in range(PLANES):
        for h in range(2):
            @pl.when((o < last) & (o >= p))
            def _():
                sent(e, p, h, UP)

            @pl.when((o > 0) & (o <= p))
            def _():
                sent(e, p, h, DOWN)

            if h:
                sent(e, p, h, SIDE)
            else:
                @pl.when((o != p - 1) & (o != p + 1))
                def _():
                    sent(e, p, h, SIDE)

            sent(e, p, h, MATE)
            sent(yp, p, h, PASS)

    @pl.when(o < last)
    def _():
        sent(yp, o, 0, YUP)

    @pl.when(o > 0)
    def _():
        sent(yp, o, 0, YDOWN)

    for k in range(NC):
        for q in range(1, COLS):
            ycopy(k, q).wait_send()
        for p in range(PLANES):
            @pl.when(o != p)
            def _():
                zcopy(k, p, p, 0).wait_send()


def solution(mesh):
    row_spec = P(('data', 'outer', 'expert'), None)
    weight_spec = P(('outer', 'expert'), None, None)
    vmem = pl.BlockSpec(memory_space=pltpu.VMEM)
    anyspace = pl.BlockSpec(memory_space=pl.ANY)
    dma = pltpu.SemaphoreType.DMA

    def per_device(tokens, w_router, routes, w_gate, w_up, w_down):
        return pl.pallas_call(
            kernel,
            name='moe',
            out_shape=jax.ShapeDtypeStruct((TOK, DIM), BF16),
            in_specs=[anyspace, anyspace, vmem, anyspace, anyspace, anyspace],
            out_specs=anyspace,
            scratch_shapes=[
                pltpu.VMEM((COLS, CT, DIM), BF16),
                pltpu.VMEM((COLS, PLANES, TOPK, 128), F32),
                pltpu.VMEM((NEXP, DIM), BF16),
                pltpu.VMEM((JLOC, ROWS, DIM), BF16),
                pltpu.VMEM((JLOC, DIM, FF), BF16),
                pltpu.VMEM((JLOC, DIM, FF), BF16),
                pltpu.VMEM((WSLOT, JLOC, FF, CW), BF16),
                pltpu.VMEM((JLOC, ROWS, FF), BF16),
                pltpu.VMEM((NC, COLS - 1, ROWS, CW), BF16),
                pltpu.VMEM((NC, COLS, ROWS, CW), BF16),
                pltpu.VMEM((COLS, 3 * CT, ROWS), BF16),
                pltpu.VMEM((NC, PLANES, TOK, CW), F32),
                pltpu.VMEM((NC, PLANES + 1, TOK, CW), F32),
                pltpu.VMEM((TOK, DIM), BF16),
                dma((2,)), dma((2, JLOC)), dma((WSLOT,)), dma((NC,)),
                dma((7, PLANES, 2)), dma((7, PLANES)),
                dma((COLS, PLANES, 2)), dma((COLS, PLANES)),
                dma((NC, COLS - 1)), dma((NC, COLS - 1)),
                dma((NC, PLANES)), dma((NC, PLANES + 1)),
            ],
            compiler_params=pltpu.CompilerParams(
                collective_id=0, has_side_effects=True, vmem_limit_bytes=67043328),
        )(tokens, w_router.T, routes.T, w_gate, w_up, w_down)

    return jax.shard_map(
        per_device, mesh=mesh,
        in_specs=(row_spec, P(), row_spec, weight_spec, weight_spec, weight_spec),
        out_specs=row_spec, check_vma=False)
```

```python
import jax
import jax.numpy as jnp
from jax import lax
from jax.experimental import pallas as pl
from jax.experimental.pallas import tpu as pltpu
from jax.sharding import PartitionSpec as P

MESH = pl.DeviceIdType.MESH
F32, BF16 = jnp.float32, jnp.bfloat16
PLANES = 4
COLS = 4
JLOC = 4
TOK = 64
TOPK = 8
CAP = 10
DIM = 2048
FF = 1024
NEXP = 64
CW = 256
NC = DIM // CW
HALF = TOK // 2
WSLOT = 6
GR = JLOC * CAP
MR = 2 * COLS * CAP
CT = 2 * TOK
HT = COLS * CT
NB, OWN, FAR, NEAR = range(4)
OUT, CROSS, SIDE, MATE, PASS, YOUT, YCROSS = range(7)


def iota(shape, dim):
    return lax.broadcasted_iota(jnp.int32, shape, dim)


def dot(a, b):
    return jnp.dot(a, b, preferred_element_type=F32)


def dot_nt(a, b):
    return lax.dot_general(a, b, (((1,), (1,)), ((), ())), preferred_element_type=F32)


def kernel(x_hbm, wr_hbm, rt_ref, wg_hbm, wu_hbm, wd_hbm, out_hbm,
           x_all, r_all, wr, xs, wgb, wub, wdb, hid, ysend, yrecv, wst, part, zr, obuf,
           lsem, wsem, dsem, osem, bx_s, br_s, bx_r, br_r, ys_s, ys_r, zs_s, zs_r):
    d = lax.axis_index('data')
    o = lax.axis_index('outer')
    e = lax.axis_index('expert')
    c = e % 2
    y = e // 2
    mate = e + 1 - 2 * c
    yp = e + 2 - 4 * y
    diag = mate + yp - e
    rel = (e, mate, yp, diag)
    side = o // 2
    nbp = o + 1 - 2 * (o % 2)
    other = PLANES - 1 - o
    planes = (nbp, o, 3 - 3 * side, 2 - side)
    halves = (side, 1 - side)
    end = (o == 0) | (o == PLANES - 1)
    inner = jnp.logical_not(end)

    def at_end(fn):
        pl.when(end)(fn)

    def at_inner(fn):
        pl.when(inner)(fn)

    def rows_of(col, g, h, n):
        p = planes[g]
        start = col * CT + (p % 2) * TOK + h * HALF
        return p // 2, pl.ds(pl.multiple_of(start, HALF), n)

    own_half, own_rows = rows_of(e, OWN, 0, TOK)
    xcp = pltpu.make_async_copy(x_hbm, x_all.at[own_half, own_rows], lsem.at[0])
    xcp.start()

    dup = (iota((TOK, 128), 1) % TOK == iota((TOK, 128), 0)).astype(BF16)
    r_all[side, e, o % 2] = dot(rt_ref[...].astype(F32).astype(BF16), dup)

    barrier = pltpu.get_barrier_semaphore()

    def greet(oo, ee):
        pl.semaphore_signal(barrier, inc=1, device_id=(d, oo, ee), device_id_type=MESH)

    for q in range(1, 4):
        greet(o, rel[q])
    greet(nbp, e)

    @at_inner
    def _():
        greet(other, e)

    xcp.wait()
    wrcp = pltpu.make_async_copy(wr_hbm, wr, lsem.at[1])
    wrcp.start()
    wcp = []
    for j in range(JLOC):
        a = pltpu.make_async_copy(wg_hbm.at[j], wgb.at[j], wsem.at[0, j])
        b = pltpu.make_async_copy(wu_hbm.at[j], wub.at[j], wsem.at[1, j])
        a.start()
        b.start()
        wcp.append((a, b))

    def wd_copy(n):
        return pltpu.make_async_copy(
            wd_hbm.at[:, :, pl.ds((n % NC) * CW, CW)], wdb.at[n % WSLOT], dsem.at[n % WSLOT])

    for n in range(WSLOT):
        wd_copy(n).start()

    @at_end
    def _():
        pl.semaphore_wait(barrier, 4)

    @at_inner
    def _():
        pl.semaphore_wait(barrier, 5)

    def block(col, g, h, direction, oo, ee):
        half, rows = rows_of(col, g, h, HALF)
        cps = [pltpu.make_async_remote_copy(
            src_ref=x_all.at[half, rows], dst_ref=x_all.at[half, rows],
            send_sem=bx_s.at[direction, g, h], recv_sem=bx_r.at[col, planes[g], h],
            device_id=(d, oo, ee), device_id_type=MESH)]
        if h == 0:
            tile = r_all.at[half, col, planes[g] % 2]
            cps.insert(0, pltpu.make_async_remote_copy(
                src_ref=tile, dst_ref=tile,
                send_sem=br_s.at[direction, g], recv_sem=br_r.at[col, planes[g]],
                device_id=(d, oo, ee), device_id_type=MESH))
        return cps

    targets = {OUT: (e, nbp, e), CROSS: (e, other, e), SIDE: (e, o, yp), MATE: (e, o, mate),
               PASS: (yp, o, mate), YOUT: (yp, nbp, e), YCROSS: (yp, other, e)}

    def send(g, h, *directions):
        for direction in directions:
            col, oo, ee = targets[direction]
            for cp in block(col, g, h, direction, oo, ee):
                cp.start()

    def arrive(col, g, h):
        for cp in block(col, g, h, MATE, o, mate):
            cp.wait_recv()

    def sent(g, h, *directions):
        for direction in directions:
            for cp in block(targets[direction][0], g, h, direction, o, mate):
                cp.wait_send()

    def get(g, h, *directions):
        arrive(e, g, h)
        send(g, h, *directions, MATE)

    def yget(g, h, *directions):
        arrive(yp, g, h)
        send(g, h, *directions, PASS)

    @at_end
    def _():
        for h in range(2):
            send(OWN, h, OUT, SIDE, MATE)
        for h in range(2):
            get(NB, h, SIDE)
            yget(OWN, h)
        for h in range(2):
            get(NEAR, h, SIDE)
            yget(NB, h)

    @at_inner
    def _():
        for h in range(2):
            send(OWN, h, OUT, CROSS, SIDE, MATE)
        get(NB, 0, CROSS, SIDE)
        get(NEAR, 0, OUT)
        yget(OWN, 0)
        get(NB, 1, CROSS, SIDE)
        send(OWN, 0, YCROSS)
        get(NEAR, 1, OUT, SIDE)
        yget(OWN, 1)
        get(FAR, 0, OUT)
        yget(NB, 0)
        get(FAR, 1, OUT, SIDE)
        send(FAR, 0, SIDE)
        yget(NB, 1)

    def late_blocks(step):
        if step == 0:
            @at_end
            def _():
                get(FAR, 0, SIDE)
                yget(NEAR, 0)

            @at_inner
            def _():
                yget(NEAR, 0)
                yget(NEAR, 1)
        elif step == 1:
            @at_end
            def _():
                get(FAR, 1)
                yget(NEAR, 1)

            @at_inner
            def _():
                yget(FAR, 1, YOUT)
        else:
            @at_end
            def _():
                yget(FAR, 0)
                yget(FAR, 1)

            @at_inner
            def _():
                yget(FAR, 0)

    def from_mate(g):
        for col in (mate, diag):
            for h in range(2):
                arrive(col, g, h)

    col_i, row_i = iota((CT, CT), 1), iota((CT, CT), 0)
    same = col_i // TOK == row_i // TOK
    before = (same & (row_i < col_i)).astype(BF16)
    after = (same & (col_i < row_i)).astype(BF16)
    eye = (col_i == row_i).astype(BF16)
    low = iota((TOPK, CT), 1) < TOK
    mine = ((o * COLS + e) * JLOC).astype(F32)

    def pick(ps):
        half = halves[ps]
        r = r_all[half]
        routes = jnp.concatenate(
            [jnp.where(low, r[k, 0], r[k, 1]) for k in range(COLS)], axis=1)
        m = [jnp.max((routes == mine + j).astype(F32), axis=0, keepdims=True)
             for j in range(JLOC)]
        m = jnp.concatenate(m + [jnp.zeros((8 - JLOC, HT), F32)], axis=0)
        mb = m.astype(BF16)
        pos = jnp.concatenate(
            [dot(mb[:, k * CT:(k + 1) * CT], before) for k in range(COLS)], axis=1)
        pm = jnp.where(m > 0.5, pos, -1.0)
        ri, ci = iota((MR, HT), 0), iota((MR, HT), 1)
        q = (ri % GR) // CAP
        col = jnp.where(q == 0, rel[0], jnp.where(q == 1, rel[1], jnp.where(q == 2, rel[2], rel[3])))
        par = jnp.where(ri < GR, planes[2 * ps] % 2, planes[2 * ps + 1] % 2)
        want = jnp.where((ci // CT == col) & ((ci // TOK) % 2 == par), ri % CAP, -2).astype(F32)
        sel = jnp.concatenate(
            [(pm[j:j + 1, :] == want).astype(F32) for j in range(JLOC)], axis=0).astype(BF16)
        for n in range(DIM // 512):
            cols = pl.ds(n * 512, 512)
            got = dot(sel, x_all[half, :, cols])
            for j in range(JLOC):
                xs[j, :, cols] = got[j * MR:(j + 1) * MR].astype(BF16)

    def gates(ps):
        half = halves[ps]
        r = r_all[half, e]
        routes = jnp.where(low, r[0], r[1])
        exp_id = iota((NEXP, CT), 0).astype(F32)
        hot = jnp.zeros((NEXP, CT), F32)
        for k in range(TOPK):
            hot = hot + (routes[k:k + 1, :] == exp_id).astype(F32)
        hot = hot.astype(BF16)
        chosen = dot_nt(eye, hot) > 0.5
        pos = jnp.where(chosen, dot_nt(after, hot), -1.0)
        logits = dot_nt(x_all[half, pl.ds(pl.multiple_of(e * CT, CT), CT)], wr[...])
        top = jnp.max(jnp.where(chosen, logits, -jnp.inf), axis=1, keepdims=True)
        ex = jnp.where(chosen, jnp.exp(logits - top), 0.0)
        gate = ex / jnp.sum(ex, axis=1, keepdims=True)
        g1 = gate.astype(BF16)
        rest = gate - g1.astype(F32)
        g2 = rest.astype(BF16)
        g3 = (rest - g2.astype(F32)).astype(BF16)
        pos = pos.astype(BF16)
        slot = (iota((CT, GR), 1) % CAP).astype(F32)
        for q in range(COLS):
            first = (o * COLS + rel[q]) * JLOC
            expand = (iota((NEXP, GR), 0) == first + iota((NEXP, GR), 1) // CAP).astype(BF16)
            hit = dot(pos, expand) == slot
            for k, g in enumerate((g1, g2, g3)):
                w = jnp.where(hit, dot(g, expand), 0.0)
                for i in range(2):
                    par = planes[2 * ps + i] % 2
                    wst[2 * ps + i, q, k * TOK:(k + 1) * TOK, :] = jnp.where(
                        par == 0, w[:TOK], w[TOK:]).astype(BF16)

    def gate_up(ps, j):
        if ps == 0:
            wcp[j][0].wait()
            wcp[j][1].wait()
        for n in range(FF // 512):
            cols = slice(n * 512, (n + 1) * 512)
            ga = dot(xs[j], wgb[j, :, cols])
            gu = dot(xs[j], wub[j, :, cols])
            hid[j, :, cols] = (jax.nn.silu(ga) * gu).astype(BF16)

    def ycopy(g, k, q):
        return pltpu.make_async_remote_copy(
            src_ref=ysend.at[g, k, q - 1], dst_ref=yrecv.at[g, k, q],
            send_sem=ys_s.at[g, k, q - 1], recv_sem=ys_r.at[g, k, q - 1],
            device_id=(d, o, rel[q]), device_id_type=MESH)

    def ystart(g, k):
        for q in (2, 3, 1):
            ycopy(g, k, q).start()

    def down_chunk(ps, k):
        n = ps * NC + k
        wd_copy(n).wait()
        outs = [dot(hid[j], wdb[n % WSLOT, j]) for j in range(JLOC)]
        for i in range(2):
            g = 2 * ps + i
            for q in (2, 3, 1, 0):
                at = i * GR + q * CAP
                rows = jnp.concatenate([r[at:at + CAP] for r in outs], axis=0).astype(BF16)
                if q:
                    ysend[g, k, q - 1] = rows
                else:
                    yrecv[g, k, 0] = rows
            if g != OWN:
                ystart(g, k)
        if n + WSLOT < 2 * NC:
            wd_copy(n + WSLOT).start()

    def zcopy(k, g, slot, oo):
        return pltpu.make_async_remote_copy(
            src_ref=part.at[k, g], dst_ref=zr.at[k, slot],
            send_sem=zs_s.at[k, g], recv_sem=zs_r.at[k, slot],
            device_id=(d, oo, e), device_id_type=MESH)

    def sums(g, k):
        for q in range(1, COLS):
            ycopy(g, k, q).wait_recv()
        acc = dot(wst[g, 0], yrecv[g, k, 0])
        for q in range(1, COLS):
            acc = acc + dot(wst[g, q], yrecv[g, k, q])
        part[k, g] = acc[0:TOK] + acc[TOK:2 * TOK] + acc[2 * TOK:3 * TOK]
        if g != OWN:
            @at_end
            def _():
                zcopy(k, g, {NB: 0, FAR: 1, NEAR: 2}[g], nbp).start()

    def relay(k, g, slot_in, slot_out, oo):
        zcopy(k, g, slot_in, nbp).wait_recv()
        part[k, g] = part[k, g] + zr[k, slot_in]
        zcopy(k, g, slot_out, oo).start()

    def relay_near(k):
        @at_inner
        def _():
            relay(k, FAR, 1, 4, other)
            relay(k, NEAR, 2, 3, other)

    def relay_far(k):
        @at_inner
        def _():
            relay(k, NB, 4, 0, nbp)

    def ocopy(k):
        cols = pl.ds(k * CW, CW)
        return pltpu.make_async_copy(obuf.at[:, cols], out_hbm.at[:, cols], osem.at[k])

    def finish(k):
        cols = pl.ds(k * CW, CW)
        zcopy(k, OWN, 0, nbp).wait_recv()

        @at_end
        def _():
            obuf[:, cols] = (part[k, OWN] + zr[k, 0]).astype(BF16)

        @at_inner
        def _():
            zcopy(k, OWN, 3, nbp).wait_recv()
            obuf[:, cols] = (part[k, OWN] + zr[k, 0] + zr[k, 3]).astype(BF16)

        ocopy(k).start()

    from_mate(OWN)
    from_mate(NB)
    pick(0)
    gate_up(0, 0)
    late_blocks(0)
    gate_up(0, 1)
    gate_up(0, 2)
    late_blocks(1)
    gate_up(0, 3)
    for k in range(3):
        down_chunk(0, k)
    late_blocks(2)
    for k in range(3, NC):
        down_chunk(0, k)
    wrcp.wait()
    gates(0)

    from_mate(NEAR)
    from_mate(FAR)
    pick(1)
    for j in range(JLOC):
        gate_up(1, j)
        sums(NB, 2 * j)
        sums(NB, 2 * j + 1)
    for k in range(NC):
        down_chunk(1, k)
    for k in range(NC):
        ystart(OWN, k)
    gates(1)
    for k in range(NC + 2):
        if k < NC:
            sums(FAR, k)
            sums(NEAR, k)
        if 0 <= k - 1 < NC:
            relay_near(k - 1)
        if k >= 2:
            relay_far(k - 2)
        if 4 <= k < NC:
            sums(OWN, 2 * (k - 4))
            sums(OWN, 2 * (k - 4) + 1)
    for k in range(NC):
        finish(k)
    for k in range(NC):
        ocopy(k).wait()

    for g in range(4):
        for h in range(2):
            sent(g, h, MATE, PASS)

    @at_end
    def _():
        for h in range(2):
            sent(OWN, h, OUT, SIDE)
            sent(NB, h, SIDE)
            sent(NEAR, h, SIDE)
        sent(FAR, 0, SIDE)

    @at_inner
    def _():
        for h in range(2):
            sent(OWN, h, OUT, CROSS, SIDE)
            sent(NB, h, CROSS, SIDE)
            sent(NEAR, h, OUT)
            sent(FAR, h, OUT, SIDE)
        sent(NEAR, 1, SIDE)
        sent(OWN, 0, YCROSS)
        sent(FAR, 1, YOUT)

    for k in range(NC):
        for g in range(4):
            for q in range(1, COLS):
                ycopy(g, k, q).wait_send()
            if g != OWN:
                zcopy(k, g, 0, nbp).wait_send()


def solution(mesh):
    row_spec = P(('data', 'outer', 'expert'), None)
    weight_spec = P(('outer', 'expert'), None, None)
    vmem = pl.BlockSpec(memory_space=pltpu.VMEM)
    anyspace = pl.BlockSpec(memory_space=pl.ANY)
    dma = pltpu.SemaphoreType.DMA

    def per_device(tokens, w_router, routes, w_gate, w_up, w_down):
        return pl.pallas_call(
            kernel,
            name='moe',
            out_shape=jax.ShapeDtypeStruct((TOK, DIM), BF16),
            in_specs=[anyspace, anyspace, vmem, anyspace, anyspace, anyspace],
            out_specs=anyspace,
            scratch_shapes=[
                pltpu.VMEM((2, HT, DIM), BF16),
                pltpu.VMEM((2, COLS, 2, TOPK, 128), F32),
                pltpu.VMEM((NEXP, DIM), BF16),
                pltpu.VMEM((JLOC, MR, DIM), BF16),
                pltpu.VMEM((JLOC, DIM, FF), BF16),
                pltpu.VMEM((JLOC, DIM, FF), BF16),
                pltpu.VMEM((WSLOT, JLOC, FF, CW), BF16),
                pltpu.VMEM((JLOC, MR, FF), BF16),
                pltpu.VMEM((4, NC, COLS - 1, GR, CW), BF16),
                pltpu.VMEM((4, NC, COLS, GR, CW), BF16),
                pltpu.VMEM((4, COLS, 3 * TOK, GR), BF16),
                pltpu.VMEM((NC, 4, TOK, CW), F32),
                pltpu.VMEM((NC, 5, TOK, CW), F32),
                pltpu.VMEM((TOK, DIM), BF16),
                dma((2,)), dma((2, JLOC)), dma((WSLOT,)), dma((NC,)),
                dma((7, 4, 2)), dma((7, 4)),
                dma((COLS, PLANES, 2)), dma((COLS, PLANES)),
                dma((4, NC, COLS - 1)), dma((4, NC, COLS - 1)),
                dma((NC, 4)), dma((NC, 5)),
            ],
            compiler_params=pltpu.CompilerParams(
                collective_id=0, has_side_effects=True, vmem_limit_bytes=67043328),
        )(tokens, w_router.T, routes.T, w_gate, w_up, w_down)

    return jax.shard_map(
        per_device, mesh=mesh,
        in_specs=(row_spec, P(), row_spec, weight_spec, weight_spec, weight_spec),
        out_specs=row_spec, check_vma=False)
```

```python
import jax
import jax.numpy as jnp
from jax import lax
from jax.experimental import pallas as pl
from jax.experimental.pallas import tpu as pltpu
from jax.sharding import PartitionSpec as P

MESH = pl.DeviceIdType.MESH
F32, BF16 = jnp.float32, jnp.bfloat16
PLANES = 4
COLS = 4
JLOC = 4
TOK = 64
TOPK = 8
CAP = 10
DIM = 2048
FF = 1024
NEXP = 64
CW = 256
NC = DIM // CW
HALF = TOK // 2
WSLOT = 6
GR = JLOC * CAP
MR = 2 * COLS * CAP
SW = COLS * GR
CT = 2 * TOK
HT = COLS * CT
NB, OWN, FAR, NEAR = range(4)
OUT, CROSS, SIDE, MATE, PASS, YOUT, YCROSS = range(7)


def iota(shape, dim):
    return lax.broadcasted_iota(jnp.int32, shape, dim)


def dot(a, b):
    return jnp.dot(a, b, preferred_element_type=F32)


def dot_nt(a, b):
    return lax.dot_general(a, b, (((1,), (1,)), ((), ())), preferred_element_type=F32)


def kernel(x_hbm, wr_hbm, rt_ref, wg_hbm, wu_hbm, wd_hbm, out_hbm,
           x_all, r_all, wr, xs, wgb, wub, wdb, hid, ysend, yrecv, wst, part, zr, obuf,
           lsem, wsem, dsem, osem, bx_s, br_s, bx_r, br_r, ys_s, ys_r, zs_s, zs_r):
    d = lax.axis_index('data')
    o = lax.axis_index('outer')
    e = lax.axis_index('expert')
    c = e % 2
    y = e // 2
    mate = e + 1 - 2 * c
    yp = e + 2 - 4 * y
    diag = mate + yp - e
    rel = (e, mate, yp, diag)
    side = o // 2
    nbp = o + 1 - 2 * (o % 2)
    other = PLANES - 1 - o
    planes = (nbp, o, 3 - 3 * side, 2 - side)
    halves = (side, 1 - side)
    end = (o == 0) | (o == PLANES - 1)
    inner = jnp.logical_not(end)

    def at_end(fn):
        pl.when(end)(fn)

    def at_inner(fn):
        pl.when(inner)(fn)

    def rows_of(col, g, h, n):
        p = planes[g]
        start = col * CT + (p % 2) * TOK + h * HALF
        return p // 2, pl.ds(pl.multiple_of(start, HALF), n)

    own_half, own_rows = rows_of(e, OWN, 0, TOK)
    xcp = pltpu.make_async_copy(x_hbm, x_all.at[own_half, own_rows], lsem.at[0])
    xcp.start()

    dup = (iota((TOK, 128), 1) % TOK == iota((TOK, 128), 0)).astype(BF16)
    r_all[side, e, o % 2] = dot(rt_ref[...].astype(F32).astype(BF16), dup)

    barrier = pltpu.get_barrier_semaphore()

    def greet(oo, ee):
        pl.semaphore_signal(barrier, inc=1, device_id=(d, oo, ee), device_id_type=MESH)

    for q in range(1, 4):
        greet(o, rel[q])
    greet(nbp, e)

    @at_inner
    def _():
        greet(other, e)

    xcp.wait()
    wrcp = pltpu.make_async_copy(wr_hbm, wr, lsem.at[1])
    wrcp.start()
    wcp = []
    for j in range(JLOC):
        a = pltpu.make_async_copy(wg_hbm.at[j], wgb.at[j], wsem.at[0, j])
        b = pltpu.make_async_copy(wu_hbm.at[j], wub.at[j], wsem.at[1, j])
        a.start()
        b.start()
        wcp.append((a, b))

    def wd_copy(n):
        return pltpu.make_async_copy(
            wd_hbm.at[:, :, pl.ds((n % NC) * CW, CW)], wdb.at[n % WSLOT], dsem.at[n % WSLOT])

    for n in range(WSLOT):
        wd_copy(n).start()

    @at_end
    def _():
        pl.semaphore_wait(barrier, 4)

    @at_inner
    def _():
        pl.semaphore_wait(barrier, 5)

    def block(col, g, h, direction, oo, ee):
        half, rows = rows_of(col, g, h, HALF)
        cps = [pltpu.make_async_remote_copy(
            src_ref=x_all.at[half, rows], dst_ref=x_all.at[half, rows],
            send_sem=bx_s.at[direction, g, h], recv_sem=bx_r.at[col, planes[g], h],
            device_id=(d, oo, ee), device_id_type=MESH)]
        if h == 0:
            tile = r_all.at[half, col, planes[g] % 2]
            cps.insert(0, pltpu.make_async_remote_copy(
                src_ref=tile, dst_ref=tile,
                send_sem=br_s.at[direction, g], recv_sem=br_r.at[col, planes[g]],
                device_id=(d, oo, ee), device_id_type=MESH))
        return cps

    targets = {OUT: (e, nbp, e), CROSS: (e, other, e), SIDE: (e, o, yp), MATE: (e, o, mate),
               PASS: (yp, o, mate), YOUT: (yp, nbp, e), YCROSS: (yp, other, e)}

    def send(g, h, *directions):
        for direction in directions:
            col, oo, ee = targets[direction]
            for cp in block(col, g, h, direction, oo, ee):
                cp.start()

    def arrive(col, g, h):
        for cp in block(col, g, h, MATE, o, mate):
            cp.wait_recv()

    def sent(g, h, *directions):
        for direction in directions:
            for cp in block(targets[direction][0], g, h, direction, o, mate):
                cp.wait_send()

    def get(g, h, *directions):
        arrive(e, g, h)
        send(g, h, *directions, MATE)

    def yget(g, h, *directions):
        arrive(yp, g, h)
        send(g, h, *directions, PASS)

    @at_end
    def _():
        for h in range(2):
            send(OWN, h, OUT, SIDE, MATE)
        for h in range(2):
            get(NB, h, SIDE)
            yget(OWN, h)
        get(NEAR, 0, SIDE)
        yget(NB, 0)

    @at_inner
    def _():
        for h in range(2):
            send(OWN, h, OUT, CROSS, SIDE, MATE)
        get(NB, 0, CROSS, SIDE)
        get(NEAR, 0, OUT)
        yget(OWN, 0)
        get(NB, 1, CROSS, SIDE)
        send(OWN, 0, YCROSS)
        get(NEAR, 1, OUT, SIDE)
        yget(OWN, 1)
        get(FAR, 0, OUT)
        yget(NB, 0)

    def mid_blocks():
        @at_end
        def _():
            get(NEAR, 1, SIDE)
            yget(NB, 1)

        @at_inner
        def _():
            get(FAR, 1, OUT, SIDE)
            send(FAR, 0, SIDE)
            yget(NB, 1)

    def late_blocks(step):
        if step == 0:
            @at_end
            def _():
                get(FAR, 0, SIDE)
                yget(NEAR, 0)

            @at_inner
            def _():
                yget(NEAR, 0)
                yget(NEAR, 1)
        elif step == 1:
            @at_end
            def _():
                get(FAR, 1)
                yget(NEAR, 1)

            @at_inner
            def _():
                yget(FAR, 1, YOUT)
        else:
            @at_end
            def _():
                yget(FAR, 0)
                yget(FAR, 1)

            @at_inner
            def _():
                yget(FAR, 0)

    def from_mate(g):
        for col in (mate, diag):
            for h in range(2):
                arrive(col, g, h)

    col_i, row_i = iota((CT, CT), 1), iota((CT, CT), 0)
    same = col_i // TOK == row_i // TOK
    before = (same & (row_i < col_i)).astype(BF16)
    after = (same & (col_i < row_i)).astype(BF16)
    eye = (col_i == row_i).astype(BF16)
    low = iota((TOPK, CT), 1) < TOK
    mine = ((o * COLS + e) * JLOC).astype(F32)

    def pick(ps):
        half = halves[ps]
        r = r_all[half]
        routes = jnp.concatenate(
            [jnp.where(low, r[k, 0], r[k, 1]) for k in range(COLS)], axis=1)
        m = [jnp.max((routes == mine + j).astype(F32), axis=0, keepdims=True)
             for j in range(JLOC)]
        m = jnp.concatenate(m + [jnp.zeros((8 - JLOC, HT), F32)], axis=0)
        mb = m.astype(BF16)
        pos = jnp.concatenate(
            [dot(mb[:, k * CT:(k + 1) * CT], before) for k in range(COLS)], axis=1)
        pm = jnp.where(m > 0.5, pos, -1.0)
        ri, ci = iota((MR, HT), 0), iota((MR, HT), 1)
        q = (ri % GR) // CAP
        col = jnp.where(q == 0, rel[0], jnp.where(q == 1, rel[1], jnp.where(q == 2, rel[2], rel[3])))
        par = jnp.where(ri < GR, planes[2 * ps] % 2, planes[2 * ps + 1] % 2)
        want = jnp.where((ci // CT == col) & ((ci // TOK) % 2 == par), ri % CAP, -2).astype(F32)
        sel = jnp.concatenate(
            [(pm[j:j + 1, :] == want).astype(F32) for j in range(JLOC)], axis=0).astype(BF16)
        for n in range(DIM // 512):
            cols = pl.ds(n * 512, 512)
            got = dot(sel, x_all[half, :, cols])
            for j in range(JLOC):
                xs[j, :, cols] = got[j * MR:(j + 1) * MR].astype(BF16)

    def gates(ps):
        half = halves[ps]
        r = r_all[half, e]
        routes = jnp.where(low, r[0], r[1])
        exp_id = iota((NEXP, CT), 0).astype(F32)
        hot = jnp.zeros((NEXP, CT), F32)
        for k in range(TOPK):
            hot = hot + (routes[k:k + 1, :] == exp_id).astype(F32)
        hot = hot.astype(BF16)
        chosen = dot_nt(eye, hot) > 0.5
        pos = jnp.where(chosen, dot_nt(after, hot), -1.0)
        logits = dot_nt(x_all[half, pl.ds(pl.multiple_of(e * CT, CT), CT)], wr[...])
        top = jnp.max(jnp.where(chosen, logits, -jnp.inf), axis=1, keepdims=True)
        ex = jnp.where(chosen, jnp.exp(logits - top), 0.0)
        gate = ex / jnp.sum(ex, axis=1, keepdims=True)
        g1 = gate.astype(BF16)
        rest = gate - g1.astype(F32)
        g2 = rest.astype(BF16)
        g3 = (rest - g2.astype(F32)).astype(BF16)
        pos = pos.astype(BF16)
        slot = (iota((CT, SW), 1) % CAP).astype(F32)
        n_i = iota((NEXP, SW), 1)
        q = n_i // GR
        col = jnp.where(q == 0, rel[0], jnp.where(q == 1, rel[1], jnp.where(q == 2, rel[2], rel[3])))
        expert = (o * COLS + col) * JLOC + (n_i % GR) // CAP
        expand = (iota((NEXP, SW), 0) == expert).astype(BF16)
        hit = dot(pos, expand) == slot
        for k, g in enumerate((g1, g2, g3)):
            w = jnp.where(hit, dot(g, expand), 0.0)
            for i in range(2):
                par = planes[2 * ps + i] % 2
                wst[2 * ps + i, k * TOK:(k + 1) * TOK, :] = jnp.where(
                    par == 0, w[:TOK], w[TOK:]).astype(BF16)

    def gate_up(ps, j):
        if ps == 0:
            wcp[j][0].wait()
            wcp[j][1].wait()
        for n in range(FF // 512):
            cols = slice(n * 512, (n + 1) * 512)
            ga = dot(xs[j], wgb[j, :, cols])
            gu = dot(xs[j], wub[j, :, cols])
            hid[j, :, cols] = (jax.nn.silu(ga) * gu).astype(BF16)

    def ycopy(g, k, q):
        return pltpu.make_async_remote_copy(
            src_ref=ysend.at[g, k, q - 1], dst_ref=yrecv.at[g, k, q],
            send_sem=ys_s.at[g, k, q - 1], recv_sem=ys_r.at[g, k, q - 1],
            device_id=(d, o, rel[q]), device_id_type=MESH)

    def ystart(g, k):
        for q in (2, 3, 1):
            ycopy(g, k, q).start()

    def down_chunk(ps, k):
        n = ps * NC + k
        wd_copy(n).wait()
        outs = [dot(hid[j], wdb[n % WSLOT, j]) for j in range(JLOC)]
        for i in range(2):
            g = 2 * ps + i
            for q in (2, 3, 1, 0):
                at = i * GR + q * CAP
                rows = jnp.concatenate([r[at:at + CAP] for r in outs], axis=0).astype(BF16)
                if q:
                    ysend[g, k, q - 1] = rows
                else:
                    yrecv[g, k, 0] = rows
            if g in (NB, FAR):
                ystart(g, k)
        if n + WSLOT < 2 * NC:
            wd_copy(n + WSLOT).start()

    def zcopy(k, g, slot, oo):
        return pltpu.make_async_remote_copy(
            src_ref=part.at[k, g], dst_ref=zr.at[k, slot],
            send_sem=zs_s.at[k, g], recv_sem=zs_r.at[k, slot],
            device_id=(d, oo, e), device_id_type=MESH)

    def sums(g, *chunks):
        for k in chunks:
            for q in range(1, COLS):
                ycopy(g, k, q).wait_recv()
        for k in chunks:
            acc = dot(wst[g], yrecv[g, k].reshape(SW, CW))
            part[k, g] = acc[0:TOK] + acc[TOK:2 * TOK] + acc[2 * TOK:3 * TOK]
        if g != OWN:
            @at_end
            def _():
                for k in chunks:
                    zcopy(k, g, {NB: 0, FAR: 1, NEAR: 2}[g], nbp).start()

    def relay(k, g, slot_in, slot_out, oo):
        zcopy(k, g, slot_in, nbp).wait_recv()
        part[k, g] = part[k, g] + zr[k, slot_in]
        zcopy(k, g, slot_out, oo).start()

    def relay_far(k):
        @at_inner
        def _():
            relay(k, FAR, 1, 4, other)

    def relay_near(k):
        @at_inner
        def _():
            relay(k, NEAR, 2, 3, other)

    def relay_back(k):
        @at_inner
        def _():
            relay(k, NB, 4, 0, nbp)

    def ocopy(k):
        cols = pl.ds(k * CW, CW)
        return pltpu.make_async_copy(obuf.at[:, cols], out_hbm.at[:, cols], osem.at[k])

    def finish(k):
        cols = pl.ds(k * CW, CW)
        zcopy(k, OWN, 0, nbp).wait_recv()

        @at_end
        def _():
            obuf[:, cols] = (part[k, OWN] + zr[k, 0]).astype(BF16)

        @at_inner
        def _():
            zcopy(k, OWN, 3, nbp).wait_recv()
            obuf[:, cols] = (part[k, OWN] + zr[k, 0] + zr[k, 3]).astype(BF16)

        ocopy(k).start()

    wrcp.wait()
    gates(0)
    mid_blocks()
    from_mate(OWN)
    from_mate(NB)
    pick(0)
    gate_up(0, 0)
    late_blocks(0)
    gate_up(0, 1)
    gate_up(0, 2)
    late_blocks(1)
    gate_up(0, 3)
    for k in range(NC):
        if k == NC - 1:
            late_blocks(2)
        down_chunk(0, k)

    from_mate(NEAR)
    from_mate(FAR)
    pick(1)
    for j in range(JLOC):
        gate_up(1, j)
        sums(NB, 2 * j, 2 * j + 1)
    lead = 4
    for k in range(NC):
        down_chunk(1, k)
        if k == 3:
            gates(1)
        if k >= lead:
            sums(FAR, k - lead)
    for k in range(NC):
        ystart(NEAR, k)
    for k in range(NC):
        ystart(OWN, k)
    for k in range(NC):
        if k + lead < NC:
            sums(FAR, k + lead)
        relay_far(k)
        if k >= 4:
            relay_back(k - 4)
    for k in range(NC):
        sums(NEAR, k)
        if k >= 1:
            relay_near(k - 1)
        if k < 4:
            relay_back(k + 4)
        else:
            sums(OWN, 2 * (k - 4), 2 * (k - 4) + 1)
    relay_near(NC - 1)
    for k in range(NC):
        finish(k)
    for k in range(NC):
        ocopy(k).wait()

    for g in range(4):
        for h in range(2):
            sent(g, h, MATE, PASS)

    @at_end
    def _():
        for h in range(2):
            sent(OWN, h, OUT, SIDE)
            sent(NB, h, SIDE)
            sent(NEAR, h, SIDE)
        sent(FAR, 0, SIDE)

    @at_inner
    def _():
        for h in range(2):
            sent(OWN, h, OUT, CROSS, SIDE)
            sent(NB, h, CROSS, SIDE)
            sent(NEAR, h, OUT)
            sent(FAR, h, OUT, SIDE)
        sent(NEAR, 1, SIDE)
        sent(OWN, 0, YCROSS)
        sent(FAR, 1, YOUT)

    for k in range(NC):
        for g in range(4):
            for q in range(1, COLS):
                ycopy(g, k, q).wait_send()
            if g != OWN:
                zcopy(k, g, 0, nbp).wait_send()


def solution(mesh):
    row_spec = P(('data', 'outer', 'expert'), None)
    weight_spec = P(('outer', 'expert'), None, None)
    vmem = pl.BlockSpec(memory_space=pltpu.VMEM)
    anyspace = pl.BlockSpec(memory_space=pl.ANY)
    dma = pltpu.SemaphoreType.DMA

    def per_device(tokens, w_router, routes, w_gate, w_up, w_down):
        return pl.pallas_call(
            kernel,
            name='moe',
            out_shape=jax.ShapeDtypeStruct((TOK, DIM), BF16),
            in_specs=[anyspace, anyspace, vmem, anyspace, anyspace, anyspace],
            out_specs=anyspace,
            scratch_shapes=[
                pltpu.VMEM((2, HT, DIM), BF16),
                pltpu.VMEM((2, COLS, 2, TOPK, 128), F32),
                pltpu.VMEM((NEXP, DIM), BF16),
                pltpu.VMEM((JLOC, MR, DIM), BF16),
                pltpu.VMEM((JLOC, DIM, FF), BF16),
                pltpu.VMEM((JLOC, DIM, FF), BF16),
                pltpu.VMEM((WSLOT, JLOC, FF, CW), BF16),
                pltpu.VMEM((JLOC, MR, FF), BF16),
                pltpu.VMEM((4, NC, COLS - 1, GR, CW), BF16),
                pltpu.VMEM((4, NC, COLS, GR, CW), BF16),
                pltpu.VMEM((4, 3 * TOK, SW), BF16),
                pltpu.VMEM((NC, 4, TOK, CW), F32),
                pltpu.VMEM((NC, 5, TOK, CW), F32),
                pltpu.VMEM((TOK, DIM), BF16),
                dma((2,)), dma((2, JLOC)), dma((WSLOT,)), dma((NC,)),
                dma((7, 4, 2)), dma((7, 4)),
                dma((COLS, PLANES, 2)), dma((COLS, PLANES)),
                dma((4, NC, COLS - 1)), dma((4, NC, COLS - 1)),
                dma((NC, 4)), dma((NC, 5)),
            ],
            compiler_params=pltpu.CompilerParams(
                collective_id=0, has_side_effects=True, vmem_limit_bytes=67043328),
        )(tokens, w_router.T, routes.T, w_gate, w_up, w_down)

    return jax.shard_map(
        per_device, mesh=mesh,
        in_specs=(row_spec, P(), row_spec, weight_spec, weight_spec, weight_spec),
        out_specs=row_spec, check_vma=False)
```

```python
import jax
import jax.numpy as jnp
from jax import lax
from jax.experimental import pallas as pl
from jax.experimental.pallas import tpu as pltpu
from jax.sharding import PartitionSpec as P

MESH = pl.DeviceIdType.MESH
F32, BF16 = jnp.float32, jnp.bfloat16
PLANES = 4
COLS = 4
JLOC = 4
TOK = 64
TOPK = 8
CAP = 10
DIM = 2048
FF = 1024
NEXP = 64
CW = 256
NC = DIM // CW
DIRECT = 3
WSLOT = 6
GR = JLOC * CAP
MR = 2 * COLS * CAP
SW = COLS * GR
CT = 2 * TOK
HT = COLS * CT
NB, OWN, FAR, NEAR = range(4)
OUT, CROSS, SIDE, MATE, PASS, YCROSS = range(6)


def iota(shape, dim):
    return lax.broadcasted_iota(jnp.int32, shape, dim)


def dot(a, b):
    return jnp.dot(a, b, preferred_element_type=F32)


def dot_nt(a, b):
    return lax.dot_general(a, b, (((1,), (1,)), ((), ())), preferred_element_type=F32)


def kernel(x_hbm, wr_hbm, rt_hbm, wg_hbm, wu_hbm, wd_hbm, out_hbm,
           x_all, r_all, wr, rt, sel, xs, wgb, wub, wdb, hid, ysend, yrecv, wst, part, zr, obuf,
           lsem, wsem, dsem, osem, bx_s, br_s, bx_r, br_r, ys_s, ys_r, zs_s, zs_r):
    d = lax.axis_index('data')
    o = lax.axis_index('outer')
    e = lax.axis_index('expert')
    c = e % 2
    y = e // 2
    mate = e + 1 - 2 * c
    yp = e + 2 - 4 * y
    diag = mate + yp - e
    rel = (e, mate, yp, diag)
    side = o // 2
    nbp = o + 1 - 2 * (o % 2)
    other = PLANES - 1 - o
    planes = (nbp, o, 3 - 3 * side, 2 - side)
    halves = (side, 1 - side)
    end = (o == 0) | (o == PLANES - 1)
    inner = jnp.logical_not(end)

    def at_end(fn):
        pl.when(end)(fn)

    def at_inner(fn):
        pl.when(inner)(fn)

    def rows_of(col, g, i, n):
        p = planes[g]
        start = col * CT + (p % 2) * TOK + i * (TOK // n)
        return p // 2, pl.ds(pl.multiple_of(start, TOK // n), TOK // n)

    own_half, own_rows = rows_of(e, OWN, 0, 1)
    xcp = pltpu.make_async_copy(x_hbm, x_all.at[own_half, own_rows], lsem.at[0])
    xcp.start()
    rtcp = pltpu.make_async_copy(rt_hbm, rt, lsem.at[2])
    rtcp.start()

    barrier = pltpu.get_barrier_semaphore()

    def greet(oo, ee):
        pl.semaphore_signal(barrier, inc=1, device_id=(d, oo, ee), device_id_type=MESH)

    for q in range(1, 4):
        greet(o, rel[q])
    greet(nbp, e)

    @at_end
    def _():
        greet(planes[NEAR], e)

    @at_inner
    def _():
        greet(other, e)
        greet(planes[FAR], e)

    rtcp.wait()
    dup = (iota((TOK, 128), 1) % TOK == iota((TOK, 128), 0)).astype(BF16)
    r_all[side, e, o % 2] = dot(rt[...].astype(F32).astype(BF16), dup)

    xcp.wait()
    wrcp = pltpu.make_async_copy(wr_hbm, wr, lsem.at[1])
    wrcp.start()
    wcp = []
    for j in range(JLOC):
        a = pltpu.make_async_copy(wg_hbm.at[j], wgb.at[j], wsem.at[0, j])
        b = pltpu.make_async_copy(wu_hbm.at[j], wub.at[j], wsem.at[1, j])
        a.start()
        b.start()
        wcp.append((a, b))

    def wd_copy(n):
        return pltpu.make_async_copy(
            wd_hbm.at[:, :, pl.ds((n % NC) * CW, CW)], wdb.at[n % WSLOT], dsem.at[n % WSLOT])

    for n in range(WSLOT):
        wd_copy(n).start()

    @at_end
    def _():
        pl.semaphore_wait(barrier, 5)

    @at_inner
    def _():
        pl.semaphore_wait(barrier, 6)

    def count(g, direction=MATE):
        return 4 if g == FAR or (g, direction) == (NB, CROSS) else 2

    def block(col, g, i, n, direction, oo, ee):
        half, rows = rows_of(col, g, i, n)
        cps = [pltpu.make_async_remote_copy(
            src_ref=x_all.at[half, rows], dst_ref=x_all.at[half, rows],
            send_sem=bx_s.at[direction, g, i], recv_sem=bx_r.at[col, planes[g], i],
            device_id=(d, oo, ee), device_id_type=MESH)]
        if i == 0:
            tile = r_all.at[half, col, planes[g] % 2]
            cps.insert(0, pltpu.make_async_remote_copy(
                src_ref=tile, dst_ref=tile,
                send_sem=br_s.at[direction, g], recv_sem=br_r.at[col, planes[g]],
                device_id=(d, oo, ee), device_id_type=MESH))
        return cps

    targets = {OUT: (e, nbp, e), CROSS: (e, other, e), SIDE: (e, o, yp), MATE: (e, o, mate),
               PASS: (yp, o, mate), YCROSS: (yp, other, e)}

    def pieces(g, i, direction):
        n, base = count(g, direction), count(g)
        return n, range(i * n // base, (i + 1) * n // base)

    def send(g, i, *directions):
        for direction in directions:
            col, oo, ee = targets[direction]
            n, parts = pieces(g, i, direction)
            for k in parts:
                for cp in block(col, g, k, n, direction, oo, ee):
                    cp.start()

    def arrive(col, g, i):
        for cp in block(col, g, i, count(g), MATE, o, mate):
            cp.wait_recv()

    def sent(g, i, *directions):
        for direction in directions:
            n, parts = pieces(g, i, direction)
            for k in parts:
                for cp in block(targets[direction][0], g, k, n, direction, o, mate):
                    cp.wait_send()

    def get(g, i, *directions):
        arrive(e, g, i)
        send(g, i, *directions, MATE)

    def yget(g, i, *directions):
        arrive(yp, g, i)
        send(g, i, *directions, PASS)

    def from_mate(g, i):
        arrive(mate, g, i)
        arrive(diag, g, i)

    def early_blocks():
        @at_end
        def _():
            for h in range(2):
                send(OWN, h, OUT, SIDE, MATE)
            for h in range(2):
                get(NB, h, SIDE)
                yget(OWN, h)
            get(NEAR, 0, SIDE)
            yget(NB, 0)

        @at_inner
        def _():
            for h in range(2):
                send(OWN, h, OUT, CROSS, SIDE, MATE)
            get(NB, 0, CROSS, SIDE)
            get(NEAR, 0, OUT)
            yget(OWN, 0)
            get(NB, 1, CROSS, SIDE)
            send(OWN, 0, YCROSS)
            get(NEAR, 1, OUT, SIDE)
            yget(OWN, 1)
            get(FAR, 0, OUT, SIDE)
            get(FAR, 1, OUT, SIDE)
            yget(NB, 0)

    def mid_blocks():
        @at_end
        def _():
            get(NEAR, 1, SIDE)
            yget(NB, 1)

        @at_inner
        def _():
            get(FAR, 2, OUT, SIDE)
            get(FAR, 3, OUT, SIDE)
            yget(NB, 1)

    zlate = ([(FAR, 0)], [(FAR, 1)], [(FAR, 2)], [(FAR, 3)], [], [], [], [])
    ylate_end = ([], [(NEAR, 0)], [], [(NEAR, 1)], [(FAR, 0)], [(FAR, 1)], [(FAR, 2)], [(FAR, 3)])
    ylate_inner = ([(NEAR, 0)], [(NEAR, 1)], [(FAR, 0), (FAR, 1)], [(FAR, 2)], [(FAR, 3)], [], [], [])

    def late_blocks(step):
        @at_end
        def _():
            for g, i in zlate[step]:
                get(g, i, SIDE)
            for g, i in ylate_end[step]:
                yget(g, i)

        if ylate_inner[step]:
            @at_inner
            def _():
                for g, i in ylate_inner[step]:
                    yget(g, i)

    col_i, row_i = iota((CT, CT), 1), iota((CT, CT), 0)
    same = col_i // TOK == row_i // TOK
    before = (same & (row_i < col_i)).astype(BF16)
    after = (same & (col_i < row_i)).astype(BF16)
    eye = (col_i == row_i).astype(BF16)
    low = iota((TOPK, CT), 1) < TOK
    mine = ((o * COLS + e) * JLOC).astype(F32)

    def choose(ps):
        half = halves[ps]
        r = r_all[half]
        routes = jnp.concatenate(
            [jnp.where(low, r[k, 0], r[k, 1]) for k in range(COLS)], axis=1)
        m = [jnp.max((routes == mine + j).astype(F32), axis=0, keepdims=True)
             for j in range(JLOC)]
        m = jnp.concatenate(m + [jnp.zeros((8 - JLOC, HT), F32)], axis=0)
        mb = m.astype(BF16)
        pos = jnp.concatenate(
            [dot(mb[:, k * CT:(k + 1) * CT], before) for k in range(COLS)], axis=1)
        pm = jnp.where(m > 0.5, pos, -1.0)
        ri, ci = iota((MR, HT), 0), iota((MR, HT), 1)
        q = (ri % GR) // CAP
        col = jnp.where(q == 0, rel[0], jnp.where(q == 1, rel[1], jnp.where(q == 2, rel[2], rel[3])))
        par = jnp.where(ri < GR, planes[2 * ps] % 2, planes[2 * ps + 1] % 2)
        want = jnp.where((ci // CT == col) & ((ci // TOK) % 2 == par), ri % CAP, -2).astype(F32)
        sel[...] = jnp.concatenate(
            [(pm[j:j + 1, :] == want).astype(F32) for j in range(JLOC)], axis=0).astype(BF16)

    def pick(ps):
        for n in range(DIM // 512):
            cols = pl.ds(n * 512, 512)
            got = dot(sel[...], x_all[halves[ps], :, cols])
            for j in range(JLOC):
                xs[j, :, cols] = got[j * MR:(j + 1) * MR].astype(BF16)

    def gates(ps):
        half = halves[ps]
        r = r_all[half, e]
        routes = jnp.where(low, r[0], r[1])
        exp_id = iota((NEXP, CT), 0).astype(F32)
        hot = jnp.zeros((NEXP, CT), F32)
        for k in range(TOPK):
            hot = hot + (routes[k:k + 1, :] == exp_id).astype(F32)
        hot = hot.astype(BF16)
        chosen = dot_nt(eye, hot) > 0.5
        pos = jnp.where(chosen, dot_nt(after, hot), -1.0)
        logits = dot_nt(x_all[half, pl.ds(pl.multiple_of(e * CT, CT), CT)], wr[...])
        top = jnp.max(jnp.where(chosen, logits, -jnp.inf), axis=1, keepdims=True)
        ex = jnp.where(chosen, jnp.exp(logits - top), 0.0)
        gate = ex / jnp.sum(ex, axis=1, keepdims=True)
        g1 = gate.astype(BF16)
        rest = gate - g1.astype(F32)
        g2 = rest.astype(BF16)
        g3 = (rest - g2.astype(F32)).astype(BF16)
        pos = pos.astype(BF16)
        slot = (iota((CT, SW), 1) % CAP).astype(F32)
        n_i = iota((NEXP, SW), 1)
        q = n_i // GR
        col = jnp.where(q == 0, rel[0], jnp.where(q == 1, rel[1], jnp.where(q == 2, rel[2], rel[3])))
        expert = (o * COLS + col) * JLOC + (n_i % GR) // CAP
        expand = (iota((NEXP, SW), 0) == expert).astype(BF16)
        hit = dot(pos, expand) == slot
        for k, g in enumerate((g1, g2, g3)):
            w = jnp.where(hit, dot(g, expand), 0.0)
            for i in range(2):
                par = planes[2 * ps + i] % 2
                wst[2 * ps + i, k * TOK:(k + 1) * TOK, :] = jnp.where(
                    par == 0, w[:TOK], w[TOK:]).astype(BF16)

    def gate_up(ps, j):
        if ps == 0:
            wcp[j][0].wait()
            wcp[j][1].wait()
        for n in range(FF // 512):
            cols = slice(n * 512, (n + 1) * 512)
            ga = dot(xs[j], wgb[j, :, cols])
            gu = dot(xs[j], wub[j, :, cols])
            hid[j, :, cols] = (jax.nn.silu(ga) * gu).astype(BF16)

    def ycopy(g, k, q):
        return pltpu.make_async_remote_copy(
            src_ref=ysend.at[g, k, q - 1], dst_ref=yrecv.at[g, k, q],
            send_sem=ys_s.at[g, k, q - 1], recv_sem=ys_r.at[g, k, q - 1],
            device_id=(d, o, rel[q]), device_id_type=MESH)

    def ystart(g, k):
        for q in (2, 3, 1):
            ycopy(g, k, q).start()

    def down_chunk(ps, k):
        n = ps * NC + k
        wd_copy(n).wait()
        outs = [dot(hid[j], wdb[n % WSLOT, j]) for j in range(JLOC)]
        for i in range(2):
            g = 2 * ps + i
            for q in (2, 3, 1, 0):
                at = i * GR + q * CAP
                rows = jnp.concatenate([r[at:at + CAP] for r in outs], axis=0).astype(BF16)
                if q:
                    ysend[g, k, q - 1] = rows
                else:
                    yrecv[g, k, 0] = rows
        if ps == 0:
            ystart(NB, k)
        if n + WSLOT < 2 * NC:
            wd_copy(n + WSLOT).start()

    def zcopy(k, g, slot, oo):
        return pltpu.make_async_remote_copy(
            src_ref=part.at[k, g], dst_ref=zr.at[k, slot],
            send_sem=zs_s.at[k, g], recv_sem=zs_r.at[k, slot],
            device_id=(d, oo, e), device_id_type=MESH)

    def sums(g, *chunks):
        for k in chunks:
            for q in range(1, COLS):
                ycopy(g, k, q).wait_recv()
        for k in chunks:
            acc = dot(wst[g], yrecv[g, k].reshape(SW, CW))
            part[k, g] = acc[0:TOK] + acc[TOK:2 * TOK] + acc[2 * TOK:3 * TOK]

    def zsend(k, g, slot, oo):
        zcopy(k, g, slot, oo).start()

    def relay(k, g, slot_in, slot_out, oo):
        zcopy(k, g, slot_in, nbp).wait_recv()
        part[k, g] = part[k, g] + zr[k, slot_in]
        zcopy(k, g, slot_out, oo).start()

    def relay_far(k):
        relay(k, FAR, 1, 4, other)

    def relay_near(k):
        relay(k, NEAR, 2, 3, other)

    def relay_back(k):
        relay(k, NB, 4, 0, nbp)

    def ocopy(k):
        cols = pl.ds(k * CW, CW)
        return pltpu.make_async_copy(obuf.at[:, cols], out_hbm.at[:, cols], osem.at[k])

    def finish(k, *slots):
        cols = pl.ds(k * CW, CW)
        total = None
        for slot in slots:
            zcopy(k, OWN, slot, nbp).wait_recv()
        total = part[k, OWN]
        for slot in slots:
            total = total + zr[k, slot]
        obuf[:, cols] = total.astype(BF16)
        ocopy(k).start()

    early_blocks()
    wrcp.wait()
    gates(0)
    from_mate(OWN, 0)
    from_mate(NB, 0)
    choose(0)
    mid_blocks()
    from_mate(OWN, 1)
    from_mate(NB, 1)
    pick(0)
    for j in range(JLOC):
        gate_up(0, j)
        late_blocks(j)
    for k in range(NC):
        down_chunk(0, k)
        if k % 2:
            late_blocks(JLOC + k // 2)

    def sums_nb(*chunks):
        sums(NB, *chunks)

        @at_end
        def _():
            for k in chunks:
                zsend(k, NB, 0, nbp)

    from_mate(NEAR, 0)
    from_mate(NEAR, 1)
    from_mate(FAR, 0)
    choose(1)
    sums_nb(0, 1)
    for i in range(1, 4):
        from_mate(FAR, i)
    pick(1)
    for j in range(JLOC):
        gate_up(1, j)
        if j < JLOC - 1:
            sums_nb(2 * j + 2, 2 * j + 3)

    def sums_far(k):
        sums(FAR, k)
        zsend(k, FAR, 1, nbp)

    lead = 4
    relayed = tuple(range(DIRECT, NC))
    for k in range(NC):
        down_chunk(1, k)
        if k == lead - 1:
            gates(1)

        @at_end
        def _():
            ystart(FAR, k)
            if k >= lead:
                sums_far(k - lead)

        @at_inner
        def _():
            if k < DIRECT:
                ystart(NEAR, k)
            if k == DIRECT - 1:
                for m in range(DIRECT):
                    ystart(FAR, m)
            if k >= DIRECT:
                ystart(FAR, k)
            if lead <= k < lead + DIRECT:
                sums(NEAR, k - lead)
                zsend(k - lead, NEAR, 3, other)

    @at_end
    def _():
        for k in relayed + tuple(range(DIRECT)):
            ystart(NEAR, k)
        for k in range(NC):
            ystart(OWN, k)
        for k in range(lead, NC):
            sums_far(k)
        for k in relayed:
            sums(NEAR, k)
            zsend(k, NEAR, 2, nbp)
        for k in range(DIRECT):
            sums(NEAR, k)
            zsend(k, NEAR, 2, planes[NEAR])
        for k in range(0, NC, 2):
            sums(OWN, k, k + 1)
        for k in range(NC):
            finish(k, 0)

    @at_inner
    def _():
        for k in relayed:
            ystart(NEAR, k)
        for k in range(NC):
            ystart(OWN, k)
        for k in range(NC):
            sums(FAR, k)
            relay_far(k)
            if k >= 4:
                relay_back(k - 4)
        for n, k in enumerate(relayed):
            sums(NEAR, k)
            relay_near(k)
            if n < 4:
                relay_back(n + 4)
            if n >= 1:
                sums(OWN, 2 * n - 2, 2 * n - 1)
        for k in relayed:
            finish(k, 0, 3)
        for k in range(DIRECT):
            finish(k, 0, 3, 2)

    for k in range(NC):
        ocopy(k).wait()

    for g in range(4):
        for i in range(count(g)):
            sent(g, i, MATE, PASS)
            if g != NEAR:
                sent(g, i, SIDE)
    sent(NEAR, 1, SIDE)

    @at_end
    def _():
        sent(NEAR, 0, SIDE)
        for h in range(2):
            sent(OWN, h, OUT)

    @at_inner
    def _():
        for h in range(2):
            sent(OWN, h, OUT, CROSS)
            sent(NB, h, CROSS)
            sent(NEAR, h, OUT)
        for i in range(4):
            sent(FAR, i, OUT)
        sent(OWN, 0, YCROSS)

    for k in range(NC):
        for g in range(4):
            for q in range(1, COLS):
                ycopy(g, k, q).wait_send()
            if g != OWN:
                zcopy(k, g, 0, nbp).wait_send()


def solution(mesh):
    row_spec = P(('data', 'outer', 'expert'), None)
    weight_spec = P(('outer', 'expert'), None, None)
    anyspace = pl.BlockSpec(memory_space=pl.ANY)
    dma = pltpu.SemaphoreType.DMA

    def per_device(tokens, w_router, routes, w_gate, w_up, w_down):
        return pl.pallas_call(
            kernel,
            name='moe',
            out_shape=jax.ShapeDtypeStruct((TOK, DIM), BF16),
            in_specs=[anyspace] * 6,
            out_specs=anyspace,
            scratch_shapes=[
                pltpu.VMEM((2, HT, DIM), BF16),
                pltpu.VMEM((2, COLS, 2, TOPK, 128), F32),
                pltpu.VMEM((NEXP, DIM), BF16),
                pltpu.VMEM((TOPK, TOK), jnp.int32),
                pltpu.VMEM((JLOC * MR, HT), BF16),
                pltpu.VMEM((JLOC, MR, DIM), BF16),
                pltpu.VMEM((JLOC, DIM, FF), BF16),
                pltpu.VMEM((JLOC, DIM, FF), BF16),
                pltpu.VMEM((WSLOT, JLOC, FF, CW), BF16),
                pltpu.VMEM((JLOC, MR, FF), BF16),
                pltpu.VMEM((4, NC, COLS - 1, GR, CW), BF16),
                pltpu.VMEM((4, NC, COLS, GR, CW), BF16),
                pltpu.VMEM((4, 3 * TOK, SW), BF16),
                pltpu.VMEM((NC, 4, TOK, CW), F32),
                pltpu.VMEM((NC, 5, TOK, CW), F32),
                pltpu.VMEM((TOK, DIM), BF16),
                dma((3,)), dma((2, JLOC)), dma((WSLOT,)), dma((NC,)),
                dma((6, 4, 4)), dma((6, 4)),
                dma((COLS, PLANES, 4)), dma((COLS, PLANES)),
                dma((4, NC, COLS - 1)), dma((4, NC, COLS - 1)),
                dma((NC, 4)), dma((NC, 5)),
            ],
            compiler_params=pltpu.CompilerParams(
                collective_id=0, has_side_effects=True, vmem_limit_bytes=67043328),
        )(tokens, w_router.T, routes.T, w_gate, w_up, w_down)

    return jax.shard_map(
        per_device, mesh=mesh,
        in_specs=(row_spec, P(), row_spec, weight_spec, weight_spec, weight_spec),
        out_specs=row_spec, check_vma=False)
```

```python
import jax
import jax.numpy as jnp
from jax import lax
from jax.experimental import pallas as pl
from jax.experimental.pallas import tpu as pltpu
from jax.sharding import PartitionSpec as P

MESH = pl.DeviceIdType.MESH
F32, BF16 = jnp.float32, jnp.bfloat16
PLANES = 4
COLS = 4
JLOC = 4
TOK = 64
TOPK = 8
CAP = 10
DIM = 2048
FF = 1024
NEXP = 64
CW = 256
NC = DIM // CW
DIRECT = 3
WSLOT = 6
GR = JLOC * CAP
MR = 2 * COLS * CAP
SW = COLS * GR
CT = 2 * TOK
HT = COLS * CT
NB, OWN, FAR, NEAR = range(4)
OUT, CROSS, SIDE, MATE, PASS, YCROSS, YOUT = range(7)
ZPART = {NB: 0, FAR: 1, NEAR: 2, OWN: 3}


def iota(shape, dim):
    return lax.broadcasted_iota(jnp.int32, shape, dim)


def dot(a, b):
    return jnp.dot(a, b, preferred_element_type=F32)


def dot_nt(a, b):
    return lax.dot_general(a, b, (((1,), (1,)), ((), ())), preferred_element_type=F32)


def kernel(x_hbm, wr_hbm, rt_hbm, wg_hbm, wu_hbm, wd_hbm, out_hbm,
           x_all, r_all, wr, rt, sel, xs, wgb, wub, wdb, hid, ysend, yrecv, wst, part, zr, obuf,
           lsem, wsem, dsem, osem, bx_s, br_s, bx_r, br_r, mx_r, mr_r, ys_s, ys_r, zs_s, zs_r):
    d = lax.axis_index('data')
    o = lax.axis_index('outer')
    e = lax.axis_index('expert')
    c = e % 2
    y = e // 2
    mate = e + 1 - 2 * c
    yp = e + 2 - 4 * y
    diag = mate + yp - e
    rel = (e, mate, yp, diag)
    side = o // 2
    nbp = o + 1 - 2 * (o % 2)
    other = PLANES - 1 - o
    planes = (nbp, o, 3 - 3 * side, 2 - side)
    halves = (side, 1 - side)
    end = (o == 0) | (o == PLANES - 1)
    inner = jnp.logical_not(end)

    def at_end(fn):
        pl.when(end)(fn)

    def at_inner(fn):
        pl.when(inner)(fn)

    def rows_of(col, g, i, n):
        p = planes[g]
        start = col * CT + (p % 2) * TOK + i * (TOK // n)
        return p // 2, pl.ds(pl.multiple_of(start, TOK // n), TOK // n)

    own_half, own_rows = rows_of(e, OWN, 0, 1)
    xcp = pltpu.make_async_copy(x_hbm, x_all.at[own_half, own_rows], lsem.at[0])
    xcp.start()
    rtcp = pltpu.make_async_copy(rt_hbm, rt, lsem.at[2])
    rtcp.start()

    barrier = pltpu.get_barrier_semaphore()

    def greet(oo, ee):
        pl.semaphore_signal(barrier, inc=1, device_id=(d, oo, ee), device_id_type=MESH)

    for q in range(1, 4):
        greet(o, rel[q])
    greet(nbp, e)

    @at_end
    def _():
        greet(planes[NEAR], e)

    @at_inner
    def _():
        greet(other, e)
        greet(planes[FAR], e)

    rtcp.wait()
    dup = (iota((TOK, 128), 1) % TOK == iota((TOK, 128), 0)).astype(BF16)
    r_all[side, e, o % 2] = dot(rt[...].astype(F32).astype(BF16), dup)

    xcp.wait()
    wrcp = pltpu.make_async_copy(wr_hbm, wr, lsem.at[1])
    wrcp.start()
    wcp = []
    for j in range(JLOC):
        a = pltpu.make_async_copy(wg_hbm.at[j], wgb.at[j], wsem.at[0, j])
        b = pltpu.make_async_copy(wu_hbm.at[j], wub.at[j], wsem.at[1, j])
        a.start()
        b.start()
        wcp.append((a, b))

    def wd_copy(n):
        return pltpu.make_async_copy(
            wd_hbm.at[:, :, pl.ds((n % NC) * CW, CW)], wdb.at[n % WSLOT], dsem.at[n % WSLOT])

    for n in range(WSLOT):
        wd_copy(n).start()

    @at_end
    def _():
        pl.semaphore_wait(barrier, 5)

    @at_inner
    def _():
        pl.semaphore_wait(barrier, 6)

    def count(g, direction=MATE):
        return 4 if g == FAR or (g, direction) == (NB, CROSS) else 2

    targets = {OUT: (e, nbp, e), CROSS: (e, other, e), SIDE: (e, o, yp), MATE: (e, o, mate),
               PASS: (yp, o, mate), YCROSS: (yp, other, e), YOUT: (yp, nbp, e)}

    def block(g, i, n, direction):
        col, oo, ee = targets[direction]
        half, rows = rows_of(col, g, i, n)
        if direction in (MATE, PASS):
            x_sem, r_sem = mx_r.at[planes[g] // 2], mr_r.at[planes[g] // 2]
        else:
            lane = 0 if direction in (OUT, CROSS) else 1
            x_sem, r_sem = bx_r.at[lane, planes[g], i], br_r.at[lane, planes[g]]
        cps = [pltpu.make_async_remote_copy(
            src_ref=x_all.at[half, rows], dst_ref=x_all.at[half, rows],
            send_sem=bx_s.at[direction], recv_sem=x_sem,
            device_id=(d, oo, ee), device_id_type=MESH)]
        if i == 0:
            tile = r_all.at[half, col, planes[g] % 2]
            cps.insert(0, pltpu.make_async_remote_copy(
                src_ref=tile, dst_ref=tile,
                send_sem=br_s.at[direction], recv_sem=r_sem,
                device_id=(d, oo, ee), device_id_type=MESH))
        return cps

    def send(g, i, *directions):
        for direction in directions:
            n, base = count(g, direction), count(g)
            for k in range(i * n // base, (i + 1) * n // base):
                for cp in block(g, k, n, direction):
                    cp.start()

    def arrive(lane, g, i):
        n = count(g)
        half, rows = rows_of((e, yp)[lane], g, i, n)
        piece = x_all.at[half, rows]
        if i == 0:
            tile = r_all.at[half, (e, yp)[lane], planes[g] % 2]
            pltpu.make_async_copy(tile, tile, br_r.at[lane, planes[g]]).wait()
        pltpu.make_async_copy(piece, piece, bx_r.at[lane, planes[g], i]).wait()

    def sent(direction, nrows, ntiles):
        rows = x_all.at[0, pl.ds(0, nrows)]
        pltpu.make_async_copy(rows, rows, bx_s.at[direction]).wait()
        tiles = r_all.at[0, pl.ds(0, ntiles), 0]
        pltpu.make_async_copy(tiles, tiles, br_s.at[direction]).wait()

    def get(g, i, *directions):
        arrive(0, g, i)
        send(g, i, *directions, MATE)

    def yget(g, i, *directions):
        arrive(1, g, i)
        send(g, i, *directions, PASS)

    def routes_from_mate(ps):
        tiles = r_all.at[halves[ps], pl.ds(0, 2)]
        pltpu.make_async_copy(tiles, tiles, mr_r.at[halves[ps]]).wait()

    def rows_from_mate(ps):
        rows = x_all.at[halves[ps], pl.ds(0, 2 * CT)]
        pltpu.make_async_copy(rows, rows, mx_r.at[halves[ps]]).wait()

    def early_blocks():
        @at_end
        def _():
            for h in range(2):
                send(OWN, h, OUT, SIDE, MATE)
            for h in range(2):
                get(NB, h, SIDE)
                yget(OWN, h)
            get(NEAR, 0, SIDE)
            yget(NB, 0)

        @at_inner
        def _():
            for h in range(2):
                send(OWN, h, OUT, CROSS, SIDE, MATE)
            get(NB, 0, CROSS, SIDE)
            get(NEAR, 0, OUT)
            yget(OWN, 0)
            get(NB, 1, CROSS, SIDE)
            send(OWN, 0, YCROSS)
            get(NEAR, 1, OUT, SIDE)
            yget(OWN, 1)
            get(FAR, 0, OUT)
            get(FAR, 1, OUT)
            yget(NB, 0)

    def mid_blocks():
        @at_end
        def _():
            get(NEAR, 1, SIDE)
            yget(NB, 1)

        @at_inner
        def _():
            get(FAR, 2, OUT, SIDE)
            get(FAR, 3, OUT, SIDE)
            send(FAR, 0, SIDE)
            send(FAR, 1, SIDE)
            yget(NB, 1)

    zlate = ([(FAR, 0)], [(FAR, 1)], [(FAR, 2)], [(FAR, 3)], [], [], [], [])
    ylate_end = ([], [(NEAR, 0)], [], [(NEAR, 1)], [(FAR, 0)], [(FAR, 1)], [(FAR, 2)], [(FAR, 3)])
    ylate_inner = ([(NEAR, 0)], [(NEAR, 1), (FAR, 2)], [(FAR, 3)], [(FAR, 0)], [(FAR, 1)], [], [], [])

    def late_blocks(step):
        @at_end
        def _():
            for g, i in zlate[step]:
                if i < 2:
                    get(g, i, SIDE)
                else:
                    get(g, i)
            for g, i in ylate_end[step]:
                yget(g, i)

        if ylate_inner[step]:
            @at_inner
            def _():
                for g, i in ylate_inner[step]:
                    if g == FAR and i >= 2:
                        yget(g, i, YOUT)
                    else:
                        yget(g, i)

    col_i, row_i = iota((CT, CT), 1), iota((CT, CT), 0)
    same = col_i // TOK == row_i // TOK
    before = (same & (row_i < col_i)).astype(BF16)
    after = (same & (col_i < row_i)).astype(BF16)
    eye = (col_i == row_i).astype(BF16)
    low = iota((TOPK, CT), 1) < TOK
    mine = ((o * COLS + e) * JLOC).astype(F32)

    def choose(ps):
        half = halves[ps]
        r = r_all[half]
        routes = jnp.concatenate(
            [jnp.where(low, r[k, 0], r[k, 1]) for k in range(COLS)], axis=1)
        m = [jnp.max((routes == mine + j).astype(F32), axis=0, keepdims=True)
             for j in range(JLOC)]
        m = jnp.concatenate(m + [jnp.zeros((8 - JLOC, HT), F32)], axis=0)
        mb = m.astype(BF16)
        pos = jnp.concatenate(
            [dot(mb[:, k * CT:(k + 1) * CT], before) for k in range(COLS)], axis=1)
        pm = jnp.where(m > 0.5, pos, -1.0)
        ri, ci = iota((MR, HT), 0), iota((MR, HT), 1)
        q = (ri % GR) // CAP
        col = jnp.where(q == 0, rel[0], jnp.where(q == 1, rel[1], jnp.where(q == 2, rel[2], rel[3])))
        par = jnp.where(ri < GR, planes[2 * ps] % 2, planes[2 * ps + 1] % 2)
        want = jnp.where((ci // CT == col) & ((ci // TOK) % 2 == par), ri % CAP, -2).astype(F32)
        sel[...] = jnp.concatenate(
            [(pm[j:j + 1, :] == want).astype(F32) for j in range(JLOC)], axis=0).astype(BF16)

    def pick(ps):
        for n in range(DIM // 512):
            cols = pl.ds(n * 512, 512)
            got = dot(sel[...], x_all[halves[ps], :, cols])
            for j in range(JLOC):
                xs[j, :, cols] = got[j * MR:(j + 1) * MR].astype(BF16)

    def gates(ps):
        half = halves[ps]
        r = r_all[half, e]
        routes = jnp.where(low, r[0], r[1])
        exp_id = iota((NEXP, CT), 0).astype(F32)
        hot = jnp.zeros((NEXP, CT), F32)
        for k in range(TOPK):
            hot = hot + (routes[k:k + 1, :] == exp_id).astype(F32)
        hot = hot.astype(BF16)
        chosen = dot_nt(eye, hot) > 0.5
        pos = jnp.where(chosen, dot_nt(after, hot), -1.0)
        logits = dot_nt(x_all[half, pl.ds(pl.multiple_of(e * CT, CT), CT)], wr[...])
        top = jnp.max(jnp.where(chosen, logits, -jnp.inf), axis=1, keepdims=True)
        ex = jnp.where(chosen, jnp.exp(logits - top), 0.0)
        gate = ex / jnp.sum(ex, axis=1, keepdims=True)
        g1 = gate.astype(BF16)
        rest = gate - g1.astype(F32)
        g2 = rest.astype(BF16)
        g3 = (rest - g2.astype(F32)).astype(BF16)
        pos = pos.astype(BF16)
        slot = (iota((CT, SW), 1) % CAP).astype(F32)
        n_i = iota((NEXP, SW), 1)
        q = n_i // GR
        col = jnp.where(q == 0, rel[0], jnp.where(q == 1, rel[1], jnp.where(q == 2, rel[2], rel[3])))
        expert = (o * COLS + col) * JLOC + (n_i % GR) // CAP
        expand = (iota((NEXP, SW), 0) == expert).astype(BF16)
        hit = dot(pos, expand) == slot
        for k, g in enumerate((g1, g2, g3)):
            w = jnp.where(hit, dot(g, expand), 0.0)
            for i in range(2):
                par = planes[2 * ps + i] % 2
                wst[2 * ps + i, k * TOK:(k + 1) * TOK, :] = jnp.where(
                    par == 0, w[:TOK], w[TOK:]).astype(BF16)

    def gate_up(ps, j):
        if ps == 0:
            wcp[j][0].wait()
            wcp[j][1].wait()
        for n in range(FF // 512):
            cols = slice(n * 512, (n + 1) * 512)
            ga = dot(xs[j], wgb[j, :, cols])
            gu = dot(xs[j], wub[j, :, cols])
            hid[j, :, cols] = (jax.nn.silu(ga) * gu).astype(BF16)

    def ycopy(g, k, q):
        return pltpu.make_async_remote_copy(
            src_ref=ysend.at[g, k, q - 1], dst_ref=yrecv.at[g, k, q],
            send_sem=ys_s, recv_sem=ys_r.at[g, k],
            device_id=(d, o, rel[q]), device_id_type=MESH)

    def ywait(g, k):
        rows = yrecv.at[g, k, pl.ds(1, COLS - 1)]
        pltpu.make_async_copy(rows, rows, ys_r.at[g, k]).wait()

    def ystart(g, k):
        for q in (2, 3, 1):
            ycopy(g, k, q).start()

    def down_chunk(ps, k):
        n = ps * NC + k
        wd_copy(n).wait()
        outs = [dot(hid[j], wdb[n % WSLOT, j]) for j in range(JLOC)]
        for i in range(2):
            g = 2 * ps + i
            for q in (2, 3, 1, 0):
                at = i * GR + q * CAP
                rows = jnp.concatenate([r[at:at + CAP] for r in outs], axis=0).astype(BF16)
                if q:
                    ysend[g, k, q - 1] = rows
                else:
                    yrecv[g, k, 0] = rows
        if ps == 0:
            ystart(NB, k)
        if n + WSLOT < 2 * NC:
            wd_copy(n + WSLOT).start()

    def zcopy(k, g, slot, oo):
        return pltpu.make_async_remote_copy(
            src_ref=part.at[ZPART[g], k], dst_ref=zr.at[k, slot],
            send_sem=zs_s, recv_sem=zs_r.at[k, slot],
            device_id=(d, oo, e), device_id_type=MESH)

    def zwait(k, slot):
        rows = zr.at[k, slot]
        pltpu.make_async_copy(rows, rows, zs_r.at[k, slot]).wait()

    def sums(g, *chunks):
        for k in chunks:
            ywait(g, k)
        for k in chunks:
            acc = dot(wst[g], yrecv[g, k].reshape(SW, CW))
            part[ZPART[g], k] = acc[0:TOK] + acc[TOK:2 * TOK] + acc[2 * TOK:3 * TOK]

    def zsend(k, g, slot, oo):
        zcopy(k, g, slot, oo).start()

    def relay(k, g, slot_in, slot_out, oo):
        zwait(k, slot_in)
        part[ZPART[g], k] = part[ZPART[g], k] + zr[k, slot_in]
        zcopy(k, g, slot_out, oo).start()

    def relay_far(k):
        relay(k, FAR, 1, 4, other)

    def relay_near(k):
        relay(k, NEAR, 2, 3, other)

    def relay_back(k):
        relay(k, NB, 4, 0, nbp)

    def ocopy(k):
        cols = pl.ds(k * CW, CW)
        return pltpu.make_async_copy(obuf.at[:, cols], out_hbm.at[:, cols], osem)

    def finish(k, *slots):
        cols = pl.ds(k * CW, CW)
        for slot in slots:
            zwait(k, slot)
        total = part[ZPART[OWN], k]
        for slot in slots:
            total = total + zr[k, slot]
        obuf[:, cols] = total.astype(BF16)
        ocopy(k).start()

    early_blocks()
    wrcp.wait()
    gates(0)
    routes_from_mate(0)
    choose(0)
    mid_blocks()
    rows_from_mate(0)
    pick(0)
    for j in range(JLOC):
        gate_up(0, j)
        late_blocks(j)
    for k in range(NC):
        down_chunk(0, k)
        if k % 2:
            late_blocks(JLOC + k // 2)

    def sums_nb(*chunks):
        sums(NB, *chunks)

        @at_end
        def _():
            for k in chunks:
                zsend(k, NB, 0, nbp)

    routes_from_mate(1)
    choose(1)
    sums_nb(0, 1)
    rows_from_mate(1)
    pick(1)
    for j in range(JLOC):
        gate_up(1, j)
        if j < JLOC - 1:
            sums_nb(2 * j + 2, 2 * j + 3)

    def sums_far(k):
        sums(FAR, k)
        zsend(k, FAR, 1, nbp)

    lead = 4
    relayed = tuple(range(DIRECT, NC))
    for k in range(NC):
        down_chunk(1, k)
        if k == lead - 1:
            gates(1)

        @at_end
        def _():
            ystart(FAR, k)
            if k >= lead:
                sums_far(k - lead)

        @at_inner
        def _():
            if k < DIRECT:
                ystart(NEAR, k)
            if k == DIRECT - 1:
                for m in range(DIRECT):
                    ystart(FAR, m)
            if k >= DIRECT:
                ystart(FAR, k)
            if lead <= k < lead + DIRECT:
                sums(NEAR, k - lead)
                zsend(k - lead, NEAR, 3, other)

    @at_end
    def _():
        for k in relayed + tuple(range(DIRECT)):
            ystart(NEAR, k)
        for k in range(NC):
            ystart(OWN, k)
        for k in range(lead, NC):
            sums_far(k)
        for k in relayed:
            sums(NEAR, k)
            zsend(k, NEAR, 2, nbp)
        for k in range(DIRECT):
            sums(NEAR, k)
            zsend(k, NEAR, 2, planes[NEAR])
        for k in range(0, NC, 2):
            sums(OWN, k, k + 1)
        for k in range(NC):
            finish(k, 0)

    @at_inner
    def _():
        for k in relayed:
            ystart(NEAR, k)
        for k in range(NC):
            ystart(OWN, k)
        for k in range(NC):
            sums(FAR, k)
            relay_far(k)
            if k >= 4:
                relay_back(k - 4)
        for n, k in enumerate(relayed):
            sums(NEAR, k)
            relay_near(k)
            if n < 4:
                relay_back(n + 4)
            if n >= 1:
                sums(OWN, 2 * n - 2, 2 * n - 1)
        for k in relayed:
            finish(k, 0, 3)
        for k in range(DIRECT):
            finish(k, 0, 3, 2)

    pltpu.make_async_copy(obuf, out_hbm, osem).wait()

    sent(MATE, 4 * TOK, 4)
    sent(PASS, 4 * TOK, 4)

    @at_end
    def _():
        sent(SIDE, 7 * TOK // 2, 4)
        sent(OUT, TOK, 1)

    @at_inner
    def _():
        sent(SIDE, 7 * TOK // 2, 3)
        sent(OUT, 3 * TOK, 3)
        sent(CROSS, 2 * TOK, 2)
        sent(YCROSS, TOK // 2, 1)
        half_rows = x_all.at[0, pl.ds(0, TOK // 2)]
        pltpu.make_async_copy(half_rows, half_rows, bx_s.at[YOUT]).wait()

    pltpu.make_async_copy(ysend, ysend, ys_s).wait()
    moved = part.at[pl.ds(0, 3)]
    pltpu.make_async_copy(moved, moved, zs_s).wait()


def solution(mesh):
    row_spec = P(('data', 'outer', 'expert'), None)
    weight_spec = P(('outer', 'expert'), None, None)
    anyspace = pl.BlockSpec(memory_space=pl.ANY)
    dma = pltpu.SemaphoreType.DMA

    def per_device(tokens, w_router, routes, w_gate, w_up, w_down):
        return pl.pallas_call(
            kernel,
            name='moe',
            out_shape=jax.ShapeDtypeStruct((TOK, DIM), BF16),
            in_specs=[anyspace] * 6,
            out_specs=anyspace,
            scratch_shapes=[
                pltpu.VMEM((2, HT, DIM), BF16),
                pltpu.VMEM((2, COLS, 2, TOPK, 128), F32),
                pltpu.VMEM((NEXP, DIM), BF16),
                pltpu.VMEM((TOPK, TOK), jnp.int32),
                pltpu.VMEM((JLOC * MR, HT), BF16),
                pltpu.VMEM((JLOC, MR, DIM), BF16),
                pltpu.VMEM((JLOC, DIM, FF), BF16),
                pltpu.VMEM((JLOC, DIM, FF), BF16),
                pltpu.VMEM((WSLOT, JLOC, FF, CW), BF16),
                pltpu.VMEM((JLOC, MR, FF), BF16),
                pltpu.VMEM((4, NC, COLS - 1, GR, CW), BF16),
                pltpu.VMEM((4, NC, COLS, GR, CW), BF16),
                pltpu.VMEM((4, 3 * TOK, SW), BF16),
                pltpu.VMEM((4, NC, TOK, CW), F32),
                pltpu.VMEM((NC, 5, TOK, CW), F32),
                pltpu.VMEM((TOK, DIM), BF16),
                dma((3,)), dma((2, JLOC)), dma((WSLOT,)), dma,
                dma((7,)), dma((7,)),
                dma((2, PLANES, 4)), dma((2, PLANES)), dma((2,)), dma((2,)),
                dma, dma((4, NC)), dma, dma((NC, 5)),
            ],
            compiler_params=pltpu.CompilerParams(
                collective_id=0, has_side_effects=True, vmem_limit_bytes=67043328),
        )(tokens, w_router.T, routes.T, w_gate, w_up, w_down)

    return jax.shard_map(
        per_device, mesh=mesh,
        in_specs=(row_spec, P(), row_spec, weight_spec, weight_spec, weight_spec),
        out_specs=row_spec, check_vma=False)
```

```python
import jax
import jax.numpy as jnp
from jax import lax
from jax.experimental import pallas as pl
from jax.experimental.pallas import tpu as pltpu
from jax.sharding import PartitionSpec as P

MESH = pl.DeviceIdType.MESH
F32, BF16 = jnp.float32, jnp.bfloat16
PLANES = 4
COLS = 4
JLOC = 4
TOK = 64
TOPK = 8
CAP = 10
DIM = 2048
FF = 1024
NEXP = 64
CW = 256
NC = DIM // CW
DIRECT = 3
WSLOT = 6
GR = JLOC * CAP
MR = 2 * COLS * CAP
SW = COLS * GR
CT = 2 * TOK
HT = COLS * CT
NB, OWN, FAR, NEAR = range(4)
OUT, CROSS, SIDE, MATE, PASS, YCROSS, YOUT = range(7)
ZPART = {NB: 0, FAR: 1, NEAR: 2, OWN: 3}


def iota(shape, dim):
    return lax.broadcasted_iota(jnp.int32, shape, dim)


def dot(a, b):
    return jnp.dot(a, b, preferred_element_type=F32)


def dot_nt(a, b):
    return lax.dot_general(a, b, (((1,), (1,)), ((), ())), preferred_element_type=F32)


def kernel(x_hbm, wr_hbm, rt_hbm, wg_hbm, wu_hbm, wd_hbm, out_ref,
           x_all, r_all, wr, rt, sel, xs, wgb, wub, wdb, hid, ysend, yrecv, wst, part, zr,
           lsem, wsem, dsem, bx_s, br_s, bx_r, br_r, mx_r, mr_r, ys_s, ys_r, zs_s, zs_r):
    d = lax.axis_index('data')
    o = lax.axis_index('outer')
    e = lax.axis_index('expert')
    c = e % 2
    y = e // 2
    mate = e + 1 - 2 * c
    yp = e + 2 - 4 * y
    diag = mate + yp - e
    rel = (e, mate, yp, diag)
    side = o // 2
    nbp = o + 1 - 2 * (o % 2)
    other = PLANES - 1 - o
    planes = (nbp, o, 3 - 3 * side, 2 - side)
    halves = (side, 1 - side)
    end = (o == 0) | (o == PLANES - 1)
    inner = jnp.logical_not(end)

    def at_end(fn):
        pl.when(end)(fn)

    def at_inner(fn):
        pl.when(inner)(fn)

    def rows_of(col, g, i, n):
        p = planes[g]
        start = col * CT + (p % 2) * TOK + i * (TOK // n)
        return p // 2, pl.ds(pl.multiple_of(start, TOK // n), TOK // n)

    own_half, own_rows = rows_of(e, OWN, 0, 1)
    xcp = pltpu.make_async_copy(x_hbm, x_all.at[own_half, own_rows], lsem.at[0])
    xcp.start()
    rtcp = pltpu.make_async_copy(rt_hbm, rt, lsem.at[2])
    rtcp.start()

    barrier = pltpu.get_barrier_semaphore()

    def greet(oo, ee):
        pl.semaphore_signal(barrier, inc=1, device_id=(d, oo, ee), device_id_type=MESH)

    for q in range(1, 4):
        greet(o, rel[q])
    greet(nbp, e)

    @at_end
    def _():
        greet(planes[NEAR], e)

    @at_inner
    def _():
        greet(other, e)
        greet(planes[FAR], e)

    rtcp.wait()
    dup = (iota((TOK, 128), 1) % TOK == iota((TOK, 128), 0)).astype(BF16)
    r_all[side, e, o % 2] = dot(rt[...].astype(F32).astype(BF16), dup)

    xcp.wait()
    wrcp = pltpu.make_async_copy(wr_hbm, wr, lsem.at[1])
    wrcp.start()
    wcp = []
    for j in range(JLOC):
        a = pltpu.make_async_copy(wg_hbm.at[j], wgb.at[j], wsem.at[0, j])
        b = pltpu.make_async_copy(wu_hbm.at[j], wub.at[j], wsem.at[1, j])
        a.start()
        b.start()
        wcp.append((a, b))

    def wd_copy(n):
        return pltpu.make_async_copy(
            wd_hbm.at[:, :, pl.ds((n % NC) * CW, CW)], wdb.at[n % WSLOT], dsem.at[n % WSLOT])

    for n in range(WSLOT):
        wd_copy(n).start()

    @at_end
    def _():
        pl.semaphore_wait(barrier, 5)

    @at_inner
    def _():
        pl.semaphore_wait(barrier, 6)

    def count(g, direction=MATE):
        return 4 if g == FAR or (g, direction) == (NB, CROSS) else 2

    targets = {OUT: (e, nbp, e), CROSS: (e, other, e), SIDE: (e, o, yp), MATE: (e, o, mate),
               PASS: (yp, o, mate), YCROSS: (yp, other, e), YOUT: (yp, nbp, e)}

    def block(g, i, n, direction):
        col, oo, ee = targets[direction]
        half, rows = rows_of(col, g, i, n)
        if direction in (MATE, PASS):
            x_sem, r_sem = mx_r.at[planes[g] // 2], mr_r.at[planes[g] // 2]
        else:
            lane = 0 if direction in (OUT, CROSS) else 1
            x_sem, r_sem = bx_r.at[lane, planes[g], i], br_r.at[lane, planes[g]]
        cps = [pltpu.make_async_remote_copy(
            src_ref=x_all.at[half, rows], dst_ref=x_all.at[half, rows],
            send_sem=bx_s.at[direction], recv_sem=x_sem,
            device_id=(d, oo, ee), device_id_type=MESH)]
        if i == 0:
            tile = r_all.at[half, col, planes[g] % 2]
            cps.insert(0, pltpu.make_async_remote_copy(
                src_ref=tile, dst_ref=tile,
                send_sem=br_s.at[direction], recv_sem=r_sem,
                device_id=(d, oo, ee), device_id_type=MESH))
        return cps

    def send(g, i, *directions):
        for direction in directions:
            n, base = count(g, direction), count(g)
            for k in range(i * n // base, (i + 1) * n // base):
                for cp in block(g, k, n, direction):
                    cp.start()

    def arrive(lane, g, i):
        n = count(g)
        half, rows = rows_of((e, yp)[lane], g, i, n)
        piece = x_all.at[half, rows]
        if i == 0:
            tile = r_all.at[half, (e, yp)[lane], planes[g] % 2]
            pltpu.make_async_copy(tile, tile, br_r.at[lane, planes[g]]).wait()
        pltpu.make_async_copy(piece, piece, bx_r.at[lane, planes[g], i]).wait()

    def sent(direction, nrows, ntiles):
        rows = x_all.at[0, pl.ds(0, nrows)]
        pltpu.make_async_copy(rows, rows, bx_s.at[direction]).wait()
        tiles = r_all.at[0, pl.ds(0, ntiles), 0]
        pltpu.make_async_copy(tiles, tiles, br_s.at[direction]).wait()

    def get(g, i, *directions):
        arrive(0, g, i)
        send(g, i, *directions, MATE)

    def yget(g, i, *directions):
        arrive(1, g, i)
        send(g, i, *directions, PASS)

    def routes_from_mate(ps):
        tiles = r_all.at[halves[ps], pl.ds(0, 2)]
        pltpu.make_async_copy(tiles, tiles, mr_r.at[halves[ps]]).wait()

    def rows_from_mate(ps):
        rows = x_all.at[halves[ps], pl.ds(0, 2 * CT)]
        pltpu.make_async_copy(rows, rows, mx_r.at[halves[ps]]).wait()

    def early_blocks():
        @at_end
        def _():
            for h in range(2):
                send(OWN, h, OUT, SIDE, MATE)
            for h in range(2):
                get(NB, h, SIDE)
                yget(OWN, h)
            get(NEAR, 0, SIDE)
            yget(NB, 0)

        @at_inner
        def _():
            for h in range(2):
                send(OWN, h, OUT, CROSS, SIDE, MATE)
            get(NB, 0, CROSS, SIDE)
            get(NEAR, 0, OUT)
            yget(OWN, 0)
            get(NB, 1, CROSS, SIDE)
            send(OWN, 0, YCROSS)
            get(NEAR, 1, OUT, SIDE)
            yget(OWN, 1)
            get(FAR, 0, OUT)
            get(FAR, 1, OUT)
            yget(NB, 0)

    def mid_blocks():
        @at_end
        def _():
            get(NEAR, 1, SIDE)
            yget(NB, 1)

        @at_inner
        def _():
            get(FAR, 2, OUT, SIDE)
            get(FAR, 3, OUT, SIDE)
            send(FAR, 0, SIDE)
            send(FAR, 1, SIDE)
            yget(NB, 1)

    zlate = ([(FAR, 0)], [(FAR, 1)], [(FAR, 2)], [(FAR, 3)], [], [], [], [])
    ylate_end = ([], [(NEAR, 0)], [], [(NEAR, 1)], [(FAR, 0)], [(FAR, 1)], [(FAR, 2)], [(FAR, 3)])
    ylate_inner = ([(NEAR, 0)], [(NEAR, 1), (FAR, 2)], [(FAR, 3)], [(FAR, 0)], [(FAR, 1)], [], [], [])

    def late_blocks(step):
        @at_end
        def _():
            for g, i in zlate[step]:
                if i < 2:
                    get(g, i, SIDE)
                else:
                    get(g, i)
            for g, i in ylate_end[step]:
                yget(g, i)

        if ylate_inner[step]:
            @at_inner
            def _():
                for g, i in ylate_inner[step]:
                    if g == FAR and i >= 2:
                        yget(g, i, YOUT)
                    else:
                        yget(g, i)

    col_i, row_i = iota((CT, CT), 1), iota((CT, CT), 0)
    same = col_i // TOK == row_i // TOK
    before = (same & (row_i < col_i)).astype(BF16)
    after = (same & (col_i < row_i)).astype(BF16)
    eye = (col_i == row_i).astype(BF16)
    low = iota((TOPK, CT), 1) < TOK
    mine = ((o * COLS + e) * JLOC).astype(F32)

    def choose(ps):
        half = halves[ps]
        r = r_all[half]
        routes = jnp.concatenate(
            [jnp.where(low, r[k, 0], r[k, 1]) for k in range(COLS)], axis=1)
        m = [jnp.max((routes == mine + j).astype(F32), axis=0, keepdims=True)
             for j in range(JLOC)]
        m = jnp.concatenate(m + [jnp.zeros((8 - JLOC, HT), F32)], axis=0)
        mb = m.astype(BF16)
        pos = jnp.concatenate(
            [dot(mb[:, k * CT:(k + 1) * CT], before) for k in range(COLS)], axis=1)
        pm = jnp.where(m > 0.5, pos, -1.0)
        ri, ci = iota((MR, HT), 0), iota((MR, HT), 1)
        q = (ri % GR) // CAP
        col = jnp.where(q == 0, rel[0], jnp.where(q == 1, rel[1], jnp.where(q == 2, rel[2], rel[3])))
        par = jnp.where(ri < GR, planes[2 * ps] % 2, planes[2 * ps + 1] % 2)
        want = jnp.where((ci // CT == col) & ((ci // TOK) % 2 == par), ri % CAP, -2).astype(F32)
        sel[...] = jnp.concatenate(
            [(pm[j:j + 1, :] == want).astype(F32) for j in range(JLOC)], axis=0).astype(BF16)

    def pick(ps):
        for n in range(DIM // 512):
            cols = pl.ds(n * 512, 512)
            got = dot(sel[...], x_all[halves[ps], :, cols])
            for j in range(JLOC):
                xs[j, :, cols] = got[j * MR:(j + 1) * MR].astype(BF16)

    def gates(ps):
        half = halves[ps]
        r = r_all[half, e]
        routes = jnp.where(low, r[0], r[1])
        exp_id = iota((NEXP, CT), 0).astype(F32)
        hot = jnp.zeros((NEXP, CT), F32)
        for k in range(TOPK):
            hot = hot + (routes[k:k + 1, :] == exp_id).astype(F32)
        hot = hot.astype(BF16)
        chosen = dot_nt(eye, hot) > 0.5
        pos = jnp.where(chosen, dot_nt(after, hot), -1.0)
        logits = dot_nt(x_all[half, pl.ds(pl.multiple_of(e * CT, CT), CT)], wr[...])
        top = jnp.max(jnp.where(chosen, logits, -jnp.inf), axis=1, keepdims=True)
        ex = jnp.where(chosen, jnp.exp(logits - top), 0.0)
        gate = ex / jnp.sum(ex, axis=1, keepdims=True)
        g1 = gate.astype(BF16)
        rest = gate - g1.astype(F32)
        g2 = rest.astype(BF16)
        g3 = (rest - g2.astype(F32)).astype(BF16)
        pos = pos.astype(BF16)
        slot = (iota((CT, SW), 1) % CAP).astype(F32)
        n_i = iota((NEXP, SW), 1)
        q = n_i // GR
        col = jnp.where(q == 0, rel[0], jnp.where(q == 1, rel[1], jnp.where(q == 2, rel[2], rel[3])))
        expert = (o * COLS + col) * JLOC + (n_i % GR) // CAP
        expand = (iota((NEXP, SW), 0) == expert).astype(BF16)
        hit = dot(pos, expand) == slot
        for k, g in enumerate((g1, g2, g3)):
            w = jnp.where(hit, dot(g, expand), 0.0)
            for i in range(2):
                par = planes[2 * ps + i] % 2
                wst[2 * ps + i, k * TOK:(k + 1) * TOK, :] = jnp.where(
                    par == 0, w[:TOK], w[TOK:]).astype(BF16)

    def gate_up(ps, j):
        if ps == 0:
            wcp[j][0].wait()
            wcp[j][1].wait()
        for n in range(FF // 512):
            cols = slice(n * 512, (n + 1) * 512)
            ga = dot(xs[j], wgb[j, :, cols])
            gu = dot(xs[j], wub[j, :, cols])
            hid[j, :, cols] = (jax.nn.silu(ga) * gu).astype(BF16)

    def ycopy(g, k, q):
        return pltpu.make_async_remote_copy(
            src_ref=ysend.at[g, k, q - 1], dst_ref=yrecv.at[g, k, q],
            send_sem=ys_s, recv_sem=ys_r.at[g, k],
            device_id=(d, o, rel[q]), device_id_type=MESH)

    def ywait(g, k):
        rows = yrecv.at[g, k, pl.ds(1, COLS - 1)]
        pltpu.make_async_copy(rows, rows, ys_r.at[g, k]).wait()

    def ystart(g, k):
        for q in (2, 3, 1):
            ycopy(g, k, q).start()

    def down_chunk(ps, k):
        n = ps * NC + k
        wd_copy(n).wait()
        outs = [dot(hid[j], wdb[n % WSLOT, j]) for j in range(JLOC)]
        for i in range(2):
            g = 2 * ps + i
            for q in (2, 3, 1, 0):
                at = i * GR + q * CAP
                rows = jnp.concatenate([r[at:at + CAP] for r in outs], axis=0).astype(BF16)
                if q:
                    ysend[g, k, q - 1] = rows
                else:
                    yrecv[g, k, 0] = rows
        if ps == 0:
            ystart(NB, k)
        if n + WSLOT < 2 * NC:
            wd_copy(n + WSLOT).start()

    def zcopy(k, g, slot, oo):
        return pltpu.make_async_remote_copy(
            src_ref=part.at[ZPART[g], k], dst_ref=zr.at[k, slot],
            send_sem=zs_s, recv_sem=zs_r.at[k, slot],
            device_id=(d, oo, e), device_id_type=MESH)

    def zwait(k, slot):
        rows = zr.at[k, slot]
        pltpu.make_async_copy(rows, rows, zs_r.at[k, slot]).wait()

    def sums(g, *chunks):
        for k in chunks:
            ywait(g, k)
        for k in chunks:
            acc = dot(wst[g], yrecv[g, k].reshape(SW, CW))
            part[ZPART[g], k] = acc[0:TOK] + acc[TOK:2 * TOK] + acc[2 * TOK:3 * TOK]

    def zsend(k, g, slot, oo):
        zcopy(k, g, slot, oo).start()

    def relay(k, g, slot_in, slot_out, oo):
        zwait(k, slot_in)
        part[ZPART[g], k] = part[ZPART[g], k] + zr[k, slot_in]
        zcopy(k, g, slot_out, oo).start()

    def relay_far(k):
        relay(k, FAR, 1, 4, other)

    def relay_near(k):
        relay(k, NEAR, 2, 3, other)

    def relay_back(k):
        relay(k, NB, 4, 0, nbp)

    def finish(k, *slots):
        cols = pl.ds(k * CW, CW)
        for slot in slots:
            zwait(k, slot)
        total = part[ZPART[OWN], k]
        for slot in slots:
            total = total + zr[k, slot]
        out_ref[:, cols] = total.astype(BF16)

    early_blocks()
    wrcp.wait()
    gates(0)
    routes_from_mate(0)
    choose(0)
    mid_blocks()
    rows_from_mate(0)
    pick(0)
    for j in range(JLOC):
        gate_up(0, j)
        late_blocks(j)
    for k in range(NC):
        down_chunk(0, k)
        if k % 2:
            late_blocks(JLOC + k // 2)

    def sums_nb(*chunks):
        sums(NB, *chunks)

        @at_end
        def _():
            for k in chunks:
                zsend(k, NB, 0, nbp)

    routes_from_mate(1)
    choose(1)
    rows_from_mate(1)
    pick(1)
    for j in range(JLOC):
        gate_up(1, j)
        if j < JLOC - 1:
            sums_nb(2 * j, 2 * j + 1)

    def sums_far(k):
        sums(FAR, k)
        zsend(k, FAR, 1, nbp)

    lead = 4
    relayed = tuple(range(DIRECT, NC))
    for k in range(NC):
        down_chunk(1, k)
        if k == lead - 1:
            gates(1)

        @at_end
        def _():
            ystart(FAR, k)
            if k >= lead:
                sums_far(k - lead)

        @at_inner
        def _():
            if k < DIRECT:
                ystart(NEAR, k)
            if k == DIRECT - 1:
                for m in range(DIRECT):
                    ystart(FAR, m)
            if k >= DIRECT:
                ystart(FAR, k)
            if lead <= k < lead + DIRECT:
                sums(NEAR, k - lead)
                zsend(k - lead, NEAR, 3, other)

    @at_end
    def _():
        for k in relayed + tuple(range(DIRECT)):
            ystart(NEAR, k)
        for k in range(NC):
            ystart(OWN, k)
        for k in range(lead, NC):
            sums_far(k)
        for k in relayed:
            sums(NEAR, k)
            zsend(k, NEAR, 2, nbp)
        for k in range(DIRECT):
            sums(NEAR, k)
            zsend(k, NEAR, 2, planes[NEAR])
        sums(NB, NC - 2, NC - 1)
        for k in (NC - 2, NC - 1):
            zsend(k, NB, 0, nbp)
        for k in range(0, NC, 2):
            sums(OWN, k, k + 1)
        for k in range(NC):
            finish(k, 0)

    @at_inner
    def _():
        for k in relayed:
            ystart(NEAR, k)
        for k in range(NC):
            ystart(OWN, k)
        for k in range(NC):
            sums(FAR, k)
            relay_far(k)
            if k == 0:
                sums(NB, NC - 2, NC - 1)
            if k >= 4:
                relay_back(k - 4)
        for n, k in enumerate(relayed):
            sums(NEAR, k)
            relay_near(k)
            if n < 4:
                relay_back(n + 4)
            if n >= 1:
                sums(OWN, 2 * n - 2, 2 * n - 1)
        for k in relayed[:-2]:
            finish(k, 0, 3)
        for k in range(DIRECT):
            finish(k, 0, 3, 2)
        for k in relayed[-2:]:
            finish(k, 0, 3)


    sent(MATE, 4 * TOK, 4)
    sent(PASS, 4 * TOK, 4)

    @at_end
    def _():
        sent(SIDE, 7 * TOK // 2, 4)
        sent(OUT, TOK, 1)

    @at_inner
    def _():
        sent(SIDE, 7 * TOK // 2, 3)
        sent(OUT, 3 * TOK, 3)
        sent(CROSS, 2 * TOK, 2)
        sent(YCROSS, TOK // 2, 1)
        half_rows = x_all.at[0, pl.ds(0, TOK // 2)]
        pltpu.make_async_copy(half_rows, half_rows, bx_s.at[YOUT]).wait()

    pltpu.make_async_copy(ysend, ysend, ys_s).wait()
    moved = part.at[pl.ds(0, 3)]
    pltpu.make_async_copy(moved, moved, zs_s).wait()


def solution(mesh):
    row_spec = P(('data', 'outer', 'expert'), None)
    weight_spec = P(('outer', 'expert'), None, None)
    anyspace = pl.BlockSpec(memory_space=pl.ANY)
    dma = pltpu.SemaphoreType.DMA

    def per_device(tokens, w_router, routes, w_gate, w_up, w_down):
        return pl.pallas_call(
            kernel,
            name='moe',
            out_shape=pltpu.VMEM((TOK, DIM), BF16),
            in_specs=[anyspace] * 6,
            out_specs=pl.BlockSpec(memory_space=pltpu.VMEM),
            scratch_shapes=[
                pltpu.VMEM((2, HT, DIM), BF16),
                pltpu.VMEM((2, COLS, 2, TOPK, 128), F32),
                pltpu.VMEM((NEXP, DIM), BF16),
                pltpu.VMEM((TOPK, TOK), jnp.int32),
                pltpu.VMEM((JLOC * MR, HT), BF16),
                pltpu.VMEM((JLOC, MR, DIM), BF16),
                pltpu.VMEM((JLOC, DIM, FF), BF16),
                pltpu.VMEM((JLOC, DIM, FF), BF16),
                pltpu.VMEM((WSLOT, JLOC, FF, CW), BF16),
                pltpu.VMEM((JLOC, MR, FF), BF16),
                pltpu.VMEM((4, NC, COLS - 1, GR, CW), BF16),
                pltpu.VMEM((4, NC, COLS, GR, CW), BF16),
                pltpu.VMEM((4, 3 * TOK, SW), BF16),
                pltpu.VMEM((4, NC, TOK, CW), F32),
                pltpu.VMEM((NC, 5, TOK, CW), F32),
                dma((3,)), dma((2, JLOC)), dma((WSLOT,)),
                dma((7,)), dma((7,)),
                dma((2, PLANES, 4)), dma((2, PLANES)), dma((2,)), dma((2,)),
                dma, dma((4, NC)), dma, dma((NC, 5)),
            ],
            compiler_params=pltpu.CompilerParams(
                collective_id=0, has_side_effects=True, vmem_limit_bytes=67043328 - (1 << 20)),
        )(tokens, w_router.T, routes.T, w_gate, w_up, w_down)

    return jax.shard_map(
        per_device, mesh=mesh,
        in_specs=(row_spec, P(), row_spec, weight_spec, weight_spec, weight_spec),
        out_specs=row_spec, check_vma=False)
```

```python
import jax
import jax.numpy as jnp
from jax import lax
from jax.experimental import pallas as pl
from jax.experimental.pallas import tpu as pltpu
from jax.sharding import PartitionSpec as P

MESH = pl.DeviceIdType.MESH
F32, BF16 = jnp.float32, jnp.bfloat16
PLANES = 4
COLS = 4
JLOC = 4
TOK = 64
TOPK = 8
CAP = 10
DIM = 2048
FF = 1024
NEXP = 64
CW = 256
NC = DIM // CW
DIRECT = 3
WSLOT = 6
GR = JLOC * CAP
MR = 2 * COLS * CAP
SW = COLS * GR
CT = 2 * TOK
HT = COLS * CT
NB, OWN, FAR, NEAR = range(4)
OUT, CROSS, SIDE, MATE, PASS, YCROSS, YOUT = range(7)
ZPART = {NB: 0, FAR: 1, NEAR: 2, OWN: 3}


def iota(shape, dim):
    return lax.broadcasted_iota(jnp.int32, shape, dim)


def dot(a, b):
    return jnp.dot(a, b, preferred_element_type=F32)


def dot_nt(a, b):
    return lax.dot_general(a, b, (((1,), (1,)), ((), ())), preferred_element_type=F32)


def kernel(x_hbm, wr_hbm, rt_hbm, wg_hbm, wu_hbm, wd_hbm, out_ref,
           x_all, r_all, wr, rt, sel, xs, wgb, wub, wdb, hid, ysend, yrecv, wst, part, zr,
           lsem, wsem, dsem, bx_s, br_s, bx_r, br_r, mx_r, mr_r, ys_s, ys_r, zs_s, zs_r, zh_r):
    d = lax.axis_index('data')
    o = lax.axis_index('outer')
    e = lax.axis_index('expert')
    c = e % 2
    y = e // 2
    mate = e + 1 - 2 * c
    yp = e + 2 - 4 * y
    diag = mate + yp - e
    rel = (e, mate, yp, diag)
    side = o // 2
    nbp = o + 1 - 2 * (o % 2)
    other = PLANES - 1 - o
    planes = (nbp, o, 3 - 3 * side, 2 - side)
    halves = (side, 1 - side)
    end = (o == 0) | (o == PLANES - 1)
    inner = jnp.logical_not(end)

    def at_end(fn):
        pl.when(end)(fn)

    def at_inner(fn):
        pl.when(inner)(fn)

    def rows_of(col, g, i, n):
        p = planes[g]
        start = col * CT + (p % 2) * TOK + i * (TOK // n)
        return p // 2, pl.ds(pl.multiple_of(start, TOK // n), TOK // n)

    own_half, own_rows = rows_of(e, OWN, 0, 1)
    xcp = pltpu.make_async_copy(x_hbm, x_all.at[own_half, own_rows], lsem.at[0])
    xcp.start()
    rtcp = pltpu.make_async_copy(rt_hbm, rt, lsem.at[2])
    rtcp.start()

    barrier = pltpu.get_barrier_semaphore()

    def greet(oo, ee):
        pl.semaphore_signal(barrier, inc=1, device_id=(d, oo, ee), device_id_type=MESH)

    for q in range(1, 4):
        greet(o, rel[q])
    greet(nbp, e)

    @at_end
    def _():
        greet(planes[NEAR], e)

    @at_inner
    def _():
        greet(other, e)
        greet(planes[FAR], e)

    rtcp.wait()
    dup = (iota((TOK, 128), 1) % TOK == iota((TOK, 128), 0)).astype(BF16)
    r_all[side, e, o % 2] = dot(rt[...].astype(F32).astype(BF16), dup)

    xcp.wait()
    wrcp = pltpu.make_async_copy(wr_hbm, wr, lsem.at[1])
    wrcp.start()
    wcp = []
    for j in range(JLOC):
        a = pltpu.make_async_copy(wg_hbm.at[j], wgb.at[j], wsem.at[0, j])
        b = pltpu.make_async_copy(wu_hbm.at[j], wub.at[j], wsem.at[1, j])
        a.start()
        b.start()
        wcp.append((a, b))

    def wd_copy(n):
        return pltpu.make_async_copy(
            wd_hbm.at[:, :, pl.ds((n % NC) * CW, CW)], wdb.at[n % WSLOT], dsem.at[n % WSLOT])

    for n in range(WSLOT):
        wd_copy(n).start()

    @at_end
    def _():
        pl.semaphore_wait(barrier, 5)

    @at_inner
    def _():
        pl.semaphore_wait(barrier, 6)

    def count(g, direction=MATE):
        return 4 if g == FAR or (g, direction) == (NB, CROSS) else 2

    targets = {OUT: (e, nbp, e), CROSS: (e, other, e), SIDE: (e, o, yp), MATE: (e, o, mate),
               PASS: (yp, o, mate), YCROSS: (yp, other, e), YOUT: (yp, nbp, e)}

    def block(g, i, n, direction):
        col, oo, ee = targets[direction]
        half, rows = rows_of(col, g, i, n)
        if direction in (MATE, PASS):
            x_sem, r_sem = mx_r.at[planes[g] // 2], mr_r.at[planes[g] // 2]
        else:
            lane = 0 if direction in (OUT, CROSS) else 1
            x_sem, r_sem = bx_r.at[lane, planes[g], i], br_r.at[lane, planes[g]]
        cps = [pltpu.make_async_remote_copy(
            src_ref=x_all.at[half, rows], dst_ref=x_all.at[half, rows],
            send_sem=bx_s.at[direction], recv_sem=x_sem,
            device_id=(d, oo, ee), device_id_type=MESH)]
        if i == 0:
            tile = r_all.at[half, col, planes[g] % 2]
            cps.insert(0, pltpu.make_async_remote_copy(
                src_ref=tile, dst_ref=tile,
                send_sem=br_s.at[direction], recv_sem=r_sem,
                device_id=(d, oo, ee), device_id_type=MESH))
        return cps

    def send(g, i, *directions):
        for direction in directions:
            n, base = count(g, direction), count(g)
            for k in range(i * n // base, (i + 1) * n // base):
                for cp in block(g, k, n, direction):
                    cp.start()

    def arrive(lane, g, i):
        n = count(g)
        half, rows = rows_of((e, yp)[lane], g, i, n)
        piece = x_all.at[half, rows]
        if i == 0:
            tile = r_all.at[half, (e, yp)[lane], planes[g] % 2]
            pltpu.make_async_copy(tile, tile, br_r.at[lane, planes[g]]).wait()
        pltpu.make_async_copy(piece, piece, bx_r.at[lane, planes[g], i]).wait()

    def sent(direction, nrows, ntiles):
        rows = x_all.at[0, pl.ds(0, nrows)]
        pltpu.make_async_copy(rows, rows, bx_s.at[direction]).wait()
        tiles = r_all.at[0, pl.ds(0, ntiles), 0]
        pltpu.make_async_copy(tiles, tiles, br_s.at[direction]).wait()

    def get(g, i, *directions):
        arrive(0, g, i)
        send(g, i, *directions, MATE)

    def yget(g, i, *directions):
        arrive(1, g, i)
        send(g, i, *directions, PASS)

    def routes_from_mate(ps):
        tiles = r_all.at[halves[ps], pl.ds(0, 2)]
        pltpu.make_async_copy(tiles, tiles, mr_r.at[halves[ps]]).wait()

    def rows_from_mate(ps):
        rows = x_all.at[halves[ps], pl.ds(0, 2 * CT)]
        pltpu.make_async_copy(rows, rows, mx_r.at[halves[ps]]).wait()

    def early_blocks():
        @at_end
        def _():
            for h in range(2):
                send(OWN, h, OUT, SIDE, MATE)
            for h in range(2):
                get(NB, h, SIDE)
                yget(OWN, h)
            get(NEAR, 0, SIDE)
            yget(NB, 0)

        @at_inner
        def _():
            for h in range(2):
                send(OWN, h, OUT, CROSS, SIDE, MATE)
            get(NB, 0, CROSS, SIDE)
            get(NEAR, 0, OUT)
            yget(OWN, 0)
            get(NB, 1, CROSS, SIDE)
            send(OWN, 0, YCROSS)
            get(NEAR, 1, OUT, SIDE)
            yget(OWN, 1)
            get(FAR, 0, OUT)
            get(FAR, 1, OUT)
            yget(NB, 0)

    def mid_blocks():
        @at_end
        def _():
            get(NEAR, 1, SIDE)
            yget(NB, 1)

        @at_inner
        def _():
            get(FAR, 2, OUT, SIDE)
            get(FAR, 3, OUT, SIDE)
            send(FAR, 0, SIDE)
            send(FAR, 1, SIDE)
            yget(NB, 1)

    zlate = ([(FAR, 0)], [(FAR, 1)], [(FAR, 2)], [(FAR, 3)], [], [], [], [])
    ylate_end = ([], [(NEAR, 0)], [], [(NEAR, 1)], [(FAR, 0)], [(FAR, 1)], [(FAR, 2)], [(FAR, 3)])
    ylate_inner = ([(NEAR, 0)], [(NEAR, 1), (FAR, 2)], [(FAR, 3)], [(FAR, 0)], [(FAR, 1)], [], [], [])

    def late_blocks(step):
        @at_end
        def _():
            for g, i in zlate[step]:
                if i < 2:
                    get(g, i, SIDE)
                else:
                    get(g, i)
            for g, i in ylate_end[step]:
                yget(g, i)

        if ylate_inner[step]:
            @at_inner
            def _():
                for g, i in ylate_inner[step]:
                    if g == FAR and i >= 2:
                        yget(g, i, YOUT)
                    else:
                        yget(g, i)

    col_i, row_i = iota((CT, CT), 1), iota((CT, CT), 0)
    same = col_i // TOK == row_i // TOK
    before = (same & (row_i < col_i)).astype(BF16)
    after = (same & (col_i < row_i)).astype(BF16)
    eye = (col_i == row_i).astype(BF16)
    low = iota((TOPK, CT), 1) < TOK
    mine = ((o * COLS + e) * JLOC).astype(F32)

    def choose(ps):
        half = halves[ps]
        r = r_all[half]
        routes = jnp.concatenate(
            [jnp.where(low, r[k, 0], r[k, 1]) for k in range(COLS)], axis=1)
        m = [jnp.max((routes == mine + j).astype(F32), axis=0, keepdims=True)
             for j in range(JLOC)]
        m = jnp.concatenate(m + [jnp.zeros((8 - JLOC, HT), F32)], axis=0)
        mb = m.astype(BF16)
        pos = jnp.concatenate(
            [dot(mb[:, k * CT:(k + 1) * CT], before) for k in range(COLS)], axis=1)
        pm = jnp.where(m > 0.5, pos, -1.0)
        ri, ci = iota((MR, HT), 0), iota((MR, HT), 1)
        q = (ri % GR) // CAP
        col = jnp.where(q == 0, rel[0], jnp.where(q == 1, rel[1], jnp.where(q == 2, rel[2], rel[3])))
        par = jnp.where(ri < GR, planes[2 * ps] % 2, planes[2 * ps + 1] % 2)
        want = jnp.where((ci // CT == col) & ((ci // TOK) % 2 == par), ri % CAP, -2).astype(F32)
        sel[...] = jnp.concatenate(
            [(pm[j:j + 1, :] == want).astype(F32) for j in range(JLOC)], axis=0).astype(BF16)

    def pick(ps):
        for n in range(DIM // 512):
            cols = pl.ds(n * 512, 512)
            got = dot(sel[...], x_all[halves[ps], :, cols])
            for j in range(JLOC):
                xs[j, :, cols] = got[j * MR:(j + 1) * MR].astype(BF16)

    def gates(ps):
        half = halves[ps]
        r = r_all[half, e]
        routes = jnp.where(low, r[0], r[1])
        exp_id = iota((NEXP, CT), 0).astype(F32)
        hot = jnp.zeros((NEXP, CT), F32)
        for k in range(TOPK):
            hot = hot + (routes[k:k + 1, :] == exp_id).astype(F32)
        hot = hot.astype(BF16)
        chosen = dot_nt(eye, hot) > 0.5
        pos = jnp.where(chosen, dot_nt(after, hot), -1.0)
        logits = dot_nt(x_all[half, pl.ds(pl.multiple_of(e * CT, CT), CT)], wr[...])
        top = jnp.max(jnp.where(chosen, logits, -jnp.inf), axis=1, keepdims=True)
        ex = jnp.where(chosen, jnp.exp(logits - top), 0.0)
        gate = ex / jnp.sum(ex, axis=1, keepdims=True)
        g1 = gate.astype(BF16)
        rest = gate - g1.astype(F32)
        g2 = rest.astype(BF16)
        g3 = (rest - g2.astype(F32)).astype(BF16)
        pos = pos.astype(BF16)
        slot = (iota((CT, SW), 1) % CAP).astype(F32)
        n_i = iota((NEXP, SW), 1)
        q = n_i // GR
        col = jnp.where(q == 0, rel[0], jnp.where(q == 1, rel[1], jnp.where(q == 2, rel[2], rel[3])))
        expert = (o * COLS + col) * JLOC + (n_i % GR) // CAP
        expand = (iota((NEXP, SW), 0) == expert).astype(BF16)
        hit = dot(pos, expand) == slot
        for k, g in enumerate((g1, g2, g3)):
            w = jnp.where(hit, dot(g, expand), 0.0)
            for i in range(2):
                par = planes[2 * ps + i] % 2
                wst[2 * ps + i, k * TOK:(k + 1) * TOK, :] = jnp.where(
                    par == 0, w[:TOK], w[TOK:]).astype(BF16)

    def gate_up(ps, j):
        if ps == 0:
            wcp[j][0].wait()
            wcp[j][1].wait()
        for n in range(FF // 512):
            cols = slice(n * 512, (n + 1) * 512)
            ga = dot(xs[j], wgb[j, :, cols])
            gu = dot(xs[j], wub[j, :, cols])
            hid[j, :, cols] = (jax.nn.silu(ga) * gu).astype(BF16)

    def ycopy(g, k, q):
        return pltpu.make_async_remote_copy(
            src_ref=ysend.at[g, k, q - 1], dst_ref=yrecv.at[g, k, q],
            send_sem=ys_s, recv_sem=ys_r.at[g, k],
            device_id=(d, o, rel[q]), device_id_type=MESH)

    def ywait(g, k):
        rows = yrecv.at[g, k, pl.ds(1, COLS - 1)]
        pltpu.make_async_copy(rows, rows, ys_r.at[g, k]).wait()

    def ystart(g, k):
        for q in (2, 3, 1):
            ycopy(g, k, q).start()

    def down_chunk(ps, k):
        n = ps * NC + k
        wd_copy(n).wait()
        outs = [dot(hid[j], wdb[n % WSLOT, j]) for j in range(JLOC)]
        for i in range(2):
            g = 2 * ps + i
            for q in (2, 3, 1, 0):
                at = i * GR + q * CAP
                rows = jnp.concatenate([r[at:at + CAP] for r in outs], axis=0).astype(BF16)
                if q:
                    ysend[g, k, q - 1] = rows
                else:
                    yrecv[g, k, 0] = rows
        if ps == 0:
            ystart(NB, k)
        if n + WSLOT < 2 * NC:
            wd_copy(n + WSLOT).start()

    def zcopy(k, g, slot, oo):
        return pltpu.make_async_remote_copy(
            src_ref=part.at[ZPART[g], k], dst_ref=zr.at[k, slot],
            send_sem=zs_s, recv_sem=zs_r.at[k, slot],
            device_id=(d, oo, e), device_id_type=MESH)

    def zwait(k, slot):
        rows = zr.at[k, slot]
        pltpu.make_async_copy(rows, rows, zs_r.at[k, slot]).wait()

    def half_copy(i, slot, oo):
        cols = pl.ds(i * (CW // 2), CW // 2)
        sem = zs_r.at[0, slot] if i == 0 else zh_r.at[slot // 4]
        return pltpu.make_async_remote_copy(
            src_ref=part.at[ZPART[FAR], 0, :, cols], dst_ref=zr.at[0, slot, :, cols],
            send_sem=zs_s, recv_sem=sem, device_id=(d, oo, e), device_id_type=MESH)

    def half_wait(i, slot):
        rows = zr.at[0, slot, :, pl.ds(i * (CW // 2), CW // 2)]
        pltpu.make_async_copy(rows, rows, zs_r.at[0, slot] if i == 0 else zh_r.at[slot // 4]).wait()

    def sums(g, *chunks):
        for k in chunks:
            ywait(g, k)
        for k in chunks:
            acc = dot(wst[g], yrecv[g, k].reshape(SW, CW))
            part[ZPART[g], k] = acc[0:TOK] + acc[TOK:2 * TOK] + acc[2 * TOK:3 * TOK]

    def zsend(k, g, slot, oo):
        zcopy(k, g, slot, oo).start()

    def relay(k, g, slot_in, slot_out, oo):
        zwait(k, slot_in)
        part[ZPART[g], k] = part[ZPART[g], k] + zr[k, slot_in]
        zcopy(k, g, slot_out, oo).start()

    def relay_far(k):
        if k:
            relay(k, FAR, 1, 4, other)
            return
        for i in range(2):
            cols = pl.ds(i * (CW // 2), CW // 2)
            half_wait(i, 1)
            part[ZPART[FAR], 0, :, cols] = part[ZPART[FAR], 0, :, cols] + zr[0, 1, :, cols]
            half_copy(i, 4, other).start()

    def relay_near(k):
        relay(k, NEAR, 2, 3, other)

    def relay_back(k):
        if k:
            relay(k, NB, 4, 0, nbp)
            return
        for i in range(2):
            half_wait(i, 4)
        part[ZPART[NB], 0] = part[ZPART[NB], 0] + zr[0, 4]
        zcopy(0, NB, 0, nbp).start()

    def finish(k, *slots):
        cols = pl.ds(k * CW, CW)
        for slot in slots:
            zwait(k, slot)
        total = part[ZPART[OWN], k]
        for slot in slots:
            total = total + zr[k, slot]
        out_ref[:, cols] = total.astype(BF16)

    early_blocks()
    wrcp.wait()
    gates(0)
    routes_from_mate(0)
    choose(0)
    mid_blocks()
    rows_from_mate(0)
    pick(0)
    for j in range(JLOC):
        gate_up(0, j)
        late_blocks(j)
    for k in range(NC):
        down_chunk(0, k)
        for step in {0: (4,), 2: (5,), 3: (6,), 5: (7,)}.get(k, ()):
            late_blocks(step)

    def sums_nb(*chunks):
        sums(NB, *chunks)

        @at_end
        def _():
            for k in chunks:
                zsend(k, NB, 0, nbp)

    routes_from_mate(1)
    choose(1)
    rows_from_mate(1)
    pick(1)
    for j in range(JLOC):
        gate_up(1, j)
        if j < JLOC - 1:
            sums_nb(2 * j, 2 * j + 1)

    def sums_far(k):
        sums(FAR, k)
        if k:
            zsend(k, FAR, 1, nbp)
        else:
            for i in range(2):
                half_copy(i, 1, nbp).start()

    lead = 4
    relayed = tuple(range(DIRECT, NC))
    for k in range(NC):
        down_chunk(1, k)
        if k == lead - 1:
            gates(1)

        @at_end
        def _():
            ystart(FAR, k)
            if k >= lead:
                sums_far(k - lead)

        @at_inner
        def _():
            if k < DIRECT:
                ystart(NEAR, k)
            if k == DIRECT - 1:
                for m in range(DIRECT):
                    ystart(FAR, m)
            if k >= DIRECT:
                ystart(FAR, k)
            if lead <= k < lead + DIRECT:
                sums(NEAR, k - lead)
                zsend(k - lead, NEAR, 3, other)

    @at_end
    def _():
        for k in relayed + tuple(range(DIRECT)):
            ystart(NEAR, k)
        for k in range(NC):
            ystart(OWN, k)
        for k in range(lead, NC):
            sums_far(k)
        for k in relayed:
            sums(NEAR, k)
            zsend(k, NEAR, 2, nbp)
        for k in range(DIRECT):
            sums(NEAR, k)
            zsend(k, NEAR, 2, planes[NEAR])
        sums(NB, NC - 2, NC - 1)
        for k in (NC - 2, NC - 1):
            zsend(k, NB, 0, nbp)
        for k in range(0, NC, 2):
            sums(OWN, k, k + 1)
        for k in range(NC):
            finish(k, 0)

    @at_inner
    def _():
        for k in relayed:
            ystart(NEAR, k)
        for k in range(NC):
            ystart(OWN, k)
        for k in range(NC):
            sums(FAR, k)
            relay_far(k)
            if k == 0:
                sums(NB, NC - 2, NC - 1)
            if k >= 4:
                relay_back(k - 4)
        for n, k in enumerate(relayed):
            sums(NEAR, k)
            relay_near(k)
            if n < 4:
                relay_back(n + 4)
            if n >= 1:
                sums(OWN, 2 * n - 2, 2 * n - 1)
        for k in relayed[:-2]:
            finish(k, 0, 3)
        for k in range(DIRECT):
            finish(k, 0, 3, 2)
        for k in relayed[-2:]:
            finish(k, 0, 3)


    sent(MATE, 4 * TOK, 4)
    sent(PASS, 4 * TOK, 4)

    @at_end
    def _():
        sent(SIDE, 7 * TOK // 2, 4)
        sent(OUT, TOK, 1)

    @at_inner
    def _():
        sent(SIDE, 7 * TOK // 2, 3)
        sent(OUT, 3 * TOK, 3)
        sent(CROSS, 2 * TOK, 2)
        sent(YCROSS, TOK // 2, 1)
        half_rows = x_all.at[0, pl.ds(0, TOK // 2)]
        pltpu.make_async_copy(half_rows, half_rows, bx_s.at[YOUT]).wait()

    pltpu.make_async_copy(ysend, ysend, ys_s).wait()
    moved = part.at[pl.ds(0, 3)]
    pltpu.make_async_copy(moved, moved, zs_s).wait()


def solution(mesh):
    row_spec = P(('data', 'outer', 'expert'), None)
    weight_spec = P(('outer', 'expert'), None, None)
    anyspace = pl.BlockSpec(memory_space=pl.ANY)
    dma = pltpu.SemaphoreType.DMA

    def per_device(tokens, w_router, routes, w_gate, w_up, w_down):
        return pl.pallas_call(
            kernel,
            name='moe',
            out_shape=pltpu.VMEM((TOK, DIM), BF16),
            in_specs=[anyspace] * 6,
            out_specs=pl.BlockSpec(memory_space=pltpu.VMEM),
            scratch_shapes=[
                pltpu.VMEM((2, HT, DIM), BF16),
                pltpu.VMEM((2, COLS, 2, TOPK, 128), F32),
                pltpu.VMEM((NEXP, DIM), BF16),
                pltpu.VMEM((TOPK, TOK), jnp.int32),
                pltpu.VMEM((JLOC * MR, HT), BF16),
                pltpu.VMEM((JLOC, MR, DIM), BF16),
                pltpu.VMEM((JLOC, DIM, FF), BF16),
                pltpu.VMEM((JLOC, DIM, FF), BF16),
                pltpu.VMEM((WSLOT, JLOC, FF, CW), BF16),
                pltpu.VMEM((JLOC, MR, FF), BF16),
                pltpu.VMEM((4, NC, COLS - 1, GR, CW), BF16),
                pltpu.VMEM((4, NC, COLS, GR, CW), BF16),
                pltpu.VMEM((4, 3 * TOK, SW), BF16),
                pltpu.VMEM((4, NC, TOK, CW), F32),
                pltpu.VMEM((NC, 5, TOK, CW), F32),
                dma((3,)), dma((2, JLOC)), dma((WSLOT,)),
                dma((7,)), dma((7,)),
                dma((2, PLANES, 4)), dma((2, PLANES)), dma((2,)), dma((2,)),
                dma, dma((4, NC)), dma, dma((NC, 5)), dma((2,)),
            ],
            compiler_params=pltpu.CompilerParams(
                collective_id=0, has_side_effects=True, vmem_limit_bytes=67043328 - (1 << 20)),
        )(tokens, w_router.T, routes.T, w_gate, w_up, w_down)

    return jax.shard_map(
        per_device, mesh=mesh,
        in_specs=(row_spec, P(), row_spec, weight_spec, weight_spec, weight_spec),
        out_specs=row_spec, check_vma=False)
```

```python
import jax
import jax.numpy as jnp
from jax import lax
from jax.experimental import pallas as pl
from jax.experimental.pallas import tpu as pltpu
from jax.sharding import PartitionSpec as P

MESH = pl.DeviceIdType.MESH
F32, BF16 = jnp.float32, jnp.bfloat16
PLANES = 4
COLS = 4
JLOC = 4
TOK = 64
TOPK = 8
CAP = 10
DIM = 2048
FF = 1024
NEXP = 64
CW = 256
NC = DIM // CW
DIRECT = 3
WSLOT = 6
EARLY = 6
GR = JLOC * CAP
MR = 2 * COLS * CAP
SW = COLS * GR
CT = 2 * TOK
HT = COLS * CT
NB, OWN, FAR, NEAR = range(4)
OUT, CROSS, SIDE, MATE, PASS, YCROSS, YOUT = range(7)
ZPART = {NB: 0, FAR: 1, NEAR: 2, OWN: 3}


def iota(shape, dim):
    return lax.broadcasted_iota(jnp.int32, shape, dim)


def dot(a, b):
    return jnp.dot(a, b, preferred_element_type=F32)


def dot_nt(a, b):
    return lax.dot_general(a, b, (((1,), (1,)), ((), ())), preferred_element_type=F32)


def kernel(x_hbm, wr_hbm, rt_hbm, wg_hbm, wu_hbm, wd_hbm, out_ref,
           x_all, r_all, wr, rt, sel, xs, wgb, wub, wdb, hid, ysend, yrecv, wst, part, zr,
           lsem, wsem, dsem, bx_s, br_s, bx_r, br_r, mx_r, mr_r, ys_s, ys_r, zs_s, zs_r, zh_r):
    d = lax.axis_index('data')
    o = lax.axis_index('outer')
    e = lax.axis_index('expert')
    c = e % 2
    y = e // 2
    mate = e + 1 - 2 * c
    yp = e + 2 - 4 * y
    diag = mate + yp - e
    rel = (e, mate, yp, diag)
    side = o // 2
    nbp = o + 1 - 2 * (o % 2)
    other = PLANES - 1 - o
    planes = (nbp, o, 3 - 3 * side, 2 - side)
    halves = (side, 1 - side)
    end = (o == 0) | (o == PLANES - 1)
    inner = jnp.logical_not(end)

    def at_end(fn):
        pl.when(end)(fn)

    def at_inner(fn):
        pl.when(inner)(fn)

    def rows_of(col, g, i, n):
        p = planes[g]
        start = col * CT + (p % 2) * TOK + i * (TOK // n)
        return p // 2, pl.ds(pl.multiple_of(start, TOK // n), TOK // n)

    own_half, own_rows = rows_of(e, OWN, 0, 1)
    xcp = pltpu.make_async_copy(x_hbm, x_all.at[own_half, own_rows], lsem.at[0])
    xcp.start()
    rtcp = pltpu.make_async_copy(rt_hbm, rt, lsem.at[2])
    rtcp.start()

    barrier = pltpu.get_barrier_semaphore()

    def greet(oo, ee):
        pl.semaphore_signal(barrier, inc=1, device_id=(d, oo, ee), device_id_type=MESH)

    for q in range(1, 4):
        greet(o, rel[q])
    greet(nbp, e)

    @at_end
    def _():
        greet(planes[NEAR], e)

    @at_inner
    def _():
        greet(other, e)
        greet(planes[FAR], e)

    rtcp.wait()
    dup = (iota((TOK, 128), 1) % TOK == iota((TOK, 128), 0)).astype(BF16)
    r_all[side, e, o % 2] = dot(rt[...].astype(F32).astype(BF16), dup)

    xcp.wait()
    wrcp = pltpu.make_async_copy(wr_hbm, wr, lsem.at[1])
    wrcp.start()
    wcp = []
    for j in range(JLOC):
        a = pltpu.make_async_copy(wg_hbm.at[j], wgb.at[j], wsem.at[0, j])
        b = pltpu.make_async_copy(wu_hbm.at[j], wub.at[j], wsem.at[1, j])
        a.start()
        b.start()
        wcp.append((a, b))

    def wd_copy(n):
        return pltpu.make_async_copy(
            wd_hbm.at[:, :, pl.ds((n if n < EARLY else n - EARLY) * CW, CW)], wdb.at[n % WSLOT], dsem.at[n % WSLOT])

    for n in range(WSLOT):
        wd_copy(n).start()

    @at_end
    def _():
        pl.semaphore_wait(barrier, 5)

    @at_inner
    def _():
        pl.semaphore_wait(barrier, 6)

    def count(g, direction=MATE):
        return 4 if g == FAR or (g, direction) == (NB, CROSS) else 2

    targets = {OUT: (e, nbp, e), CROSS: (e, other, e), SIDE: (e, o, yp), MATE: (e, o, mate),
               PASS: (yp, o, mate), YCROSS: (yp, other, e), YOUT: (yp, nbp, e)}

    def block(g, i, n, direction):
        col, oo, ee = targets[direction]
        half, rows = rows_of(col, g, i, n)
        if direction in (MATE, PASS):
            x_sem, r_sem = mx_r.at[planes[g] // 2], mr_r.at[planes[g] // 2]
        else:
            lane = 0 if direction in (OUT, CROSS) else 1
            x_sem, r_sem = bx_r.at[lane, planes[g], i], br_r.at[lane, planes[g]]
        cps = [pltpu.make_async_remote_copy(
            src_ref=x_all.at[half, rows], dst_ref=x_all.at[half, rows],
            send_sem=bx_s.at[direction], recv_sem=x_sem,
            device_id=(d, oo, ee), device_id_type=MESH)]
        if i == 0:
            tile = r_all.at[half, col, planes[g] % 2]
            cps.insert(0, pltpu.make_async_remote_copy(
                src_ref=tile, dst_ref=tile,
                send_sem=br_s.at[direction], recv_sem=r_sem,
                device_id=(d, oo, ee), device_id_type=MESH))
        return cps

    def send(g, i, *directions):
        for direction in directions:
            n, base = count(g, direction), count(g)
            for k in range(i * n // base, (i + 1) * n // base):
                for cp in block(g, k, n, direction):
                    cp.start()

    def arrive(lane, g, i):
        n = count(g)
        half, rows = rows_of((e, yp)[lane], g, i, n)
        piece = x_all.at[half, rows]
        if i == 0:
            tile = r_all.at[half, (e, yp)[lane], planes[g] % 2]
            pltpu.make_async_copy(tile, tile, br_r.at[lane, planes[g]]).wait()
        pltpu.make_async_copy(piece, piece, bx_r.at[lane, planes[g], i]).wait()

    def sent(direction, nrows, ntiles):
        rows = x_all.at[0, pl.ds(0, nrows)]
        pltpu.make_async_copy(rows, rows, bx_s.at[direction]).wait()
        tiles = r_all.at[0, pl.ds(0, ntiles), 0]
        pltpu.make_async_copy(tiles, tiles, br_s.at[direction]).wait()

    def get(g, i, *directions):
        arrive(0, g, i)
        send(g, i, *directions, MATE)

    def yget(g, i, *directions):
        arrive(1, g, i)
        send(g, i, *directions, PASS)

    def routes_from_mate(ps):
        tiles = r_all.at[halves[ps], pl.ds(0, 2)]
        pltpu.make_async_copy(tiles, tiles, mr_r.at[halves[ps]]).wait()

    def rows_from_mate(ps):
        rows = x_all.at[halves[ps], pl.ds(0, 2 * CT)]
        pltpu.make_async_copy(rows, rows, mx_r.at[halves[ps]]).wait()

    def early_blocks():
        @at_end
        def _():
            for h in range(2):
                send(OWN, h, OUT, SIDE, MATE)
            for h in range(2):
                get(NB, h, SIDE)
                yget(OWN, h)
            get(NEAR, 0, SIDE)
            yget(NB, 0)

        @at_inner
        def _():
            for h in range(2):
                send(OWN, h, OUT, CROSS, SIDE, MATE)
            get(NB, 0, CROSS, SIDE)
            get(NEAR, 0, OUT)
            yget(OWN, 0)
            get(NB, 1, CROSS, SIDE)
            send(OWN, 0, YCROSS)
            get(NEAR, 1, OUT, SIDE)
            yget(OWN, 1)
            get(FAR, 0, OUT)
            get(FAR, 1, OUT)
            yget(NB, 0)

    def mid_blocks():
        @at_end
        def _():
            get(NEAR, 1, SIDE)
            yget(NB, 1)

        @at_inner
        def _():
            get(FAR, 2, OUT, SIDE)
            get(FAR, 3, OUT, SIDE)
            send(FAR, 0, SIDE)
            send(FAR, 1, SIDE)
            yget(NB, 1)

    zlate = ([(FAR, 0)], [(FAR, 1)], [(FAR, 2)], [(FAR, 3)], [], [], [], [])
    ylate_end = ([], [(NEAR, 0)], [], [(NEAR, 1)], [(FAR, 0)], [(FAR, 1)], [(FAR, 2)], [(FAR, 3)])
    ylate_inner = ([(NEAR, 0)], [(NEAR, 1), (FAR, 2)], [(FAR, 3)], [(FAR, 0)], [(FAR, 1)], [], [], [])

    def late_blocks(step):
        @at_end
        def _():
            for g, i in zlate[step]:
                if i < 2:
                    get(g, i, SIDE)
                else:
                    get(g, i)
            for g, i in ylate_end[step]:
                yget(g, i)

        if ylate_inner[step]:
            @at_inner
            def _():
                for g, i in ylate_inner[step]:
                    if g == FAR and i >= 2:
                        yget(g, i, YOUT)
                    else:
                        yget(g, i)

    col_i, row_i = iota((CT, CT), 1), iota((CT, CT), 0)
    same = col_i // TOK == row_i // TOK
    before = (same & (row_i < col_i)).astype(BF16)
    after = (same & (col_i < row_i)).astype(BF16)
    eye = (col_i == row_i).astype(BF16)
    low = iota((TOPK, CT), 1) < TOK
    mine = ((o * COLS + e) * JLOC).astype(F32)

    def choose(ps):
        half = halves[ps]
        r = r_all[half]
        routes = jnp.concatenate(
            [jnp.where(low, r[k, 0], r[k, 1]) for k in range(COLS)], axis=1)
        m = [jnp.max((routes == mine + j).astype(F32), axis=0, keepdims=True)
             for j in range(JLOC)]
        m = jnp.concatenate(m + [jnp.zeros((8 - JLOC, HT), F32)], axis=0)
        mb = m.astype(BF16)
        pos = jnp.concatenate(
            [dot(mb[:, k * CT:(k + 1) * CT], before) for k in range(COLS)], axis=1)
        pm = jnp.where(m > 0.5, pos, -1.0)
        ri, ci = iota((MR, HT), 0), iota((MR, HT), 1)
        q = (ri % GR) // CAP
        col = jnp.where(q == 0, rel[0], jnp.where(q == 1, rel[1], jnp.where(q == 2, rel[2], rel[3])))
        par = jnp.where(ri < GR, planes[2 * ps] % 2, planes[2 * ps + 1] % 2)
        want = jnp.where((ci // CT == col) & ((ci // TOK) % 2 == par), ri % CAP, -2).astype(F32)
        sel[...] = jnp.concatenate(
            [(pm[j:j + 1, :] == want).astype(F32) for j in range(JLOC)], axis=0).astype(BF16)

    def pick(ps):
        for n in range(DIM // 512):
            cols = pl.ds(n * 512, 512)
            got = dot(sel[...], x_all[halves[ps], :, cols])
            for j in range(JLOC):
                xs[j, :, cols] = got[j * MR:(j + 1) * MR].astype(BF16)

    def gates(ps):
        half = halves[ps]
        r = r_all[half, e]
        routes = jnp.where(low, r[0], r[1])
        exp_id = iota((NEXP, CT), 0).astype(F32)
        hot = jnp.zeros((NEXP, CT), F32)
        for k in range(TOPK):
            hot = hot + (routes[k:k + 1, :] == exp_id).astype(F32)
        hot = hot.astype(BF16)
        chosen = dot_nt(eye, hot) > 0.5
        pos = jnp.where(chosen, dot_nt(after, hot), -1.0)
        logits = dot_nt(x_all[half, pl.ds(pl.multiple_of(e * CT, CT), CT)], wr[...])
        top = jnp.max(jnp.where(chosen, logits, -jnp.inf), axis=1, keepdims=True)
        ex = jnp.where(chosen, jnp.exp(logits - top), 0.0)
        gate = ex / jnp.sum(ex, axis=1, keepdims=True)
        g1 = gate.astype(BF16)
        rest = gate - g1.astype(F32)
        g2 = rest.astype(BF16)
        g3 = (rest - g2.astype(F32)).astype(BF16)
        pos = pos.astype(BF16)
        slot = (iota((CT, SW), 1) % CAP).astype(F32)
        n_i = iota((NEXP, SW), 1)
        q = n_i // GR
        col = jnp.where(q == 0, rel[0], jnp.where(q == 1, rel[1], jnp.where(q == 2, rel[2], rel[3])))
        expert = (o * COLS + col) * JLOC + (n_i % GR) // CAP
        expand = (iota((NEXP, SW), 0) == expert).astype(BF16)
        hit = dot(pos, expand) == slot
        for k, g in enumerate((g1, g2, g3)):
            w = jnp.where(hit, dot(g, expand), 0.0)
            for i in range(2):
                par = planes[2 * ps + i] % 2
                wst[2 * ps + i, k * TOK:(k + 1) * TOK, :] = jnp.where(
                    par == 0, w[:TOK], w[TOK:]).astype(BF16)

    def gate_up(ps, j):
        if ps == 0:
            wcp[j][0].wait()
            wcp[j][1].wait()
        for n in range(FF // 512):
            cols = slice(n * 512, (n + 1) * 512)
            ga = dot(xs[j], wgb[j, :, cols])
            gu = dot(xs[j], wub[j, :, cols])
            hid[j, ps * MR:(ps + 1) * MR, cols] = (jax.nn.silu(ga) * gu).astype(BF16)

    def ycopy(g, k, q):
        return pltpu.make_async_remote_copy(
            src_ref=ysend.at[g, k, q - 1], dst_ref=yrecv.at[g, k, q],
            send_sem=ys_s, recv_sem=ys_r.at[g, k],
            device_id=(d, o, rel[q]), device_id_type=MESH)

    def ywait(g, k):
        rows = yrecv.at[g, k, pl.ds(1, COLS - 1)]
        pltpu.make_async_copy(rows, rows, ys_r.at[g, k]).wait()

    def ystart(g, k):
        for q in (2, 3, 1):
            ycopy(g, k, q).start()

    def down_chunk(ps, k):
        n = k if ps == 0 else EARLY + k
        both = ps == 1 and k >= EARLY
        first = 0 if both else ps * MR
        wd_copy(n).wait()
        outs = [dot(hid[j, first:(ps + 1) * MR], wdb[n % WSLOT, j]) for j in range(JLOC)]
        for pp in ((1, 0) if both else (ps,)):
            for i in range(2):
                g = 2 * pp + i
                for q in (2, 3, 1, 0):
                    at = pp * MR - first + i * GR + q * CAP
                    rows = jnp.concatenate([r[at:at + CAP] for r in outs], axis=0).astype(BF16)
                    if q:
                        ysend[g, k, q - 1] = rows
                    else:
                        yrecv[g, k, 0] = rows
        if ps == 0:
            ystart(NB, k)
        if n + WSLOT < EARLY + NC:
            wd_copy(n + WSLOT).start()

    def zcopy(k, g, slot, oo):
        return pltpu.make_async_remote_copy(
            src_ref=part.at[ZPART[g], k], dst_ref=zr.at[k, slot],
            send_sem=zs_s, recv_sem=zs_r.at[k, slot],
            device_id=(d, oo, e), device_id_type=MESH)

    def zwait(k, slot):
        rows = zr.at[k, slot]
        pltpu.make_async_copy(rows, rows, zs_r.at[k, slot]).wait()

    def half_copy(i, slot, oo):
        cols = pl.ds(i * (CW // 2), CW // 2)
        sem = zs_r.at[0, slot] if i == 0 else zh_r.at[slot // 4]
        return pltpu.make_async_remote_copy(
            src_ref=part.at[ZPART[FAR], 0, :, cols], dst_ref=zr.at[0, slot, :, cols],
            send_sem=zs_s, recv_sem=sem, device_id=(d, oo, e), device_id_type=MESH)

    def half_wait(i, slot):
        rows = zr.at[0, slot, :, pl.ds(i * (CW // 2), CW // 2)]
        pltpu.make_async_copy(rows, rows, zs_r.at[0, slot] if i == 0 else zh_r.at[slot // 4]).wait()

    def sums(g, *chunks):
        for k in chunks:
            ywait(g, k)
        for k in chunks:
            acc = dot(wst[g], yrecv[g, k].reshape(SW, CW))
            part[ZPART[g], k] = acc[0:TOK] + acc[TOK:2 * TOK] + acc[2 * TOK:3 * TOK]

    def zsend(k, g, slot, oo):
        zcopy(k, g, slot, oo).start()

    def relay(k, g, slot_in, slot_out, oo):
        zwait(k, slot_in)
        part[ZPART[g], k] = part[ZPART[g], k] + zr[k, slot_in]
        zcopy(k, g, slot_out, oo).start()

    def relay_far(k):
        if k:
            relay(k, FAR, 1, 4, other)
            return
        for i in range(2):
            cols = pl.ds(i * (CW // 2), CW // 2)
            half_wait(i, 1)
            part[ZPART[FAR], 0, :, cols] = part[ZPART[FAR], 0, :, cols] + zr[0, 1, :, cols]
            half_copy(i, 4, other).start()

    def relay_near(k):
        relay(k, NEAR, 2, 3, other)

    def relay_back(k):
        if k:
            relay(k, NB, 4, 0, nbp)
            return
        for i in range(2):
            half_wait(i, 4)
        part[ZPART[NB], 0] = part[ZPART[NB], 0] + zr[0, 4]
        zcopy(0, NB, 0, nbp).start()

    def finish(k, *slots):
        cols = pl.ds(k * CW, CW)
        for slot in slots:
            zwait(k, slot)
        total = part[ZPART[OWN], k]
        for slot in slots:
            total = total + zr[k, slot]
        out_ref[:, cols] = total.astype(BF16)

    early_blocks()
    wrcp.wait()
    gates(0)
    routes_from_mate(0)
    choose(0)
    mid_blocks()
    rows_from_mate(0)
    pick(0)
    for j in range(JLOC):
        gate_up(0, j)
        late_blocks(j)
    for k in range(EARLY):
        down_chunk(0, k)
        for step in {0: (4, 5), 1: (6,), 3: (7,)}.get(k, ()):
            late_blocks(step)

    def sums_nb(*chunks):
        sums(NB, *chunks)

        @at_end
        def _():
            for k in chunks:
                zsend(k, NB, 0, nbp)

    routes_from_mate(1)
    choose(1)
    rows_from_mate(1)
    pick(1)
    for j in range(JLOC):
        gate_up(1, j)
        if j < JLOC - 1:
            sums_nb(2 * j, 2 * j + 1)

    def sums_far(k):
        sums(FAR, k)
        if k:
            zsend(k, FAR, 1, nbp)
        else:
            for i in range(2):
                half_copy(i, 1, nbp).start()

    lead = 4
    relayed = tuple(range(DIRECT, NC))
    for k in range(NC):
        down_chunk(1, k)
        if k == lead - 1:
            gates(1)

        @at_end
        def _():
            ystart(FAR, k)
            if k >= lead:
                sums_far(k - lead)

        @at_inner
        def _():
            if k < DIRECT:
                ystart(NEAR, k)
            if k == DIRECT - 1:
                for m in range(DIRECT):
                    ystart(FAR, m)
            if k >= DIRECT:
                ystart(FAR, k)
            if lead <= k < lead + DIRECT:
                sums(NEAR, k - lead)
                zsend(k - lead, NEAR, 3, other)

    @at_end
    def _():
        for k in relayed + tuple(range(DIRECT)):
            ystart(NEAR, k)
        for k in range(EARLY, NC):
            ystart(NB, k)
        for k in range(NC):
            ystart(OWN, k)
        for k in range(lead, NC):
            sums_far(k)
        for k in relayed:
            sums(NEAR, k)
            zsend(k, NEAR, 2, nbp)
        for k in range(DIRECT):
            sums(NEAR, k)
            zsend(k, NEAR, 2, planes[NEAR])
        sums(NB, NC - 2, NC - 1)
        for k in (NC - 2, NC - 1):
            zsend(k, NB, 0, nbp)
        for k in range(0, NC, 2):
            sums(OWN, k, k + 1)
        for k in range(NC):
            finish(k, 0)

    @at_inner
    def _():
        for k in relayed:
            ystart(NEAR, k)
        for k in range(EARLY, NC):
            ystart(NB, k)
        for k in range(NC):
            ystart(OWN, k)
        for k in range(NC):
            sums(FAR, k)
            relay_far(k)
            if k >= 4:
                relay_back(k - 4)
        for n, k in enumerate(relayed):
            sums(NEAR, k)
            relay_near(k)
            if n < 4:
                relay_back(n + 4)
            if n == 1:
                sums(NB, NC - 2, NC - 1)
            if n >= 2:
                sums(OWN, 2 * n - 4, 2 * n - 3)
        sums(OWN, NC - 2, NC - 1)
        for k in relayed[:-2]:
            finish(k, 0, 3)
        for k in range(DIRECT):
            finish(k, 0, 3, 2)
        for k in relayed[-2:]:
            finish(k, 0, 3)


    sent(MATE, 4 * TOK, 4)
    sent(PASS, 4 * TOK, 4)

    @at_end
    def _():
        sent(SIDE, 7 * TOK // 2, 4)
        sent(OUT, TOK, 1)

    @at_inner
    def _():
        sent(SIDE, 7 * TOK // 2, 3)
        sent(OUT, 3 * TOK, 3)
        sent(CROSS, 2 * TOK, 2)
        sent(YCROSS, TOK // 2, 1)
        half_rows = x_all.at[0, pl.ds(0, TOK // 2)]
        pltpu.make_async_copy(half_rows, half_rows, bx_s.at[YOUT]).wait()

    pltpu.make_async_copy(ysend, ysend, ys_s).wait()
    moved = part.at[pl.ds(0, 3)]
    pltpu.make_async_copy(moved, moved, zs_s).wait()


def solution(mesh):
    row_spec = P(('data', 'outer', 'expert'), None)
    weight_spec = P(('outer', 'expert'), None, None)
    anyspace = pl.BlockSpec(memory_space=pl.ANY)
    dma = pltpu.SemaphoreType.DMA

    def per_device(tokens, w_router, routes, w_gate, w_up, w_down):
        return pl.pallas_call(
            kernel,
            name='moe',
            out_shape=pltpu.VMEM((TOK, DIM), BF16),
            in_specs=[anyspace] * 6,
            out_specs=pl.BlockSpec(memory_space=pltpu.VMEM),
            scratch_shapes=[
                pltpu.VMEM((2, HT, DIM), BF16),
                pltpu.VMEM((2, COLS, 2, TOPK, 128), F32),
                pltpu.VMEM((NEXP, DIM), BF16),
                pltpu.VMEM((TOPK, TOK), jnp.int32),
                pltpu.VMEM((JLOC * MR, HT), BF16),
                pltpu.VMEM((JLOC, MR, DIM), BF16),
                pltpu.VMEM((JLOC, DIM, FF), BF16),
                pltpu.VMEM((JLOC, DIM, FF), BF16),
                pltpu.VMEM((WSLOT, JLOC, FF, CW), BF16),
                pltpu.VMEM((JLOC, 2 * MR, FF), BF16),
                pltpu.VMEM((4, NC, COLS - 1, GR, CW), BF16),
                pltpu.VMEM((4, NC, COLS, GR, CW), BF16),
                pltpu.VMEM((4, 3 * TOK, SW), BF16),
                pltpu.VMEM((4, NC, TOK, CW), F32),
                pltpu.VMEM((NC, 5, TOK, CW), F32),
                dma((3,)), dma((2, JLOC)), dma((WSLOT,)),
                dma((7,)), dma((7,)),
                dma((2, PLANES, 4)), dma((2, PLANES)), dma((2,)), dma((2,)),
                dma, dma((4, NC)), dma, dma((NC, 5)), dma((2,)),
            ],
            compiler_params=pltpu.CompilerParams(
                collective_id=0, has_side_effects=True, vmem_limit_bytes=67043328 - (1 << 20)),
        )(tokens, w_router.T, routes.T, w_gate, w_up, w_down)

    return jax.shard_map(
        per_device, mesh=mesh,
        in_specs=(row_spec, P(), row_spec, weight_spec, weight_spec, weight_spec),
        out_specs=row_spec, check_vma=False)
```

```python
import jax
import jax.numpy as jnp
from jax import lax
from jax.experimental import pallas as pl
from jax.experimental.pallas import tpu as pltpu
from jax.sharding import PartitionSpec as P

MESH = pl.DeviceIdType.MESH
F32, BF16 = jnp.float32, jnp.bfloat16
PLANES = 4
COLS = 4
JLOC = 4
TOK = 64
TOPK = 8
CAP = 10
DIM = 2048
FF = 1024
NEXP = 64
CW = 256
NC = DIM // CW
DIRECT = 3
WSLOT = 6
EARLY = 6
GR = JLOC * CAP
MR = 2 * COLS * CAP
SW = COLS * GR
CT = 2 * TOK
HT = COLS * CT
NB, OWN, FAR, NEAR = range(4)
OUT, CROSS, SIDE, MATE, PASS, YCROSS, YOUT = range(7)
ZPART = {NB: 0, FAR: 1, NEAR: 2, OWN: 3}


def iota(shape, dim):
    return lax.broadcasted_iota(jnp.int32, shape, dim)


def dot(a, b):
    return jnp.dot(a, b, preferred_element_type=F32)


def dot_nt(a, b):
    return lax.dot_general(a, b, (((1,), (1,)), ((), ())), preferred_element_type=F32)


def kernel(x_hbm, wr_hbm, rt_hbm, wg_hbm, wu_hbm, wd_hbm, out_ref,
           x_all, r_all, wr, rt, sel, xs, wgb, wub, wdb, hid, ysend, yrecv, wst, part, zr,
           lsem, wsem, dsem, bx_s, br_s, bx_r, br_r, mx_r, mr_r, ys_s, ys_r, zs_s, zs_r, zh_r, yh_r):
    d = lax.axis_index('data')
    o = lax.axis_index('outer')
    e = lax.axis_index('expert')
    c = e % 2
    y = e // 2
    mate = e + 1 - 2 * c
    yp = e + 2 - 4 * y
    diag = mate + yp - e
    rel = (e, mate, yp, diag)
    side = o // 2
    nbp = o + 1 - 2 * (o % 2)
    other = PLANES - 1 - o
    planes = (nbp, o, 3 - 3 * side, 2 - side)
    halves = (side, 1 - side)
    end = (o == 0) | (o == PLANES - 1)
    inner = jnp.logical_not(end)

    def at_end(fn):
        pl.when(end)(fn)

    def at_inner(fn):
        pl.when(inner)(fn)

    def rows_of(col, g, i, n):
        p = planes[g]
        start = col * CT + (p % 2) * TOK + i * (TOK // n)
        return p // 2, pl.ds(pl.multiple_of(start, TOK // n), TOK // n)

    own_half, own_rows = rows_of(e, OWN, 0, 1)
    xcp = pltpu.make_async_copy(x_hbm, x_all.at[own_half, own_rows], lsem.at[0])
    xcp.start()
    rtcp = pltpu.make_async_copy(rt_hbm, rt, lsem.at[2])
    rtcp.start()

    barrier = pltpu.get_barrier_semaphore()

    def greet(oo, ee):
        pl.semaphore_signal(barrier, inc=1, device_id=(d, oo, ee), device_id_type=MESH)

    for q in range(1, 4):
        greet(o, rel[q])
    greet(nbp, e)

    @at_end
    def _():
        greet(planes[NEAR], e)

    @at_inner
    def _():
        greet(other, e)
        greet(planes[FAR], e)

    rtcp.wait()
    dup = (iota((TOK, 128), 1) % TOK == iota((TOK, 128), 0)).astype(BF16)
    r_all[side, e, o % 2] = dot(rt[...].astype(F32).astype(BF16), dup)

    xcp.wait()
    wrcp = pltpu.make_async_copy(wr_hbm, wr, lsem.at[1])
    wrcp.start()
    wcp = []
    for j in range(JLOC):
        a = pltpu.make_async_copy(wg_hbm.at[j], wgb.at[j], wsem.at[0, j])
        b = pltpu.make_async_copy(wu_hbm.at[j], wub.at[j], wsem.at[1, j])
        a.start()
        b.start()
        wcp.append((a, b))

    def wd_copy(n):
        return pltpu.make_async_copy(
            wd_hbm.at[:, :, pl.ds((n if n < EARLY else n - EARLY) * CW, CW)], wdb.at[n % WSLOT], dsem.at[n % WSLOT])

    for n in range(WSLOT):
        wd_copy(n).start()

    @at_end
    def _():
        pl.semaphore_wait(barrier, 5)

    @at_inner
    def _():
        pl.semaphore_wait(barrier, 6)

    def count(g, direction=MATE):
        return 4 if g == FAR or (g, direction) == (NB, CROSS) else 2

    targets = {OUT: (e, nbp, e), CROSS: (e, other, e), SIDE: (e, o, yp), MATE: (e, o, mate),
               PASS: (yp, o, mate), YCROSS: (yp, other, e), YOUT: (yp, nbp, e)}

    def block(g, i, n, direction):
        col, oo, ee = targets[direction]
        half, rows = rows_of(col, g, i, n)
        if direction in (MATE, PASS):
            x_sem, r_sem = mx_r.at[planes[g] // 2], mr_r.at[planes[g] // 2]
        else:
            lane = 0 if direction in (OUT, CROSS) else 1
            x_sem, r_sem = bx_r.at[lane, planes[g], i], br_r.at[lane, planes[g]]
        cps = [pltpu.make_async_remote_copy(
            src_ref=x_all.at[half, rows], dst_ref=x_all.at[half, rows],
            send_sem=bx_s.at[direction], recv_sem=x_sem,
            device_id=(d, oo, ee), device_id_type=MESH)]
        if i == 0:
            tile = r_all.at[half, col, planes[g] % 2]
            cps.insert(0, pltpu.make_async_remote_copy(
                src_ref=tile, dst_ref=tile,
                send_sem=br_s.at[direction], recv_sem=r_sem,
                device_id=(d, oo, ee), device_id_type=MESH))
        return cps

    def send(g, i, *directions):
        for direction in directions:
            n, base = count(g, direction), count(g)
            for k in range(i * n // base, (i + 1) * n // base):
                for cp in block(g, k, n, direction):
                    cp.start()

    def arrive(lane, g, i):
        n = count(g)
        half, rows = rows_of((e, yp)[lane], g, i, n)
        piece = x_all.at[half, rows]
        if i == 0:
            tile = r_all.at[half, (e, yp)[lane], planes[g] % 2]
            pltpu.make_async_copy(tile, tile, br_r.at[lane, planes[g]]).wait()
        pltpu.make_async_copy(piece, piece, bx_r.at[lane, planes[g], i]).wait()

    def sent(direction, nrows, ntiles):
        rows = x_all.at[0, pl.ds(0, nrows)]
        pltpu.make_async_copy(rows, rows, bx_s.at[direction]).wait()
        tiles = r_all.at[0, pl.ds(0, ntiles), 0]
        pltpu.make_async_copy(tiles, tiles, br_s.at[direction]).wait()

    def get(g, i, *directions):
        arrive(0, g, i)
        send(g, i, *directions, MATE)

    def yget(g, i, *directions):
        arrive(1, g, i)
        send(g, i, *directions, PASS)

    def routes_from_mate(ps):
        tiles = r_all.at[halves[ps], pl.ds(0, 2)]
        pltpu.make_async_copy(tiles, tiles, mr_r.at[halves[ps]]).wait()

    def rows_from_mate(ps):
        rows = x_all.at[halves[ps], pl.ds(0, 2 * CT)]
        pltpu.make_async_copy(rows, rows, mx_r.at[halves[ps]]).wait()

    def early_blocks():
        @at_end
        def _():
            for h in range(2):
                send(OWN, h, OUT, SIDE, MATE)
            for h in range(2):
                get(NB, h, SIDE)
                yget(OWN, h)
            get(NEAR, 0, SIDE)
            yget(NB, 0)

        @at_inner
        def _():
            for h in range(2):
                send(OWN, h, OUT, CROSS, SIDE, MATE)
            get(NB, 0, CROSS, SIDE)
            get(NEAR, 0, OUT)
            yget(OWN, 0)
            get(NB, 1, CROSS, SIDE)
            send(OWN, 0, YCROSS)
            get(NEAR, 1, OUT, SIDE)
            yget(OWN, 1)
            get(FAR, 0, OUT)
            get(FAR, 1, OUT)
            yget(NB, 0)

    def mid_blocks():
        @at_end
        def _():
            get(NEAR, 1, SIDE)
            yget(NB, 1)

        @at_inner
        def _():
            get(FAR, 2, OUT, SIDE)
            get(FAR, 3, OUT, SIDE)
            send(FAR, 0, SIDE)
            send(FAR, 1, SIDE)
            yget(NB, 1)

    zlate = ([(FAR, 0)], [(FAR, 1)], [(FAR, 2)], [(FAR, 3)], [], [], [], [])
    ylate_end = ([], [(NEAR, 0)], [], [(NEAR, 1)], [(FAR, 0)], [(FAR, 1)], [(FAR, 2)], [(FAR, 3)])
    ylate_inner = ([(NEAR, 0)], [(NEAR, 1), (FAR, 2)], [(FAR, 3)], [(FAR, 0)], [(FAR, 1)], [], [], [])

    def late_blocks(step):
        @at_end
        def _():
            for g, i in zlate[step]:
                if i < 2:
                    get(g, i, SIDE)
                else:
                    get(g, i)
            for g, i in ylate_end[step]:
                yget(g, i)

        if ylate_inner[step]:
            @at_inner
            def _():
                for g, i in ylate_inner[step]:
                    if g == FAR and i >= 2:
                        yget(g, i, YOUT)
                    else:
                        yget(g, i)

    col_i, row_i = iota((CT, CT), 1), iota((CT, CT), 0)
    same = col_i // TOK == row_i // TOK
    before = (same & (row_i < col_i)).astype(BF16)
    after = (same & (col_i < row_i)).astype(BF16)
    eye = (col_i == row_i).astype(BF16)
    low = iota((TOPK, CT), 1) < TOK
    mine = ((o * COLS + e) * JLOC).astype(F32)

    def choose(ps):
        half = halves[ps]
        r = r_all[half]
        routes = jnp.concatenate(
            [jnp.where(low, r[k, 0], r[k, 1]) for k in range(COLS)], axis=1)
        m = [jnp.max((routes == mine + j).astype(F32), axis=0, keepdims=True)
             for j in range(JLOC)]
        m = jnp.concatenate(m + [jnp.zeros((8 - JLOC, HT), F32)], axis=0)
        mb = m.astype(BF16)
        pos = jnp.concatenate(
            [dot(mb[:, k * CT:(k + 1) * CT], before) for k in range(COLS)], axis=1)
        pm = jnp.where(m > 0.5, pos, -1.0)
        ri, ci = iota((MR, HT), 0), iota((MR, HT), 1)
        q = (ri % GR) // CAP
        col = jnp.where(q == 0, rel[0], jnp.where(q == 1, rel[1], jnp.where(q == 2, rel[2], rel[3])))
        par = jnp.where(ri < GR, planes[2 * ps] % 2, planes[2 * ps + 1] % 2)
        want = jnp.where((ci // CT == col) & ((ci // TOK) % 2 == par), ri % CAP, -2).astype(F32)
        sel[...] = jnp.concatenate(
            [(pm[j:j + 1, :] == want).astype(F32) for j in range(JLOC)], axis=0).astype(BF16)

    def pick(ps):
        for n in range(DIM // 512):
            cols = pl.ds(n * 512, 512)
            got = dot(sel[...], x_all[halves[ps], :, cols])
            for j in range(JLOC):
                xs[j, :, cols] = got[j * MR:(j + 1) * MR].astype(BF16)

    def gates(ps):
        half = halves[ps]
        r = r_all[half, e]
        routes = jnp.where(low, r[0], r[1])
        exp_id = iota((NEXP, CT), 0).astype(F32)
        hot = jnp.zeros((NEXP, CT), F32)
        for k in range(TOPK):
            hot = hot + (routes[k:k + 1, :] == exp_id).astype(F32)
        hot = hot.astype(BF16)
        chosen = dot_nt(eye, hot) > 0.5
        pos = jnp.where(chosen, dot_nt(after, hot), -1.0)
        logits = dot_nt(x_all[half, pl.ds(pl.multiple_of(e * CT, CT), CT)], wr[...])
        top = jnp.max(jnp.where(chosen, logits, -jnp.inf), axis=1, keepdims=True)
        ex = jnp.where(chosen, jnp.exp(logits - top), 0.0)
        gate = ex / jnp.sum(ex, axis=1, keepdims=True)
        g1 = gate.astype(BF16)
        rest = gate - g1.astype(F32)
        g2 = rest.astype(BF16)
        g3 = (rest - g2.astype(F32)).astype(BF16)
        pos = pos.astype(BF16)
        slot = (iota((CT, SW), 1) % CAP).astype(F32)
        n_i = iota((NEXP, SW), 1)
        q = n_i // GR
        col = jnp.where(q == 0, rel[0], jnp.where(q == 1, rel[1], jnp.where(q == 2, rel[2], rel[3])))
        expert = (o * COLS + col) * JLOC + (n_i % GR) // CAP
        expand = (iota((NEXP, SW), 0) == expert).astype(BF16)
        hit = dot(pos, expand) == slot
        for k, g in enumerate((g1, g2, g3)):
            w = jnp.where(hit, dot(g, expand), 0.0)
            for i in range(2):
                par = planes[2 * ps + i] % 2
                wst[2 * ps + i, k * TOK:(k + 1) * TOK, :] = jnp.where(
                    par == 0, w[:TOK], w[TOK:]).astype(BF16)

    def gate_up(ps, j):
        if ps == 0:
            wcp[j][0].wait()
            wcp[j][1].wait()
        for n in range(FF // 512):
            cols = slice(n * 512, (n + 1) * 512)
            ga = dot(xs[j], wgb[j, :, cols])
            gu = dot(xs[j], wub[j, :, cols])
            hid[j, ps * MR:(ps + 1) * MR, cols] = (jax.nn.silu(ga) * gu).astype(BF16)

    def ycopy(g, k, q):
        return pltpu.make_async_remote_copy(
            src_ref=ysend.at[g, k, q - 1], dst_ref=yrecv.at[g, k, q],
            send_sem=ys_s, recv_sem=ys_r.at[g, k],
            device_id=(d, o, rel[q]), device_id_type=MESH)

    def half_cols(i):
        return pl.ds(i * (CW // 2), CW // 2)

    def ywait_half(i):
        rows = yrecv.at[FAR, 0, pl.ds(1, COLS - 1), :, half_cols(i)]
        pltpu.make_async_copy(rows, rows, ys_r.at[FAR, 0] if i == 0 else yh_r).wait()

    def ywait(g, k):
        if (g, k) == (FAR, 0):
            ywait_half(0)
            ywait_half(1)
            return
        rows = yrecv.at[g, k, pl.ds(1, COLS - 1)]
        pltpu.make_async_copy(rows, rows, ys_r.at[g, k]).wait()

    def ystart(g, k):
        if (g, k) == (FAR, 0):
            for i in range(2):
                for q in (2, 3, 1):
                    pltpu.make_async_remote_copy(
                        src_ref=ysend.at[g, k, q - 1, :, half_cols(i)],
                        dst_ref=yrecv.at[g, k, q, :, half_cols(i)],
                        send_sem=ys_s, recv_sem=ys_r.at[g, k] if i == 0 else yh_r,
                        device_id=(d, o, rel[q]), device_id_type=MESH).start()
            return
        for q in (2, 3, 1):
            ycopy(g, k, q).start()

    def down_chunk(ps, k):
        n = k if ps == 0 else EARLY + k
        both = ps == 1 and k >= EARLY
        first = 0 if both else ps * MR
        wd_copy(n).wait()
        outs = [dot(hid[j, first:(ps + 1) * MR], wdb[n % WSLOT, j]) for j in range(JLOC)]
        for pp in ((1, 0) if both else (ps,)):
            for i in range(2):
                g = 2 * pp + i
                for q in (2, 3, 1, 0):
                    at = pp * MR - first + i * GR + q * CAP
                    rows = jnp.concatenate([r[at:at + CAP] for r in outs], axis=0).astype(BF16)
                    if q:
                        ysend[g, k, q - 1] = rows
                    else:
                        yrecv[g, k, 0] = rows
        if ps == 0:
            ystart(NB, k)
        if n + WSLOT < EARLY + NC:
            wd_copy(n + WSLOT).start()

    def zcopy(k, g, slot, oo):
        return pltpu.make_async_remote_copy(
            src_ref=part.at[ZPART[g], k], dst_ref=zr.at[k, slot],
            send_sem=zs_s, recv_sem=zs_r.at[k, slot],
            device_id=(d, oo, e), device_id_type=MESH)

    def zwait(k, slot):
        rows = zr.at[k, slot]
        pltpu.make_async_copy(rows, rows, zs_r.at[k, slot]).wait()

    def half_copy(i, slot, oo):
        cols = pl.ds(i * (CW // 2), CW // 2)
        sem = zs_r.at[0, slot] if i == 0 else zh_r.at[slot // 4]
        return pltpu.make_async_remote_copy(
            src_ref=part.at[ZPART[FAR], 0, :, cols], dst_ref=zr.at[0, slot, :, cols],
            send_sem=zs_s, recv_sem=sem, device_id=(d, oo, e), device_id_type=MESH)

    def half_wait(i, slot):
        rows = zr.at[0, slot, :, pl.ds(i * (CW // 2), CW // 2)]
        pltpu.make_async_copy(rows, rows, zs_r.at[0, slot] if i == 0 else zh_r.at[slot // 4]).wait()

    def sums(g, *chunks):
        for k in chunks:
            ywait(g, k)
        for k in chunks:
            acc = dot(wst[g], yrecv[g, k].reshape(SW, CW))
            part[ZPART[g], k] = acc[0:TOK] + acc[TOK:2 * TOK] + acc[2 * TOK:3 * TOK]

    def zsend(k, g, slot, oo):
        zcopy(k, g, slot, oo).start()

    def relay(k, g, slot_in, slot_out, oo):
        zwait(k, slot_in)
        part[ZPART[g], k] = part[ZPART[g], k] + zr[k, slot_in]
        zcopy(k, g, slot_out, oo).start()

    def relay_far(k):
        if k:
            relay(k, FAR, 1, 4, other)
            return
        for i in range(2):
            cols = pl.ds(i * (CW // 2), CW // 2)
            half_wait(i, 1)
            part[ZPART[FAR], 0, :, cols] = part[ZPART[FAR], 0, :, cols] + zr[0, 1, :, cols]
            half_copy(i, 4, other).start()

    def relay_near(k):
        relay(k, NEAR, 2, 3, other)

    def relay_back(k):
        if k:
            relay(k, NB, 4, 0, nbp)
            return
        for i in range(2):
            half_wait(i, 4)
        part[ZPART[NB], 0] = part[ZPART[NB], 0] + zr[0, 4]
        zcopy(0, NB, 0, nbp).start()

    def finish(k, *slots):
        cols = pl.ds(k * CW, CW)
        for slot in slots:
            zwait(k, slot)
        total = part[ZPART[OWN], k]
        for slot in slots:
            total = total + zr[k, slot]
        out_ref[:, cols] = total.astype(BF16)

    early_blocks()
    wrcp.wait()
    gates(0)
    routes_from_mate(0)
    choose(0)
    mid_blocks()
    rows_from_mate(0)
    pick(0)
    for j in range(JLOC):
        gate_up(0, j)
        late_blocks(j)
    for k in range(EARLY):
        down_chunk(0, k)
        for step in {0: (4, 5), 1: (6,), 3: (7,)}.get(k, ()):
            late_blocks(step)

    def sums_nb(*chunks):
        sums(NB, *chunks)

        @at_end
        def _():
            for k in chunks:
                zsend(k, NB, 0, nbp)

    routes_from_mate(1)
    choose(1)
    rows_from_mate(1)
    pick(1)
    for j in range(JLOC):
        gate_up(1, j)
        if j < JLOC - 1:
            sums_nb(2 * j, 2 * j + 1)

    def sums_far(k):
        if k:
            sums(FAR, k)
            zsend(k, FAR, 1, nbp)
            return
        for i in range(2):
            ywait_half(i)
            acc = dot(wst[FAR], yrecv[FAR, 0, :, :, half_cols(i)].reshape(SW, CW // 2))
            part[ZPART[FAR], 0, :, half_cols(i)] = (
                acc[0:TOK] + acc[TOK:2 * TOK] + acc[2 * TOK:3 * TOK])
            half_copy(i, 1, nbp).start()

    lead = 3
    relayed = tuple(range(DIRECT, NC))
    for k in range(NC):
        down_chunk(1, k)
        if k == lead - 1:
            gates(1)

        @at_end
        def _():
            ystart(FAR, k)
            if k >= lead:
                sums_far(k - lead)

        @at_inner
        def _():
            if k < DIRECT:
                ystart(NEAR, k)
            if k == DIRECT - 1:
                for m in range(DIRECT):
                    ystart(FAR, m)
            if k >= DIRECT:
                ystart(FAR, k)
            if lead <= k < lead + DIRECT:
                sums(NEAR, k - lead)
                zsend(k - lead, NEAR, 3, other)

    @at_end
    def _():
        for k in relayed + tuple(range(DIRECT)):
            ystart(NEAR, k)
        for k in range(EARLY, NC):
            ystart(NB, k)
        for k in range(NC):
            ystart(OWN, k)
        for k in range(NC - lead, NC):
            sums_far(k)
        for k in relayed:
            sums(NEAR, k)
            zsend(k, NEAR, 2, nbp)
        for k in range(DIRECT):
            sums(NEAR, k)
            zsend(k, NEAR, 2, planes[NEAR])
        sums(NB, NC - 2, NC - 1)
        for k in (NC - 2, NC - 1):
            zsend(k, NB, 0, nbp)
        for k in range(0, NC, 2):
            sums(OWN, k, k + 1)
        for k in range(NC):
            finish(k, 0)

    @at_inner
    def _():
        for k in relayed:
            ystart(NEAR, k)
        for k in range(EARLY, NC):
            ystart(NB, k)
        for k in range(NC):
            ystart(OWN, k)
        for k in range(NC):
            sums(FAR, k)
            relay_far(k)
            if k >= 4:
                relay_back(k - 4)
        for n, k in enumerate(relayed):
            sums(NEAR, k)
            relay_near(k)
            if n < 4:
                relay_back(n + 4)
            if n == 1:
                sums(NB, NC - 2, NC - 1)
            if n >= 2:
                sums(OWN, 2 * n - 4, 2 * n - 3)
        sums(OWN, NC - 2, NC - 1)
        for k in relayed[:-2]:
            finish(k, 0, 3)
        for k in range(DIRECT):
            finish(k, 0, 3, 2)
        for k in relayed[-2:]:
            finish(k, 0, 3)


    sent(MATE, 4 * TOK, 4)
    sent(PASS, 4 * TOK, 4)

    @at_end
    def _():
        sent(SIDE, 7 * TOK // 2, 4)
        sent(OUT, TOK, 1)

    @at_inner
    def _():
        sent(SIDE, 7 * TOK // 2, 3)
        sent(OUT, 3 * TOK, 3)
        sent(CROSS, 2 * TOK, 2)
        sent(YCROSS, TOK // 2, 1)
        half_rows = x_all.at[0, pl.ds(0, TOK // 2)]
        pltpu.make_async_copy(half_rows, half_rows, bx_s.at[YOUT]).wait()

    pltpu.make_async_copy(ysend, ysend, ys_s).wait()
    moved = part.at[pl.ds(0, 3)]
    pltpu.make_async_copy(moved, moved, zs_s).wait()


def solution(mesh):
    row_spec = P(('data', 'outer', 'expert'), None)
    weight_spec = P(('outer', 'expert'), None, None)
    anyspace = pl.BlockSpec(memory_space=pl.ANY)
    dma = pltpu.SemaphoreType.DMA

    def per_device(tokens, w_router, routes, w_gate, w_up, w_down):
        return pl.pallas_call(
            kernel,
            name='moe',
            out_shape=pltpu.VMEM((TOK, DIM), BF16),
            in_specs=[anyspace] * 6,
            out_specs=pl.BlockSpec(memory_space=pltpu.VMEM),
            scratch_shapes=[
                pltpu.VMEM((2, HT, DIM), BF16),
                pltpu.VMEM((2, COLS, 2, TOPK, 128), F32),
                pltpu.VMEM((NEXP, DIM), BF16),
                pltpu.VMEM((TOPK, TOK), jnp.int32),
                pltpu.VMEM((JLOC * MR, HT), BF16),
                pltpu.VMEM((JLOC, MR, DIM), BF16),
                pltpu.VMEM((JLOC, DIM, FF), BF16),
                pltpu.VMEM((JLOC, DIM, FF), BF16),
                pltpu.VMEM((WSLOT, JLOC, FF, CW), BF16),
                pltpu.VMEM((JLOC, 2 * MR, FF), BF16),
                pltpu.VMEM((4, NC, COLS - 1, GR, CW), BF16),
                pltpu.VMEM((4, NC, COLS, GR, CW), BF16),
                pltpu.VMEM((4, 3 * TOK, SW), BF16),
                pltpu.VMEM((4, NC, TOK, CW), F32),
                pltpu.VMEM((NC, 5, TOK, CW), F32),
                dma((3,)), dma((2, JLOC)), dma((WSLOT,)),
                dma((7,)), dma((7,)),
                dma((2, PLANES, 4)), dma((2, PLANES)), dma((2,)), dma((2,)),
                dma, dma((4, NC)), dma, dma((NC, 5)), dma((2,)), dma,
            ],
            compiler_params=pltpu.CompilerParams(
                collective_id=0, has_side_effects=True, vmem_limit_bytes=67043328 - (1 << 20)),
        )(tokens, w_router.T, routes.T, w_gate, w_up, w_down)

    return jax.shard_map(
        per_device, mesh=mesh,
        in_specs=(row_spec, P(), row_spec, weight_spec, weight_spec, weight_spec),
        out_specs=row_spec, check_vma=False)
```

```python
import jax
import jax.numpy as jnp
from jax import lax
from jax.experimental import pallas as pl
from jax.experimental.pallas import tpu as pltpu
from jax.sharding import PartitionSpec as P

MESH = pl.DeviceIdType.MESH
F32, BF16 = jnp.float32, jnp.bfloat16
PLANES = 4
COLS = 4
JLOC = 4
TOK = 64
TOPK = 8
CAP = 10
DIM = 2048
FF = 1024
NEXP = 64
CW = 256
NC = DIM // CW
DIRECT = 2
WSLOT = 6
EARLY = 6
GR = JLOC * CAP
MR = 2 * COLS * CAP
SW = COLS * GR
CT = 2 * TOK
HT = COLS * CT
NB, OWN, FAR, NEAR = range(4)
OUT, CROSS, SIDE, MATE, PASS, YCROSS, YOUT = range(7)
ZPART = {NB: 0, FAR: 1, NEAR: 2, OWN: 3}


def iota(shape, dim):
    return lax.broadcasted_iota(jnp.int32, shape, dim)


def dot(a, b):
    return jnp.dot(a, b, preferred_element_type=F32)


def dot_nt(a, b):
    return lax.dot_general(a, b, (((1,), (1,)), ((), ())), preferred_element_type=F32)


def kernel(x_hbm, wr_hbm, rt_hbm, wg_hbm, wu_hbm, wd_hbm, out_ref,
           x_all, r_all, wr, rt, sel, xs, wgb, wub, wdb, hid, ysend, yrecv, wst, part, zr,
           lsem, wsem, dsem, bx_s, br_s, bx_r, br_r, mx_r, mr_r, ys_s, ys_r, zs_s, zs_r, zh_r, yh_r):
    d = lax.axis_index('data')
    o = lax.axis_index('outer')
    e = lax.axis_index('expert')
    c = e % 2
    y = e // 2
    mate = e + 1 - 2 * c
    yp = e + 2 - 4 * y
    diag = mate + yp - e
    rel = (e, mate, yp, diag)
    side = o // 2
    nbp = o + 1 - 2 * (o % 2)
    other = PLANES - 1 - o
    planes = (nbp, o, 3 - 3 * side, 2 - side)
    halves = (side, 1 - side)
    end = (o == 0) | (o == PLANES - 1)
    inner = jnp.logical_not(end)

    def at_end(fn):
        pl.when(end)(fn)

    def at_inner(fn):
        pl.when(inner)(fn)

    def rows_of(col, g, i, n):
        p = planes[g]
        start = col * CT + (p % 2) * TOK + i * (TOK // n)
        return p // 2, pl.ds(pl.multiple_of(start, TOK // n), TOK // n)

    own_half, own_rows = rows_of(e, OWN, 0, 1)
    xcp = pltpu.make_async_copy(x_hbm, x_all.at[own_half, own_rows], lsem.at[0])
    xcp.start()
    rtcp = pltpu.make_async_copy(rt_hbm, rt, lsem.at[2])
    rtcp.start()

    barrier = pltpu.get_barrier_semaphore()

    def greet(oo, ee):
        pl.semaphore_signal(barrier, inc=1, device_id=(d, oo, ee), device_id_type=MESH)

    for q in range(1, 4):
        greet(o, rel[q])
    greet(nbp, e)

    @at_end
    def _():
        greet(planes[NEAR], e)

    @at_inner
    def _():
        greet(other, e)
        greet(planes[FAR], e)

    rtcp.wait()
    dup = (iota((TOK, 128), 1) % TOK == iota((TOK, 128), 0)).astype(BF16)
    r_all[side, e, o % 2] = dot(rt[...].astype(F32).astype(BF16), dup)

    xcp.wait()
    wrcp = pltpu.make_async_copy(wr_hbm, wr, lsem.at[1])
    wrcp.start()
    wcp = []
    for j in range(JLOC):
        a = pltpu.make_async_copy(wg_hbm.at[j], wgb.at[j], wsem.at[0, j])
        b = pltpu.make_async_copy(wu_hbm.at[j], wub.at[j], wsem.at[1, j])
        a.start()
        b.start()
        wcp.append((a, b))

    def wd_copy(n):
        return pltpu.make_async_copy(
            wd_hbm.at[:, :, pl.ds((n if n < EARLY else n - EARLY) * CW, CW)], wdb.at[n % WSLOT], dsem.at[n % WSLOT])

    for n in range(WSLOT):
        wd_copy(n).start()

    @at_end
    def _():
        pl.semaphore_wait(barrier, 5)

    @at_inner
    def _():
        pl.semaphore_wait(barrier, 6)

    def count(g, direction=MATE):
        return 4 if g == FAR or (g, direction) == (NB, CROSS) else 2

    targets = {OUT: (e, nbp, e), CROSS: (e, other, e), SIDE: (e, o, yp), MATE: (e, o, mate),
               PASS: (yp, o, mate), YCROSS: (yp, other, e), YOUT: (yp, nbp, e)}

    def block(g, i, n, direction):
        col, oo, ee = targets[direction]
        half, rows = rows_of(col, g, i, n)
        if direction in (MATE, PASS):
            x_sem, r_sem = mx_r.at[planes[g] // 2], mr_r.at[planes[g] // 2]
        else:
            lane = 0 if direction in (OUT, CROSS) else 1
            x_sem, r_sem = bx_r.at[lane, planes[g], i], br_r.at[lane, planes[g]]
        cps = [pltpu.make_async_remote_copy(
            src_ref=x_all.at[half, rows], dst_ref=x_all.at[half, rows],
            send_sem=bx_s.at[direction], recv_sem=x_sem,
            device_id=(d, oo, ee), device_id_type=MESH)]
        if i == 0:
            tile = r_all.at[half, col, planes[g] % 2]
            cps.insert(0, pltpu.make_async_remote_copy(
                src_ref=tile, dst_ref=tile,
                send_sem=br_s.at[direction], recv_sem=r_sem,
                device_id=(d, oo, ee), device_id_type=MESH))
        return cps

    def send(g, i, *directions):
        for direction in directions:
            n, base = count(g, direction), count(g)
            for k in range(i * n // base, (i + 1) * n // base):
                for cp in block(g, k, n, direction):
                    cp.start()

    def arrive(lane, g, i):
        n = count(g)
        half, rows = rows_of((e, yp)[lane], g, i, n)
        piece = x_all.at[half, rows]
        if i == 0:
            tile = r_all.at[half, (e, yp)[lane], planes[g] % 2]
            pltpu.make_async_copy(tile, tile, br_r.at[lane, planes[g]]).wait()
        pltpu.make_async_copy(piece, piece, bx_r.at[lane, planes[g], i]).wait()

    def sent(direction, nrows, ntiles):
        rows = x_all.at[0, pl.ds(0, nrows)]
        pltpu.make_async_copy(rows, rows, bx_s.at[direction]).wait()
        tiles = r_all.at[0, pl.ds(0, ntiles), 0]
        pltpu.make_async_copy(tiles, tiles, br_s.at[direction]).wait()

    def get(g, i, *directions):
        arrive(0, g, i)
        send(g, i, *directions, MATE)

    def yget(g, i, *directions):
        arrive(1, g, i)
        send(g, i, *directions, PASS)

    def routes_from_mate(ps):
        tiles = r_all.at[halves[ps], pl.ds(0, 2)]
        pltpu.make_async_copy(tiles, tiles, mr_r.at[halves[ps]]).wait()

    def rows_from_mate(ps):
        rows = x_all.at[halves[ps], pl.ds(0, 2 * CT)]
        pltpu.make_async_copy(rows, rows, mx_r.at[halves[ps]]).wait()

    def early_blocks():
        @at_end
        def _():
            for h in range(2):
                send(OWN, h, OUT, SIDE, MATE)
            for h in range(2):
                get(NB, h, SIDE)
                yget(OWN, h)
            get(NEAR, 0, SIDE)
            yget(NB, 0)

        @at_inner
        def _():
            for h in range(2):
                send(OWN, h, OUT, CROSS, SIDE, MATE)
            get(NB, 0, CROSS, SIDE)
            get(NEAR, 0, OUT)
            yget(OWN, 0)
            get(NB, 1, CROSS, SIDE)
            send(OWN, 0, YCROSS)
            get(NEAR, 1, OUT, SIDE)
            yget(OWN, 1)
            get(FAR, 0, OUT)
            get(FAR, 1, OUT)
            yget(NB, 0)

    def mid_blocks():
        @at_end
        def _():
            get(NEAR, 1, SIDE)
            yget(NB, 1)

        @at_inner
        def _():
            get(FAR, 2, OUT, SIDE)
            get(FAR, 3, OUT, SIDE)
            send(FAR, 0, SIDE)
            send(FAR, 1, SIDE)
            yget(NB, 1)

    zlate = ([(FAR, 0)], [(FAR, 1)], [(FAR, 2)], [(FAR, 3)], [], [], [], [])
    ylate_end = ([], [(NEAR, 0)], [], [(NEAR, 1)], [(FAR, 0)], [(FAR, 1)], [(FAR, 2)], [(FAR, 3)])
    ylate_inner = ([(NEAR, 0)], [(NEAR, 1), (FAR, 2)], [(FAR, 3)], [(FAR, 0)], [(FAR, 1)], [], [], [])

    def late_blocks(step):
        @at_end
        def _():
            for g, i in zlate[step]:
                if i < 2:
                    get(g, i, SIDE)
                else:
                    get(g, i)
            for g, i in ylate_end[step]:
                yget(g, i)

        if ylate_inner[step]:
            @at_inner
            def _():
                for g, i in ylate_inner[step]:
                    if g == FAR and i >= 2:
                        yget(g, i, YOUT)
                    else:
                        yget(g, i)

    col_i, row_i = iota((CT, CT), 1), iota((CT, CT), 0)
    same = col_i // TOK == row_i // TOK
    before = (same & (row_i < col_i)).astype(BF16)
    after = (same & (col_i < row_i)).astype(BF16)
    eye = (col_i == row_i).astype(BF16)
    low = iota((TOPK, CT), 1) < TOK
    mine = ((o * COLS + e) * JLOC).astype(F32)

    def choose(ps):
        half = halves[ps]
        r = r_all[half]
        routes = jnp.concatenate(
            [jnp.where(low, r[k, 0], r[k, 1]) for k in range(COLS)], axis=1)
        m = [jnp.max((routes == mine + j).astype(F32), axis=0, keepdims=True)
             for j in range(JLOC)]
        m = jnp.concatenate(m + [jnp.zeros((8 - JLOC, HT), F32)], axis=0)
        mb = m.astype(BF16)
        pos = jnp.concatenate(
            [dot(mb[:, k * CT:(k + 1) * CT], before) for k in range(COLS)], axis=1)
        pm = jnp.where(m > 0.5, pos, -1.0)
        ri, ci = iota((MR, HT), 0), iota((MR, HT), 1)
        q = (ri % GR) // CAP
        col = jnp.where(q == 0, rel[0], jnp.where(q == 1, rel[1], jnp.where(q == 2, rel[2], rel[3])))
        par = jnp.where(ri < GR, planes[2 * ps] % 2, planes[2 * ps + 1] % 2)
        want = jnp.where((ci // CT == col) & ((ci // TOK) % 2 == par), ri % CAP, -2).astype(F32)
        sel[...] = jnp.concatenate(
            [(pm[j:j + 1, :] == want).astype(F32) for j in range(JLOC)], axis=0).astype(BF16)

    def pick(ps):
        for n in range(DIM // 512):
            cols = pl.ds(n * 512, 512)
            got = dot(sel[...], x_all[halves[ps], :, cols])
            for j in range(JLOC):
                xs[j, :, cols] = got[j * MR:(j + 1) * MR].astype(BF16)

    def gates(ps):
        half = halves[ps]
        r = r_all[half, e]
        routes = jnp.where(low, r[0], r[1])
        exp_id = iota((NEXP, CT), 0).astype(F32)
        hot = jnp.zeros((NEXP, CT), F32)
        for k in range(TOPK):
            hot = hot + (routes[k:k + 1, :] == exp_id).astype(F32)
        hot = hot.astype(BF16)
        chosen = dot_nt(eye, hot) > 0.5
        pos = jnp.where(chosen, dot_nt(after, hot), -1.0)
        logits = dot_nt(x_all[half, pl.ds(pl.multiple_of(e * CT, CT), CT)], wr[...])
        top = jnp.max(jnp.where(chosen, logits, -jnp.inf), axis=1, keepdims=True)
        ex = jnp.where(chosen, jnp.exp(logits - top), 0.0)
        gate = ex / jnp.sum(ex, axis=1, keepdims=True)
        g1 = gate.astype(BF16)
        rest = gate - g1.astype(F32)
        g2 = rest.astype(BF16)
        g3 = (rest - g2.astype(F32)).astype(BF16)
        pos = pos.astype(BF16)
        slot = (iota((CT, SW), 1) % CAP).astype(F32)
        n_i = iota((NEXP, SW), 1)
        q = n_i // GR
        col = jnp.where(q == 0, rel[0], jnp.where(q == 1, rel[1], jnp.where(q == 2, rel[2], rel[3])))
        expert = (o * COLS + col) * JLOC + (n_i % GR) // CAP
        expand = (iota((NEXP, SW), 0) == expert).astype(BF16)
        hit = dot(pos, expand) == slot
        for k, g in enumerate((g1, g2, g3)):
            w = jnp.where(hit, dot(g, expand), 0.0)
            for i in range(2):
                par = planes[2 * ps + i] % 2
                wst[2 * ps + i, k * TOK:(k + 1) * TOK, :] = jnp.where(
                    par == 0, w[:TOK], w[TOK:]).astype(BF16)

    def gate_up(ps, j):
        if ps == 0:
            wcp[j][0].wait()
            wcp[j][1].wait()
        for n in range(FF // 512):
            cols = slice(n * 512, (n + 1) * 512)
            ga = dot(xs[j], wgb[j, :, cols])
            gu = dot(xs[j], wub[j, :, cols])
            hid[j, ps * MR:(ps + 1) * MR, cols] = (jax.nn.silu(ga) * gu).astype(BF16)

    def ycopy(g, k, q):
        return pltpu.make_async_remote_copy(
            src_ref=ysend.at[g, k, q - 1], dst_ref=yrecv.at[g, k, q],
            send_sem=ys_s, recv_sem=ys_r.at[g, k],
            device_id=(d, o, rel[q]), device_id_type=MESH)

    def half_cols(i):
        return pl.ds(i * (CW // 2), CW // 2)

    def ywait_half(i):
        rows = yrecv.at[FAR, 0, pl.ds(1, COLS - 1), :, half_cols(i)]
        pltpu.make_async_copy(rows, rows, ys_r.at[FAR, 0] if i == 0 else yh_r).wait()

    def ywait(g, k):
        if (g, k) == (FAR, 0):
            ywait_half(0)
            ywait_half(1)
            return
        rows = yrecv.at[g, k, pl.ds(1, COLS - 1)]
        pltpu.make_async_copy(rows, rows, ys_r.at[g, k]).wait()

    def ystart(g, k):
        if (g, k) == (FAR, 0):
            for i in range(2):
                for q in (2, 3, 1):
                    pltpu.make_async_remote_copy(
                        src_ref=ysend.at[g, k, q - 1, :, half_cols(i)],
                        dst_ref=yrecv.at[g, k, q, :, half_cols(i)],
                        send_sem=ys_s, recv_sem=ys_r.at[g, k] if i == 0 else yh_r,
                        device_id=(d, o, rel[q]), device_id_type=MESH).start()
            return
        for q in (2, 3, 1):
            ycopy(g, k, q).start()

    def down_chunk(ps, k):
        n = k if ps == 0 else EARLY + k
        both = ps == 1 and k >= EARLY
        first = 0 if both else ps * MR
        wd_copy(n).wait()
        outs = [dot(hid[j, first:(ps + 1) * MR], wdb[n % WSLOT, j]) for j in range(JLOC)]
        for pp in ((1, 0) if both else (ps,)):
            for i in range(2):
                g = 2 * pp + i
                for q in (2, 3, 1, 0):
                    at = pp * MR - first + i * GR + q * CAP
                    rows = jnp.concatenate([r[at:at + CAP] for r in outs], axis=0).astype(BF16)
                    if q:
                        ysend[g, k, q - 1] = rows
                    else:
                        yrecv[g, k, 0] = rows
        if ps == 0:
            ystart(NB, k)
        if n + WSLOT < EARLY + NC:
            wd_copy(n + WSLOT).start()

    def zcopy(k, g, slot, oo):
        return pltpu.make_async_remote_copy(
            src_ref=part.at[ZPART[g], k], dst_ref=zr.at[k, slot],
            send_sem=zs_s, recv_sem=zs_r.at[k, slot],
            device_id=(d, oo, e), device_id_type=MESH)

    def zwait(k, slot):
        rows = zr.at[k, slot]
        pltpu.make_async_copy(rows, rows, zs_r.at[k, slot]).wait()

    def half_copy(i, slot, oo):
        cols = pl.ds(i * (CW // 2), CW // 2)
        sem = zs_r.at[0, slot] if i == 0 else zh_r.at[slot // 4]
        return pltpu.make_async_remote_copy(
            src_ref=part.at[ZPART[FAR], 0, :, cols], dst_ref=zr.at[0, slot, :, cols],
            send_sem=zs_s, recv_sem=sem, device_id=(d, oo, e), device_id_type=MESH)

    def half_wait(i, slot):
        rows = zr.at[0, slot, :, pl.ds(i * (CW // 2), CW // 2)]
        pltpu.make_async_copy(rows, rows, zs_r.at[0, slot] if i == 0 else zh_r.at[slot // 4]).wait()

    def sums(g, *chunks):
        for k in chunks:
            ywait(g, k)
        for k in chunks:
            acc = dot(wst[g], yrecv[g, k].reshape(SW, CW))
            part[ZPART[g], k] = acc[0:TOK] + acc[TOK:2 * TOK] + acc[2 * TOK:3 * TOK]

    def zsend(k, g, slot, oo):
        zcopy(k, g, slot, oo).start()

    def relay(k, g, slot_in, slot_out, oo):
        zwait(k, slot_in)
        part[ZPART[g], k] = part[ZPART[g], k] + zr[k, slot_in]
        zcopy(k, g, slot_out, oo).start()

    def relay_far(k):
        if k:
            relay(k, FAR, 1, 4, other)
            return
        for i in range(2):
            cols = pl.ds(i * (CW // 2), CW // 2)
            half_wait(i, 1)
            part[ZPART[FAR], 0, :, cols] = part[ZPART[FAR], 0, :, cols] + zr[0, 1, :, cols]
            half_copy(i, 4, other).start()

    def relay_near(k):
        relay(k, NEAR, 2, 3, other)

    def relay_back(k):
        if k:
            relay(k, NB, 4, 0, nbp)
            return
        for i in range(2):
            half_wait(i, 4)
        part[ZPART[NB], 0] = part[ZPART[NB], 0] + zr[0, 4]
        zcopy(0, NB, 0, nbp).start()

    def finish(k, *slots):
        cols = pl.ds(k * CW, CW)
        for slot in slots:
            zwait(k, slot)
        total = part[ZPART[OWN], k]
        for slot in slots:
            total = total + zr[k, slot]
        out_ref[:, cols] = total.astype(BF16)

    early_blocks()
    wrcp.wait()
    gates(0)
    routes_from_mate(0)
    choose(0)
    mid_blocks()
    rows_from_mate(0)
    pick(0)
    for j in range(JLOC):
        gate_up(0, j)
        late_blocks(j)
    for k in range(EARLY):
        down_chunk(0, k)
        for step in {0: (4, 5), 1: (6,), 3: (7,)}.get(k, ()):
            late_blocks(step)

    def sums_nb(*chunks):
        sums(NB, *chunks)

        @at_end
        def _():
            for k in chunks:
                zsend(k, NB, 0, nbp)

    routes_from_mate(1)
    choose(1)
    rows_from_mate(1)
    pick(1)
    for j in range(JLOC):
        gate_up(1, j)
        if j < JLOC - 1:
            sums_nb(2 * j, 2 * j + 1)

    def sums_far(k):
        if k:
            sums(FAR, k)
            zsend(k, FAR, 1, nbp)
            return
        for i in range(2):
            ywait_half(i)
            acc = dot(wst[FAR], yrecv[FAR, 0, :, :, half_cols(i)].reshape(SW, CW // 2))
            part[ZPART[FAR], 0, :, half_cols(i)] = (
                acc[0:TOK] + acc[TOK:2 * TOK] + acc[2 * TOK:3 * TOK])
            half_copy(i, 1, nbp).start()

    lead = 3
    relayed = tuple(range(DIRECT, NC))
    for k in range(NC):
        down_chunk(1, k)
        if k == lead - 1:
            gates(1)

        @at_end
        def _():
            ystart(FAR, k)
            if k >= lead:
                sums_far(k - lead)

        @at_inner
        def _():
            if k < DIRECT:
                ystart(NEAR, k)
            if k == DIRECT - 1:
                for m in range(DIRECT):
                    ystart(FAR, m)
            if k >= DIRECT:
                ystart(FAR, k)
            if lead <= k < lead + DIRECT:
                sums(NEAR, k - lead)
                zsend(k - lead, NEAR, 3, other)

    @at_end
    def _():
        for k in relayed + tuple(range(DIRECT)):
            ystart(NEAR, k)
        for k in range(EARLY, NC):
            ystart(NB, k)
        for k in range(NC):
            ystart(OWN, k)
        for k in range(NC - lead, NC):
            sums_far(k)
        for k in relayed:
            sums(NEAR, k)
            zsend(k, NEAR, 2, nbp)
        for k in range(DIRECT):
            sums(NEAR, k)
            zsend(k, NEAR, 2, planes[NEAR])
        sums(NB, NC - 2, NC - 1)
        for k in (NC - 2, NC - 1):
            zsend(k, NB, 0, nbp)
        for k in range(0, NC, 2):
            sums(OWN, k, k + 1)
        for k in range(NC):
            finish(k, 0)

    @at_inner
    def _():
        for k in relayed:
            ystart(NEAR, k)
        for k in range(EARLY, NC):
            ystart(NB, k)
        for k in range(NC):
            ystart(OWN, k)
        for k in range(NC):
            sums(FAR, k)
            relay_far(k)
            if k >= 4:
                relay_back(k - 4)
        for n, k in enumerate(relayed):
            sums(NEAR, k)
            relay_near(k)
            if n < 4:
                relay_back(n + 4)
            if n == 1:
                sums(NB, NC - 2, NC - 1)
            if n >= 2:
                sums(OWN, 2 * n - 4, 2 * n - 3)
        for k in range(2 * (len(relayed) - 2), NC, 2):
            sums(OWN, k, k + 1)
        for k in relayed[:-2]:
            finish(k, 0, 3)
        for k in range(DIRECT):
            finish(k, 0, 3, 2)
        for k in relayed[-2:]:
            finish(k, 0, 3)


    sent(MATE, 4 * TOK, 4)
    sent(PASS, 4 * TOK, 4)

    @at_end
    def _():
        sent(SIDE, 7 * TOK // 2, 4)
        sent(OUT, TOK, 1)

    @at_inner
    def _():
        sent(SIDE, 7 * TOK // 2, 3)
        sent(OUT, 3 * TOK, 3)
        sent(CROSS, 2 * TOK, 2)
        sent(YCROSS, TOK // 2, 1)
        half_rows = x_all.at[0, pl.ds(0, TOK // 2)]
        pltpu.make_async_copy(half_rows, half_rows, bx_s.at[YOUT]).wait()

    pltpu.make_async_copy(ysend, ysend, ys_s).wait()
    moved = part.at[pl.ds(0, 3)]
    pltpu.make_async_copy(moved, moved, zs_s).wait()


def solution(mesh):
    row_spec = P(('data', 'outer', 'expert'), None)
    weight_spec = P(('outer', 'expert'), None, None)
    anyspace = pl.BlockSpec(memory_space=pl.ANY)
    dma = pltpu.SemaphoreType.DMA

    def per_device(tokens, w_router, routes, w_gate, w_up, w_down):
        return pl.pallas_call(
            kernel,
            name='moe',
            out_shape=pltpu.VMEM((TOK, DIM), BF16),
            in_specs=[anyspace] * 6,
            out_specs=pl.BlockSpec(memory_space=pltpu.VMEM),
            scratch_shapes=[
                pltpu.VMEM((2, HT, DIM), BF16),
                pltpu.VMEM((2, COLS, 2, TOPK, 128), F32),
                pltpu.VMEM((NEXP, DIM), BF16),
                pltpu.VMEM((TOPK, TOK), jnp.int32),
                pltpu.VMEM((JLOC * MR, HT), BF16),
                pltpu.VMEM((JLOC, MR, DIM), BF16),
                pltpu.VMEM((JLOC, DIM, FF), BF16),
                pltpu.VMEM((JLOC, DIM, FF), BF16),
                pltpu.VMEM((WSLOT, JLOC, FF, CW), BF16),
                pltpu.VMEM((JLOC, 2 * MR, FF), BF16),
                pltpu.VMEM((4, NC, COLS - 1, GR, CW), BF16),
                pltpu.VMEM((4, NC, COLS, GR, CW), BF16),
                pltpu.VMEM((4, 3 * TOK, SW), BF16),
                pltpu.VMEM((4, NC, TOK, CW), F32),
                pltpu.VMEM((NC, 5, TOK, CW), F32),
                dma((3,)), dma((2, JLOC)), dma((WSLOT,)),
                dma((7,)), dma((7,)),
                dma((2, PLANES, 4)), dma((2, PLANES)), dma((2,)), dma((2,)),
                dma, dma((4, NC)), dma, dma((NC, 5)), dma((2,)), dma,
            ],
            compiler_params=pltpu.CompilerParams(
                collective_id=0, has_side_effects=True, vmem_limit_bytes=67043328 - (1 << 20)),
        )(tokens, w_router.T, routes.T, w_gate, w_up, w_down)

    return jax.shard_map(
        per_device, mesh=mesh,
        in_specs=(row_spec, P(), row_spec, weight_spec, weight_spec, weight_spec),
        out_specs=row_spec, check_vma=False)
```
